8 devices in a mesh: col: 2 (over z, y), row: 4 (over x, core).
Axes of the slice: x: 2, y: 2, z: 1, core: 2. Of those that a mesh axis runs over, the one named last changes fastest.
Arguments:
- w_gate: float32 [2560, 6720], P('row', 'col')
- w_up: float32 [2560, 6720], P('row', 'col')
- w_down: float32 [6720, 2560], P('row', 'col')
- x_norm: bfloat16 [1024, 2560], P(None, 'row')
- x_act: bfloat16 [1024, 6720], P(None, 'row')
- dy_gate: bfloat16 [1024, 6720], P(None, 'col')
- dy_up: bfloat16 [1024, 6720], P(None, 'col')
- dy_down: bfloat16 [1024, 2560], P(None, 'col')
- r_gate: float32 [2560], P('row')
- c_gate: float32 [6720], P('col')
- r_up: float32 [2560], P('row')
- c_up: float32 [6720], P('col')
- r_down: float32 [6720], P('row')
- c_down: float32 [2560], P('col')
- hyper_params: float32 [3], replicated
Outputs:
- output 1: float32 [2560, 6720], P('row', 'col')
- output 2: float32 [2560, 6720], P('row', 'col')
- output 3: float32 [6720, 2560], P('row', 'col')
- output 4: float32 [2560], P('row')
- output 5: float32 [6720], P('col')
- output 6: float32 [2560], P('row')
- output 7: float32 [6720], P('col')
- output 8: float32 [6720], P('row')
- output 9: float32 [2560], P('col')
- output 10: bfloat16 [1024, 2560], P(None, 'row')
- output 11: bfloat16 [1024, 6720], P(None, 'row')
All inputs are finite; a program needn't handle non-finite values.
Results may differ from the reference program's by a relative error of at most 0.001.
Values are sent between devices in bfloat16 or wider.
A program may use at most 1 GiB of HBM per device.

```python
import jax
import jax.numpy as jnp
from jax import lax

D_MODEL = 2560
D_FF = 6720
TOKENS = 1024
EPS_ONE = 1e-30
EPS_TWO = 1e-3
TWO_PI = 6.283185307179586


def smooth_field(key, length, log_scale):
    key_amp, key_phase = jax.random.split(key)
    ampl_k = jax.random.normal(key_amp, (3,), jnp.float32)
    phase_k = jax.random.uniform(key_phase, (3,), jnp.float32, minval=0.0, maxval=TWO_PI)
    position = jnp.arange(length, dtype=jnp.float32) / length
    freq_k = jnp.arange(1, 4, dtype=jnp.float32)
    waves = jnp.cos(TWO_PI * position[:, None] * freq_k[None, :] + phase_k[None, :])
    return jnp.exp(log_scale * jnp.sum(waves * ampl_k[None, :], axis=1) / 1.7)


def draw_weight(key, rows, cols):
    key_z, key_r, key_c = jax.random.split(key, 3)
    noise = jax.random.normal(key_z, (rows, cols), jnp.float32)
    row_prof = smooth_field(key_r, rows, 0.5)
    col_prof = smooth_field(key_c, cols, 0.5)
    return noise * (rows ** -0.5) * row_prof[:, None] * col_prof[None, :]


def draw_tokens(key, cols, scale):
    key_z, key_a, key_b = jax.random.split(key, 3)
    noise = jax.random.normal(key_z, (TOKENS, cols), jnp.float32)
    first_half = (jnp.arange(TOKENS) < TOKENS // 2)[:, None]
    profile = jnp.where(first_half, smooth_field(key_a, cols, 0.8)[None, :], smooth_field(key_b, cols, 0.8)[None, :])
    return (noise * profile * scale).astype(jnp.bfloat16)


def draw_stat(key, length):
    return jax.random.uniform(key, (length,), jnp.float32, minval=0.5, maxval=3.0)


def setup_inputs(seed: int = 0) -> dict:
    keys = jax.random.split(jax.random.key(seed), 15)
    tok_scale = TOKENS ** -0.5
    low_end = jnp.array([0.6, 0.6, 0.15], dtype=jnp.float32)
    span_len = jnp.array([0.25, 0.6, 0.15], dtype=jnp.float32)
    unit_draw = jax.random.uniform(keys[14], (3,), jnp.float32)
    return {
        'w_gate': draw_weight(keys[0], D_MODEL, D_FF),
        'w_up': draw_weight(keys[1], D_MODEL, D_FF),
        'w_down': draw_weight(keys[2], D_FF, D_MODEL),
        'x_norm': draw_tokens(keys[3], D_MODEL, tok_scale),
        'x_act': draw_tokens(keys[4], D_FF, tok_scale),
        'dy_gate': draw_tokens(keys[5], D_FF, 1.0),
        'dy_up': draw_tokens(keys[6], D_FF, 1.0),
        'dy_down': draw_tokens(keys[7], D_MODEL, 1.0),
        'r_gate': draw_stat(keys[8], D_MODEL),
        'c_gate': draw_stat(keys[9], D_FF),
        'r_up': draw_stat(keys[10], D_MODEL),
        'c_up': draw_stat(keys[11], D_FF),
        'r_down': draw_stat(keys[12], D_FF),
        'c_down': draw_stat(keys[13], D_MODEL),
        'hyper_params': low_end + span_len * unit_draw,
    }


def factored_step(w_old, grad_w, r_old, c_old, hyper_params):
    beta_two = hyper_params[0]
    grad_sq = grad_w * grad_w + EPS_ONE
    r_new = beta_two * r_old + (1.0 - beta_two) * jnp.mean(grad_sq, axis=1)
    c_new = beta_two * c_old + (1.0 - beta_two) * jnp.mean(grad_sq, axis=0)
    v_est = r_new[:, None] * c_new[None, :] / jnp.mean(r_new)
    update = grad_w * lax.rsqrt(v_est)
    rms_u = jnp.sqrt(jnp.mean(update * update))
    update_hat = update / jnp.maximum(1.0, rms_u / hyper_params[2])
    step_size = hyper_params[1] * jnp.maximum(EPS_TWO, jnp.sqrt(jnp.mean(w_old * w_old)))
    return w_old - step_size * update_hat, r_new, c_new


def weight_grad(activations, grad_out):
    return jnp.dot(activations.T, grad_out, preferred_element_type=jnp.float32)


def input_grad(grad_out, weight):
    return jnp.dot(grad_out, weight.astype(jnp.bfloat16).T, preferred_element_type=jnp.float32)


def reference(w_gate, w_up, w_down, x_norm, x_act, dy_gate, dy_up, dy_down, r_gate, c_gate, r_up, c_up, r_down, c_down, hyper_params):
    new_gate, r_gate_new, c_gate_new = factored_step(w_gate, weight_grad(x_norm, dy_gate), r_gate, c_gate, hyper_params)
    new_up, r_up_new, c_up_new = factored_step(w_up, weight_grad(x_norm, dy_up), r_up, c_up, hyper_params)
    new_down, r_down_new, c_down_new = factored_step(w_down, weight_grad(x_act, dy_down), r_down, c_down, hyper_params)
    dx_norm = (input_grad(dy_gate, w_gate) + input_grad(dy_up, w_up)).astype(jnp.bfloat16)
    dx_act = input_grad(dy_down, w_down).astype(jnp.bfloat16)
    return (new_gate, new_up, new_down, r_gate_new, c_gate_new, r_up_new, c_up_new, r_down_new, c_down_new, dx_norm, dx_act)
```

```python
import jax
import jax.numpy as jnp
from jax import lax
from jax.sharding import PartitionSpec as P

EPS_ONE = 1e-30
EPS_TWO = 1e-3
CHUNKS = (432, 416, 416, 416)


TO_0 = [(1, 0)]
TO_1 = [(0, 1)]
SWAP = [(0, 1), (1, 0)]
ROW_X = [(0, 2), (2, 0), (1, 3), (3, 1)]
ROW_C = [(0, 1), (1, 0), (2, 3), (3, 2)]
BF16 = jnp.bfloat16
F32 = jnp.float32


def weight_grad(activations, grad_out):
    return lax.dot_general(activations, grad_out, (((0,), (0,)), ((), ())), preferred_element_type=F32)


def input_grad(grad_out, weight):
    return lax.dot_general(grad_out, weight.astype(BF16), (((1,), (1,)), ((), ())), preferred_element_type=F32)


def row_total(v):
    v = v + lax.ppermute(v, 'row', ROW_C)
    return v + lax.ppermute(v, 'row', ROW_X)


def solution(mesh):
    row_size = mesh.shape['row']
    col_size = mesh.shape['col']
    weight_spec = P('row', 'col')
    act_spec = P(None, 'row')
    grad_spec = P(None, 'col')
    in_specs = (weight_spec,) * 3 + (act_spec, act_spec) + (grad_spec,) * 3 + (P('row'), P('col')) * 3 + (P(),)
    out_specs = (weight_spec,) * 3 + (P('row'), P('col')) * 3 + (act_spec, act_spec)

    def body(w_gate, w_up, w_down, x_norm, x_act, dy_gate, dy_up, dy_down, r_gate, c_gate, r_up, c_up, r_down, c_down, hyper_params):
        d_model = w_gate.shape[0] * row_size
        d_ff = w_gate.shape[1] * col_size
        tokens = dy_down.shape[0]
        col = lax.axis_index('col')
        row = lax.axis_index('row')
        beta_two = hyper_params[0]

        quarter = tokens // row_size
        mine = lax.dynamic_slice(dy_down, (row * quarter, 0), (quarter, dy_down.shape[1]))
        q0 = lax.ppermute(mine, 'col', TO_0)
        q2 = lax.ppermute(q0, 'row', ROW_X)
        q1 = lax.ppermute(q0, 'row', ROW_C)
        q3 = lax.ppermute(q2, 'row', ROW_C)
        odd = (row % 2) == 1
        high = (row // 2) == 1
        near = jnp.concatenate([jnp.where(odd, q1, q0), jnp.where(odd, q0, q1)], axis=0)
        far = jnp.concatenate([jnp.where(odd, q3, q2), jnp.where(odd, q2, q3)], axis=0)
        dy_other = jnp.concatenate([jnp.where(high, far, near), jnp.where(high, near, far)], axis=0)

        part = input_grad(dy_gate, w_gate) + input_grad(dy_up, w_up)
        part_in = lax.ppermute(part, 'col', TO_1)

        w_down_b = w_down.astype(BF16)
        w_in = []
        at = 0
        for n in CHUNKS:
            w_in.append(lax.ppermute(w_down_b[at:at + n], 'col', TO_0))
            at += n

        grads = [weight_grad(x_norm, dy_gate), weight_grad(x_norm, dy_up), weight_grad(x_act, dy_down)]
        weights = [w_gate, w_up, w_down]
        olds = [(r_gate, c_gate), (r_up, c_up), (r_down, c_down)]
        sizes = [(d_model, d_ff), (d_model, d_ff), (d_ff, d_model)]
        row_sums, col_sums = [], []
        for g in grads:
            g_sq = g * g + EPS_ONE
            row_sums.append(jnp.sum(g_sq, axis=1))
            col_sums.append(jnp.sum(g_sq, axis=0))
        row_sums = jnp.concatenate(row_sums)
        row_sums = row_sums + lax.ppermute(row_sums, 'col', SWAP)
        col_sums = row_total(jnp.concatenate(col_sums))
        scalars = []
        news = []
        ra = ca = 0
        for g, w, (r, c), (m, n) in zip(grads, weights, olds, sizes):
            r_new = beta_two * r + (1.0 - beta_two) * (row_sums[ra:ra + r.shape[0]] / n)
            c_new = beta_two * c + (1.0 - beta_two) * (col_sums[ca:ca + c.shape[0]] / m)
            ra += r.shape[0]
            ca += c.shape[0]
            rr = lax.rsqrt(r_new)
            cc = lax.rsqrt(c_new)
            u = g * rr[:, None] * cc[None, :]
            scalars += [jnp.sum(u * u), jnp.sum(w * w), jnp.sum(r_new) / col_size]
            news.append((r_new, c_new, rr, cc))
        scal = row_total(jnp.stack(scalars))
        scal = scal + lax.ppermute(scal, 'col', SWAP)
        outs = []
        for k, (g, w, (m, n)) in enumerate(zip(grads, weights, sizes)):
            r_new, c_new, rr, cc = news[k]
            r_mean = scal[3 * k + 2] / m
            rms_u = jnp.sqrt(scal[3 * k] * r_mean / (m * n))
            step = hyper_params[1] * jnp.maximum(EPS_TWO, jnp.sqrt(scal[3 * k + 1] / (m * n)))
            scale = step * jnp.sqrt(r_mean) / jnp.maximum(1.0, rms_u / hyper_params[2])
            outs.append(w - g * (rr * scale)[:, None] * cc[None, :])

        dxn = (part + part_in).astype(BF16)
        dxn_in = lax.ppermute(dxn, 'col', TO_0)
        dx_norm = jnp.where(col == 1, dxn, dxn_in)

        dxa = []
        at = 0
        for n, w_other in zip(CHUNKS, w_in):
            dims = (((1,), (1,)), ((), ()))
            o = lax.dot_general(w_down_b[at:at + n], dy_down, dims, preferred_element_type=F32)
            o = o + lax.dot_general(w_other, dy_other, dims, preferred_element_type=F32)
            o = o.astype(BF16)
            dxa.append(jnp.where(col == 0, o, lax.ppermute(o, 'col', TO_1)))
            at += n
        dx_act = jnp.concatenate(dxa, axis=0).T
        (ng, nu, nd) = outs
        return (ng, nu, nd, news[0][0], news[0][1], news[1][0], news[1][1], news[2][0], news[2][1], dx_norm, dx_act)

    return jax.shard_map(body, mesh=mesh, in_specs=in_specs, out_specs=out_specs, check_vma=False)
```

```python
import functools

import jax
import jax.numpy as jnp
from jax import lax
from jax.experimental import pallas as pl
from jax.experimental.pallas import tpu as pltpu
from jax.sharding import PartitionSpec as P

EPS_ONE = 1e-30
EPS_TWO = 1e-3
STEPS = 7
BF16 = jnp.bfloat16
F32 = jnp.float32
MESH = pl.DeviceIdType.MESH
ANY = pl.BlockSpec(memory_space=pl.ANY)
VM = pl.BlockSpec(memory_space=pltpu.VMEM)

P_SENT = (240, 160, 64)
W_SENT = (320, 256, 96)
W_LATER = (512, 496)


def fold(v, width=128):
    acc = v[:, :width]
    for k in range(1, v.shape[1] // width):
        acc = acc + v[:, k * width:(k + 1) * width]
    return acc


def fold_rows(v):
    return jnp.sum(v.reshape(v.shape[0] // 8, 8, v.shape[1]), axis=0)


def lane_total(v):
    s = jnp.sum(jnp.sum(v, axis=0, keepdims=True), axis=1, keepdims=True)
    lane = lax.broadcasted_iota(jnp.int32, (1, 128), 1)
    return jnp.where(lane == 0, jnp.broadcast_to(s, (1, 128)), 0.0)


def column(row_vec):
    return jnp.broadcast_to(row_vec, (128, row_vec.shape[1])).T


def fused(nc, nr, sizes,
          wg, wu, wd, xn, xa, dg, du, dd, rg, ru, rd, cg, cu, cd, hyper,
          gg, gu, gd, part, part_in, wb, w_in, dy_in, r_out, c_out, s_out,
          xn_v, dd_v, p_v, r_mine, r_peer, c_all, s_all, wsq, wsq_d, rr, cc, racc, cacc, sacc,
          loc, dsem, qsem, psem, wsem, rsem, csem, ssem):
    col = lax.axis_index('col')
    row = lax.axis_index('row')
    d_model, d_ff = sizes
    nb = dg.shape[0] // STEPS
    mb = wd.shape[0] // STEPS
    quarter = dd.shape[0] // nr
    others = [(dc, dr) for dc in range(nc) for dr in range(nr) if (dc, dr) != (0, 0)]

    load_x = pltpu.make_async_copy(xn, xn_v, loc.at[0])
    load_d = pltpu.make_async_copy(dd, dd_v, loc.at[1])
    load_x.start()
    load_d.start()

    me = col * nr + row
    c_all[row] = jnp.zeros(c_all.shape[1:], F32)
    s_all[me] = jnp.zeros(s_all.shape[1:], F32)

    barrier = pltpu.get_barrier_semaphore()
    for dc, dr in others:
        pl.semaphore_signal(barrier, 1, device_id=(lax.rem(col + dc, nc), lax.rem(row + dr, nr)), device_id_type=MESH)
    pl.semaphore_wait(barrier, len(others))

    def remote(src, dst, sems, k, target):
        return pltpu.make_async_remote_copy(src_ref=src, dst_ref=dst, send_sem=sems.at[0, k], recv_sem=sems.at[1, k],
                                            device_id=target, device_id_type=MESH)

    across = (1 - col, row)
    own_rows = pl.ds(pl.multiple_of(row * quarter, quarter), quarter)
    dy_copy = remote(dd.at[own_rows], dy_in.at[own_rows], dsem, 0, across)

    @pl.when(col == 1)
    def _():
        dy_copy.start()

    p_v[...] = jnp.zeros_like(p_v)
    wsq[...] = jnp.zeros_like(wsq)
    wsq_d[...] = jnp.zeros_like(wsq_d)

    def part_body(wg_b, wu_b, dg_b, du_b):
        for k, (w_b, d_b) in enumerate(((wg_b, dg_b), (wu_b, du_b))):
            w = w_b[...]
            wsq[pl.ds(8 * k, 8), :] += fold_rows(w * w)
            p_v[...] += lax.dot_general(w.astype(BF16), d_b[...], (((0,), (0,)), ((), ())), preferred_element_type=F32)

    by_n = lambda width: pl.BlockSpec((nb, width), lambda k: (k, 0))
    by_m = lambda width: pl.BlockSpec((mb, width), lambda k: (k, 0))
    pltpu.emit_pipeline(part_body, grid=(STEPS,), in_specs=[by_n(wg.shape[1])] * 2 + [by_n(dg.shape[1])] * 2)(wg, wu, dg, du)

    save_p = pltpu.make_async_copy(p_v, part, loc.at[2])
    save_p.start()
    p_copies, w_copies = [], []
    at = 0
    for k, n in enumerate(P_SENT):
        p_copies.append(remote(p_v.at[pl.ds(at, n)], part_in.at[pl.ds(at, n)], psem, k, across))
        at += n
    at = 0
    for k, n in enumerate(W_SENT):
        w_copies.append(remote(wb.at[pl.ds(at, n)], w_in.at[pl.ds(at, n)], wsem, k, across))
        at += n

    @pl.when(col == 0)
    def _():
        p_copies[0].start()

    def cast_body(w_b, o_b):
        w = w_b[...]
        wsq_d[...] += fold_rows(w * w)
        o_b[...] = w.astype(BF16)

    pltpu.emit_pipeline(cast_body, grid=(STEPS,), in_specs=[by_m(wd.shape[1])], out_specs=[by_m(wd.shape[1])])(wd, wb)

    @pl.when(col == 1)
    def _():
        w_copies[0].start()

    q_copies = []
    for d in range(1, nr):
        q_copies.append(pltpu.make_async_remote_copy(
            src_ref=dy_in.at[own_rows], dst_ref=dy_in.at[own_rows], send_sem=qsem.at[0, d], recv_sem=qsem.at[1, row],
            device_id=(col, lax.rem(row + d, nr)), device_id_type=MESH))

    @pl.when(col == 0)
    def _():
        dy_copy.wait_recv()
        for q in q_copies:
            q.start()

    load_x.wait()
    load_d.wait()
    r_mine[...] = jnp.zeros_like(r_mine)
    racc[...] = jnp.zeros_like(racc)
    cacc[...] = jnp.zeros_like(cacc)

    def grad_body(dg_b, du_b, xa_b, gg_b, gu_b, gd_b):
        k = pl.program_id(0)
        for t, (d_b, g_b) in enumerate(((dg_b, gg_b), (du_b, gu_b))):
            g = jnp.dot(d_b[...], xn_v[...], preferred_element_type=F32)
            g_b[...] = g
            q = g * g + EPS_ONE
            racc[pl.ds(8 * t, 8), :] += fold_rows(q)
            c_all[row, pl.ds(7 * t + k, 1), :] = jnp.sum(fold(q).T, axis=0, keepdims=True)
        g = jnp.dot(xa_b[...], dd_v[...], preferred_element_type=F32)
        gd_b[...] = g
        q = g * g + EPS_ONE
        cacc[...] += fold_rows(q)
        r_mine[pl.ds(8 + k, 1), pl.ds(0, 240)] = jnp.sum(fold(q).T, axis=0, keepdims=True)

    pltpu.emit_pipeline(grad_body, grid=(STEPS,), in_specs=[by_n(dg.shape[1])] * 2 + [by_m(xa.shape[1])],
                        out_specs=[by_n(gg.shape[1])] * 2 + [by_m(gd.shape[1])])(dg, du, xa, gg, gu, gd)

    for t in range(2):
        r_mine[t:t + 1, :] = jnp.sum(racc[8 * t:8 * t + 8, :], axis=0, keepdims=True)
    c_down = jnp.sum(cacc[...], axis=0, keepdims=True)
    for k in range(5):
        c_all[row, 14 + k:15 + k, 0:256] = c_down[:, 256 * k:256 * (k + 1)]

    r_copy = remote(r_mine, r_peer, rsem, 0, across)
    r_copy.start()
    c_copies = [pltpu.make_async_remote_copy(
        src_ref=c_all.at[row], dst_ref=c_all.at[row], send_sem=csem.at[0, d], recv_sem=csem.at[1, row],
        device_id=(col, lax.rem(row + d, nr)), device_id_type=MESH) for d in range(1, nr)]
    for c in c_copies:
        c.start()

    @pl.when(col == 0)
    def _():
        p_copies[1].start()

    @pl.when(col == 1)
    def _():
        w_copies[1].start()

    beta = hyper[0]
    rr[...] = jnp.ones_like(rr)
    rr[0:1, :] = rg[...]
    rr[1:2, :] = ru[...]
    for k in range(STEPS):
        cc[k:k + 1, :] = cg[:, nb * k:nb * (k + 1)]
        cc[7 + k:8 + k, :] = cu[:, nb * k:nb * (k + 1)]
        rr[8 + k:9 + k, 0:mb] = rd[:, mb * k:mb * (k + 1)]
    for k in range(5):
        cc[14 + k:15 + k, 0:256] = cd[:, 256 * k:256 * (k + 1)]
        cc[14 + k:15 + k, 256:480] = jnp.ones((1, 224), F32)
    cc[19:24, :] = jnp.ones((5, 480), F32)

    r_copy.wait()
    for d in range(1, nr):
        c_copies[d - 1].wait_send()
        s = lax.rem(row + d, nr)
        pltpu.make_async_remote_copy(src_ref=c_all.at[s], dst_ref=c_all.at[s], send_sem=csem.at[0, d], recv_sem=csem.at[1, s],
                                     device_id=(col, s), device_id_type=MESH).wait_recv()

    line = lax.broadcasted_iota(jnp.int32, rr.shape, 0)
    r_new = beta * rr[...] + (1.0 - beta) * ((r_mine[...] + r_peer[...]) / jnp.where(line < 8, float(d_ff), float(d_model)))
    line = lax.broadcasted_iota(jnp.int32, cc.shape, 0)
    c_sum = (c_all[0] + c_all[1]) + (c_all[2] + c_all[3])
    c_new = beta * cc[...] + (1.0 - beta) * (c_sum / jnp.where(line < 14, float(d_model), float(d_ff)))
    r_out[...] = r_new
    c_out[...] = c_new
    rr[...] = lax.rsqrt(r_new)
    cc[...] = lax.rsqrt(c_new)

    sacc[...] = jnp.zeros_like(sacc)

    def square_body(gg_b, gu_b, gd_b):
        k = pl.program_id(0)
        for t, g_b in enumerate((gg_b, gu_b)):
            u = g_b[...] * rr[t:t + 1, :]
            s = fold(u * u)
            c = column(cc[pl.ds(7 * t + k, 1), :])
            sacc[pl.ds(8 * t, 8), :] += fold_rows(s * (c * c))
        c_row = jnp.concatenate([cc[14 + j:15 + j, 0:256] for j in range(5)], axis=1)
        u = gd_b[...] * c_row
        s = fold(u * u)
        r = column(rr[pl.ds(8 + k, 1), :])[0:mb]
        sacc[16:24, :] += fold_rows(s * (r * r))

    pltpu.emit_pipeline(square_body, grid=(STEPS,), in_specs=[by_n(gg.shape[1])] * 2 + [by_m(gd.shape[1])])(gg, gu, gd)

    for t in range(3):
        s_all[me, t:t + 1, :] = jnp.sum(sacc[8 * t:8 * t + 8, :], axis=0, keepdims=True)
    for t in range(2):
        s_all[me, 3 + t:4 + t, :] = jnp.sum(fold(wsq[8 * t:8 * t + 8, :]), axis=0, keepdims=True)
        s_all[me, 6 + t:7 + t, :] = lane_total(r_new[t:t + 1, :])
    s_all[me, 5:6, :] = jnp.sum(fold(wsq_d[...]), axis=0, keepdims=True)
    s_all[me, 8:9, :] = lane_total(r_new[8:15, 0:mb])
    s_copies = []
    for j, (dc, dr) in enumerate(others):
        tc, tr = lax.rem(col + dc, nc), lax.rem(row + dr, nr)
        s_copies.append(pltpu.make_async_remote_copy(
            src_ref=s_all.at[me], dst_ref=s_all.at[me], send_sem=ssem.at[0, j], recv_sem=ssem.at[1, me],
            device_id=(tc, tr), device_id_type=MESH))
    for s in s_copies:
        s.start()

    @pl.when(col == 0)
    def _():
        p_copies[2].start()

    @pl.when(col == 1)
    def _():
        w_copies[2].start()

    for j, (dc, dr) in enumerate(others):
        tc, tr = lax.rem(col + dc, nc), lax.rem(row + dr, nr)
        s_copies[j].wait_send()
        him = tc * nr + tr
        pltpu.make_async_remote_copy(src_ref=s_all.at[him], dst_ref=s_all.at[him], send_sem=ssem.at[0, j],
                                     recv_sem=ssem.at[1, him], device_id=(tc, tr), device_id_type=MESH).wait_recv()
    total = s_all[0]
    for j in range(1, nc * nr):
        total = total + s_all[j]
    s_out[...] = total

    save_p.wait()

    @pl.when(col == 0)
    def _():
        for p in p_copies:
            p.wait_send()
        for w in w_copies:
            w.wait_recv()
        for d in range(1, nr):
            q_copies[d - 1].wait_send()
            s = lax.rem(row + d, nr)
            rows = pl.ds(pl.multiple_of(s * quarter, quarter), quarter)
            pltpu.make_async_remote_copy(src_ref=dy_in.at[rows], dst_ref=dy_in.at[rows], send_sem=qsem.at[0, d],
                                         recv_sem=qsem.at[1, s], device_id=(col, s), device_id_type=MESH).wait_recv()

    @pl.when(col == 1)
    def _():
        dy_copy.wait_send()
        for p in p_copies:
            p.wait_recv()
        for w in w_copies:
            w.wait_send()


def run_fused(nc, nr, sizes, wg, wu, wd, xn, xa, dg, du, dd, rg, ru, rd, cg, cu, cd, hyper):
    f32, b16 = (lambda *s: jax.ShapeDtypeStruct(s, F32)), (lambda *s: jax.ShapeDtypeStruct(s, BF16))
    n, i = wg.shape
    m, h = wd.shape
    t = dd.shape[0]
    dma = lambda *s: pltpu.SemaphoreType.DMA(s)
    return pl.pallas_call(
        functools.partial(fused, nc, nr, sizes),
        out_shape=(f32(n, i), f32(n, i), f32(m, h), f32(i, t), f32(sum(P_SENT), t), b16(m, h), b16(sum(W_SENT), h),
                   b16(t, h), f32(16, 640), f32(24, 480), f32(16, 128)),
        in_specs=[ANY] * 8 + [VM] * 6 + [pl.BlockSpec(memory_space=pltpu.SMEM)],
        out_specs=[ANY] * 8 + [VM] * 3,
        scratch_shapes=[
            pltpu.VMEM(xn.shape, BF16), pltpu.VMEM(dd.shape, BF16), pltpu.VMEM((i, t), F32),
            pltpu.VMEM((16, 640), F32), pltpu.VMEM((16, 640), F32), pltpu.VMEM((nr, 24, 480), F32),
            pltpu.VMEM((nc * nr, 16, 128), F32), pltpu.VMEM((16, i), F32), pltpu.VMEM((8, h), F32),
            pltpu.VMEM((16, 640), F32), pltpu.VMEM((24, 480), F32), pltpu.VMEM((16, i), F32), pltpu.VMEM((8, h), F32),
            pltpu.VMEM((24, 128), F32),
            dma(3), dma(2, 1), dma(2, nr), dma(2, 3), dma(2, 3), dma(2, 1), dma(2, nr), dma(2, nc * nr)],
        compiler_params=pltpu.CompilerParams(collective_id=0, has_side_effects=True, vmem_limit_bytes=44 * 1024 * 1024),
        cost_estimate=pl.CostEstimate(flops=22_000_000_000, bytes_accessed=150_000_000, transcendentals=0),
        name="fused",
    )(wg, wu, wd, xn, xa, dg, du, dd, rg, ru, rd, cg, cu, cd, hyper)


TO_0 = [(1, 0)]
TO_1 = [(0, 1)]


def solution(mesh):
    row_size = mesh.shape['row']
    col_size = mesh.shape['col']
    weight_spec = P('row', 'col')
    act_spec = P(None, 'row')
    grad_spec = P(None, 'col')
    in_specs = (weight_spec,) * 3 + (act_spec, act_spec) + (grad_spec,) * 3 + (P('row'), P('col')) * 3 + (P(),)
    out_specs = (weight_spec,) * 3 + (P('row'), P('col')) * 3 + (act_spec, act_spec)

    def body(w_gate, w_up, w_down, x_norm, x_act, dy_gate, dy_up, dy_down, r_gate, c_gate, r_up, c_up, r_down, c_down, hyper_params):
        d_model = w_gate.shape[0] * row_size
        d_ff = w_gate.shape[1] * col_size
        col = lax.axis_index('col')
        gg, gu, gd, part, part_in, wb, w_in, dy_in, r_all, c_all, s_all = run_fused(
            col_size, row_size, (d_model, d_ff),
            w_gate.T, w_up.T, w_down, x_norm, x_act.T, dy_gate.T, dy_up.T, dy_down,
            r_gate[None], r_up[None], r_down[None], c_gate[None], c_up[None], c_down[None], hyper_params)
        sp, sw = sum(P_SENT), sum(W_SENT)

        part_late = lax.ppermute(part[sp:], 'col', TO_1)
        w_late = []
        at = sw
        for n in W_LATER:
            w_late.append(lax.ppermute(wb[at:at + n], 'col', TO_0))
            at += n

        def act_grad(first, count, w_other):
            dims = (((1,), (1,)), ((), ()))
            o = lax.dot_general(wb[first:first + count], dy_down, dims, preferred_element_type=F32)
            o = o + lax.dot_general(w_other, dy_in, dims, preferred_element_type=F32)
            o = o.astype(BF16)
            return jnp.where(col == 0, o, lax.ppermute(o, 'col', TO_1))

        dxa = [act_grad(0, sw, w_in)]

        r_new = [r_all[0], r_all[1], r_all[8:15, :w_down.shape[0] // STEPS].reshape(-1)]
        c_new = [c_all[0:7].reshape(-1), c_all[7:14].reshape(-1), c_all[14:19, :256].reshape(-1)]
        scal = jnp.sum(s_all, axis=1)
        outs = []
        for k, (g, w, (m, n)) in enumerate(((gg.T, w_gate, (d_model, d_ff)), (gu.T, w_up, (d_model, d_ff)), (gd, w_down, (d_ff, d_model)))):
            r_mean = scal[6 + k] / (m * col_size)
            rms_u = jnp.sqrt(scal[k] * r_mean / (m * n))
            step = hyper_params[1] * jnp.maximum(EPS_TWO, jnp.sqrt(scal[3 + k] / (m * n)))
            scale = step * jnp.sqrt(r_mean) / jnp.maximum(1.0, rms_u / hyper_params[2])
            outs.append(w - g * (lax.rsqrt(r_new[k]) * scale)[:, None] * lax.rsqrt(c_new[k])[None, :])

        dxn = (part + jnp.concatenate([part_in, part_late], axis=0)).astype(BF16).T
        dx_norm = jnp.where(col == 1, dxn, lax.ppermute(dxn, 'col', TO_0))
        at = sw
        for n, w_other in zip(W_LATER, w_late):
            dxa.append(act_grad(at, n, w_other))
            at += n
        dx_act = jnp.concatenate(dxa, axis=0).T
        return (*outs, r_new[0], c_new[0], r_new[1], c_new[1], r_new[2], c_new[2], dx_norm, dx_act)

    return jax.shard_map(body, mesh=mesh, in_specs=in_specs, out_specs=out_specs, check_vma=False)
```

```python
import functools

import jax
import jax.numpy as jnp
from jax import lax
from jax.experimental import pallas as pl
from jax.experimental.pallas import tpu as pltpu
from jax.sharding import PartitionSpec as P

EPS_ONE = 1e-30
EPS_TWO = 1e-3
STEPS = 7
BF16 = jnp.bfloat16
F32 = jnp.float32
MESH = pl.DeviceIdType.MESH
VM = pl.BlockSpec(memory_space=pltpu.VMEM)

HBM = pl.BlockSpec(memory_space=pltpu.HBM)

P_SENT = (240, 136, 264)
W_SENT = (320, 208, 384, 384, 384)
A_ROWS = (528, 384, 384, 384)
R_SENT = (528, 384, 64)


def fold(v, width=128):
    acc = v[:, :width]
    for k in range(1, v.shape[1] // width):
        acc = acc + v[:, k * width:(k + 1) * width]
    return acc


def fold_rows(v):
    return jnp.sum(v.reshape(v.shape[0] // 8, 8, v.shape[1]), axis=0)


def lane_total(v):
    s = jnp.sum(jnp.sum(v, axis=0, keepdims=True), axis=1, keepdims=True)
    lane = lax.broadcasted_iota(jnp.int32, (1, 128), 1)
    return jnp.where(lane == 0, jnp.broadcast_to(s, (1, 128)), 0.0)


def column(row_vec):
    return jnp.broadcast_to(row_vec, (128, row_vec.shape[1])).T


def fused(nc, nr, sizes,
          wg, wu, wd, xn, xa, dg, du, dd, rg, ru, rd, cg, cu, cd, hyper,
          gg, gu, gd, dxn, dxa_early, dxa_late, r_out, c_out, rs_out, cc_out,
          xn_v, dd_v, dy_v, p_v, pin_v, wb_v, win_v, dxa_v, dxn_v,
          rg_v, ru_v, rd_v, cg_v, cu_v, cd_v, hyp,
          r_mine, r_peer, c_all, s_all, wsq, wsq_d, rr, cc, racc, cacc, sacc,
          loc, dsem, qsem, psem, wsem, asem, rsem, csem, ssem):
    col = lax.axis_index('col')
    row = lax.axis_index('row')
    me = col * nr + row
    d_model, d_ff = sizes
    nb = dg.shape[0] // STEPS
    mb = wd.shape[0] // STEPS
    quarter = dd.shape[0] // nr
    others = [(dc, dr) for dc in range(nc) for dr in range(nr) if (dc, dr) != (0, 0)]

    c_all[row] = jnp.zeros(c_all.shape[1:], F32)
    s_all[me] = jnp.zeros(s_all.shape[1:], F32)

    barrier = pltpu.get_barrier_semaphore()
    for dc, dr in others:
        pl.semaphore_signal(barrier, 1, device_id=(lax.rem(col + dc, nc), lax.rem(row + dr, nr)), device_id_type=MESH)

    loads = [pltpu.make_async_copy(a, b, loc.at[k]) for k, (a, b) in enumerate((
        (xn, xn_v), (dd, dd_v), (rg, rg_v), (ru, ru_v), (rd, rd_v), (cg, cg_v), (cu, cu_v), (cd, cd_v), (hyper, hyp)))]
    for load in loads:
        load.start()
    pl.semaphore_wait(barrier, len(others))

    def remote(src, dst, sems, k, target):
        return pltpu.make_async_remote_copy(src_ref=src, dst_ref=dst, send_sem=sems.at[0, k], recv_sem=sems.at[1, k],
                                            device_id=target, device_id_type=MESH)

    def ranged(src, dst, sems, counts):
        copies, at = [], 0
        for k, n in enumerate(counts):
            copies.append(remote(src.at[pl.ds(at, n)], dst.at[pl.ds(at, n)], sems, k, across))
            at += n
        return copies

    across = (1 - col, row)
    chip = (col, lax.rem(row + 2, nr))
    core = (col, row + 1 - 2 * lax.rem(row, 2))
    rows_of = lambda r: pl.ds(pl.multiple_of(r * quarter, quarter), quarter)
    dy_copy = remote(dd.at[rows_of(row)], dy_v.at[rows_of(row)], dsem, 0, across)
    p_copies = ranged(p_v, pin_v, psem, P_SENT)
    w_copies = ranged(wb_v, win_v, wsem, W_SENT)
    a_copies = ranged(dxa_v, dxa_v, asem, R_SENT)

    @pl.when(col == 1)
    def _():
        dy_copy.start()

    p_v[...] = jnp.zeros_like(p_v)
    wsq[...] = jnp.zeros_like(wsq)
    wsq_d[...] = jnp.zeros_like(wsq_d)

    def part_body(wg_b, wu_b, dg_b, du_b):
        for k, (w_b, d_b) in enumerate(((wg_b, dg_b), (wu_b, du_b))):
            w = w_b[...]
            wsq[pl.ds(8 * k, 8), :] += fold_rows(w * w)
            p_v[...] += lax.dot_general(w.astype(BF16), d_b[...], (((0,), (0,)), ((), ())), preferred_element_type=F32)

    by_n = lambda width: pl.BlockSpec((nb, width), lambda k: (k, 0))
    by_m = lambda width: pl.BlockSpec((mb, width), lambda k: (k, 0))
    pltpu.emit_pipeline(part_body, grid=(STEPS,), in_specs=[by_n(wg.shape[1])] * 2 + [by_n(dg.shape[1])] * 2)(wg, wu, dg, du)

    @pl.when(col == 0)
    def _():
        p_copies[0].start()

    def cast_body(w_b):
        w = w_b[...]
        wsq_d[...] += fold_rows(w * w)
        wb_v[pl.ds(pl.multiple_of(pl.program_id(0) * mb, mb), mb), :] = w.astype(BF16)

    pltpu.emit_pipeline(cast_body, grid=(STEPS,), in_specs=[
        pl.BlockSpec((mb, wd.shape[1]), lambda k: (k, 0), pipeline_mode=pl.Buffered(4))])(wd)

    @pl.when(col == 1)
    def _():
        w_copies[0].start()

    q_far = remote(dy_v.at[rows_of(row)], dy_v.at[rows_of(row)], qsem, 0, chip)
    q_near = remote(dy_v.at[rows_of(row)], dy_v.at[rows_of(row)], qsem, 1, core)
    q_both = remote(dy_v.at[rows_of(chip[1])], dy_v.at[rows_of(chip[1])], qsem, 2, core)

    @pl.when(col == 0)
    def _():
        dy_copy.wait_recv()
        q_far.start()
        q_near.start()

    for load in loads:
        load.wait()
    r_mine[...] = jnp.zeros_like(r_mine)
    racc[...] = jnp.zeros_like(racc)
    cacc[...] = jnp.zeros_like(cacc)

    def grad_body(dg_b, du_b, xa_b, gg_b, gu_b, gd_b):
        k = pl.program_id(0)
        for t, (d_b, g_b) in enumerate(((dg_b, gg_b), (du_b, gu_b))):
            g = jnp.dot(d_b[...], xn_v[...], preferred_element_type=F32)
            g_b[...] = g
            q = g * g + EPS_ONE
            racc[pl.ds(8 * t, 8), :] += fold_rows(q)
            c_all[row, pl.ds(7 * t + k, 1), :] = jnp.sum(fold(q).T, axis=0, keepdims=True)
        g = jnp.dot(xa_b[...], dd_v[...], preferred_element_type=F32)
        gd_b[...] = g
        q = g * g + EPS_ONE
        cacc[...] += fold_rows(q)
        r_mine[pl.ds(8 + k, 1), pl.ds(0, 240)] = jnp.sum(fold(q).T, axis=0, keepdims=True)

    pltpu.emit_pipeline(grad_body, grid=(STEPS,), in_specs=[by_n(dg.shape[1])] * 2 + [by_m(xa.shape[1])],
                        out_specs=[by_n(gg.shape[1])] * 2 + [by_m(gd.shape[1])])(dg, du, xa, gg, gu, gd)

    for t in range(2):
        r_mine[t:t + 1, :] = jnp.sum(racc[8 * t:8 * t + 8, :], axis=0, keepdims=True)
    c_down = jnp.sum(cacc[...], axis=0, keepdims=True)
    for k in range(5):
        c_all[row, 14 + k:15 + k, 0:256] = c_down[:, 256 * k:256 * (k + 1)]

    r_copy = remote(r_mine, r_peer, rsem, 0, across)
    r_copy.start()
    c_copies = [pltpu.make_async_remote_copy(
        src_ref=c_all.at[row], dst_ref=c_all.at[row], send_sem=csem.at[0, d], recv_sem=csem.at[1, row],
        device_id=(col, lax.rem(row + d, nr)), device_id_type=MESH) for d in range(1, nr)]
    for c in c_copies:
        c.start()

    @pl.when(col == 0)
    def _():
        p_copies[1].start()
        q_far.wait_recv()
        q_both.start()

    @pl.when(col == 1)
    def _():
        w_copies[1].start()

    beta = hyp[0]
    rr[...] = jnp.ones_like(rr)
    rr[0:1, :] = rg_v[...].reshape(1, -1)
    rr[1:2, :] = ru_v[...].reshape(1, -1)
    r_old, g_old, u_old, d_old = [v[...].reshape(1, -1) for v in (rd_v, cg_v, cu_v, cd_v)]
    for k in range(STEPS):
        cc[k:k + 1, :] = g_old[:, nb * k:nb * (k + 1)]
        cc[7 + k:8 + k, :] = u_old[:, nb * k:nb * (k + 1)]
        rr[8 + k:9 + k, 0:mb] = r_old[:, mb * k:mb * (k + 1)]
    for k in range(5):
        cc[14 + k:15 + k, 0:256] = d_old[:, 256 * k:256 * (k + 1)]
        cc[14 + k:15 + k, 256:480] = jnp.ones((1, 224), F32)
    cc[19:24, :] = jnp.ones((5, 480), F32)

    r_copy.wait()
    for d in range(1, nr):
        c_copies[d - 1].wait_send()
        s = lax.rem(row + d, nr)
        pltpu.make_async_remote_copy(src_ref=c_all.at[s], dst_ref=c_all.at[s], send_sem=csem.at[0, d], recv_sem=csem.at[1, s],
                                     device_id=(col, s), device_id_type=MESH).wait_recv()

    line = lax.broadcasted_iota(jnp.int32, rr.shape, 0)
    r_new = beta * rr[...] + (1.0 - beta) * ((r_mine[...] + r_peer[...]) / jnp.where(line < 8, float(d_ff), float(d_model)))
    line = lax.broadcasted_iota(jnp.int32, cc.shape, 0)
    c_sum = (c_all[0] + c_all[1]) + (c_all[2] + c_all[3])
    c_new = beta * cc[...] + (1.0 - beta) * (c_sum / jnp.where(line < 14, float(d_model), float(d_ff)))
    r_out[...] = r_new
    c_out[...] = c_new
    rr[...] = lax.rsqrt(r_new)
    cc[...] = lax.rsqrt(c_new)
    cc_out[...] = cc[...]

    sacc[...] = jnp.zeros_like(sacc)

    def square_body(gg_b, gu_b, gd_b):
        k = pl.program_id(0)
        for t, g_b in enumerate((gg_b, gu_b)):
            u = g_b[...] * rr[t:t + 1, :]
            s = fold(u * u)
            c = column(cc[pl.ds(7 * t + k, 1), :])
            sacc[pl.ds(8 * t, 8), :] += fold_rows(s * (c * c))
        c_row = jnp.concatenate([cc[14 + j:15 + j, 0:256] for j in range(5)], axis=1)
        u = gd_b[...] * c_row
        s = fold(u * u)
        r = column(rr[pl.ds(8 + k, 1), :])[0:mb]
        sacc[16:24, :] += fold_rows(s * (r * r))

    pltpu.emit_pipeline(square_body, grid=(STEPS,), in_specs=[by_n(gg.shape[1])] * 2 + [by_m(gd.shape[1])])(gg, gu, gd)

    for t in range(3):
        s_all[me, t:t + 1, :] = jnp.sum(sacc[8 * t:8 * t + 8, :], axis=0, keepdims=True)
    for t in range(2):
        s_all[me, 3 + t:4 + t, :] = jnp.sum(fold(wsq[8 * t:8 * t + 8, :]), axis=0, keepdims=True)
        s_all[me, 6 + t:7 + t, :] = lane_total(r_new[t:t + 1, :])
    s_all[me, 5:6, :] = jnp.sum(fold(wsq_d[...]), axis=0, keepdims=True)
    s_all[me, 8:9, :] = lane_total(r_new[8:15, 0:mb])
    s_copies = []
    for j, (dc, dr) in enumerate(others):
        s_copies.append(pltpu.make_async_remote_copy(
            src_ref=s_all.at[me], dst_ref=s_all.at[me], send_sem=ssem.at[0, j], recv_sem=ssem.at[1, me],
            device_id=(lax.rem(col + dc, nc), lax.rem(row + dr, nr)), device_id_type=MESH))
    for s in s_copies:
        s.start()

    @pl.when(col == 0)
    def _():
        p_copies[2].start()

    @pl.when(col == 1)
    def _():
        for w in w_copies[2:]:
            w.start()

    for j, (dc, dr) in enumerate(others):
        tc, tr = lax.rem(col + dc, nc), lax.rem(row + dr, nr)
        s_copies[j].wait_send()
        him = tc * nr + tr
        pltpu.make_async_remote_copy(src_ref=s_all.at[him], dst_ref=s_all.at[him], send_sem=ssem.at[0, j],
                                     recv_sem=ssem.at[1, him], device_id=(tc, tr), device_id_type=MESH).wait_recv()
    total = s_all[0]
    for j in range(1, nc * nr):
        total = total + s_all[j]
    sums = jnp.sum(total, axis=1, keepdims=True)
    scales = []
    for t, (m, n) in enumerate(((d_model, d_ff), (d_model, d_ff), (d_ff, d_model))):
        r_mean = sums[6 + t:7 + t] / float(m * nc)
        rms_u = jnp.sqrt(sums[t:t + 1] * r_mean / float(m * n))
        step = hyp[1] * jnp.maximum(EPS_TWO, jnp.sqrt(sums[3 + t:4 + t] / float(m * n)))
        scales.append(step * jnp.sqrt(r_mean) / jnp.maximum(1.0, rms_u / hyp[2]))
    rs_out[...] = rr[...]
    rs_out[0:1, :] = rr[0:1, :] * scales[0]
    rs_out[1:2, :] = rr[1:2, :] * scales[1]
    rs_out[8:16, :] = rr[8:16, :] * scales[2]

    early = sum(R_SENT)
    total_m = wd.shape[0]
    save_early = pltpu.make_async_copy(dxa_v.at[pl.ds(0, early)], dxa_early, loc.at[9])
    save_late = pltpu.make_async_copy(dxa_v.at[pl.ds(early, total_m - early)], dxa_late, loc.at[10])
    save_n = pltpu.make_async_copy(dxn_v, dxn, loc.at[11])

    @pl.when(col == 0)
    def _():
        q_near.wait_recv()
        q_both.wait_recv()
        q_far.wait_send()
        q_near.wait_send()
        q_both.wait_send()
        w_copies[0].wait_recv()
        at = 0
        for k, n in enumerate(A_ROWS):
            w_copies[k + 1].wait_recv()
            dims = (((1,), (1,)), ((), ()))
            o = lax.dot_general(wb_v[at:at + n, :], dd_v[...], dims, preferred_element_type=F32)
            o = o + lax.dot_general(win_v[at:at + n, :], dy_v[...], dims, preferred_element_type=F32)
            dxa_v[at:at + n, :] = o.astype(BF16)
            at += n
            if k < len(R_SENT):
                a_copies[k].start()
        save_early.start()
        save_late.start()
        for p in p_copies:
            p.wait_send()
        for a in a_copies:
            a.wait_send()
        save_early.wait()
        save_late.wait()

    @pl.when(col == 1)
    def _():
        for p in p_copies:
            p.wait_recv()
        for j in range(p_v.shape[0] // 128):
            rows = slice(128 * j, 128 * (j + 1))
            dxn_v[:, rows] = (p_v[rows, :] + pin_v[rows, :]).T.astype(BF16)
        save_n.start()
        dy_copy.wait_send()
        for w in w_copies:
            w.wait_send()
        for a in a_copies:
            a.wait_recv()
        save_early.start()
        save_n.wait()
        save_early.wait()


def run_fused(nc, nr, sizes, wg, wu, wd, xn, xa, dg, du, dd, rg, ru, rd, cg, cu, cd, hyper):
    f32, b16 = (lambda *s: jax.ShapeDtypeStruct(s, F32)), (lambda *s: jax.ShapeDtypeStruct(s, BF16))
    n, i = wg.shape
    m, h = wd.shape
    t = dd.shape[0]
    early = sum(R_SENT)
    dma = lambda *s: pltpu.SemaphoreType.DMA(s)
    vf = lambda *s: pltpu.VMEM(s, F32)
    vb = lambda *s: pltpu.VMEM(s, BF16)
    return pl.pallas_call(
        functools.partial(fused, nc, nr, sizes),
        out_shape=(f32(n, i), f32(n, i), f32(m, h), b16(t, i), b16(early, t), b16(m - early, t),
                   f32(16, 640), f32(24, 480), f32(16, 640), f32(24, 480)),
        in_specs=[HBM] * 15,
        out_specs=[HBM] * 6 + [VM] * 4,
        scratch_shapes=[
            vb(*xn.shape), vb(t, h), vb(t, h), vf(i, t), vf(i, t), vb(m, h), vb(m, h), vb(m, t), vb(t, i),
            vf(i), vf(i), vf(m), vf(n), vf(n), vf(h), pltpu.SMEM((3,), F32),
            vf(16, 640), vf(16, 640), vf(nr, 24, 480), vf(nc * nr, 16, 128), vf(16, i), vf(8, h),
            vf(16, 640), vf(24, 480), vf(16, i), vf(8, h), vf(24, 128),
            dma(12), dma(2, 1), dma(2, 3), dma(2, len(P_SENT)), dma(2, len(W_SENT)), dma(2, len(R_SENT)), dma(2, 1),
            dma(2, nr), dma(2, nc * nr)],
        compiler_params=pltpu.CompilerParams(collective_id=0, has_side_effects=True, vmem_limit_bytes=60 * 1024 * 1024),
        cost_estimate=pl.CostEstimate(flops=22_000_000_000, bytes_accessed=150_000_000, transcendentals=0),
        name="fused",
    )(wg, wu, wd, xn, xa, dg, du, dd, rg, ru, rd, cg, cu, cd, hyper)


def step_kernel(r_new, c_new, rs, cc, wg, wu, wd, gg, gu, gd, ng, nu, nd, rgo, ruo, rdo, cgo, cuo, cdo):
    k = pl.program_id(0)
    nb, mb = wg.shape[0], wd.shape[0]

    @pl.when(k == 0)
    def _():
        rgo[...] = r_new[0:1, :].reshape(-1)
        ruo[...] = r_new[1:2, :].reshape(-1)
        rdo[...] = jnp.concatenate([r_new[8 + j:9 + j, 0:mb] for j in range(STEPS)], axis=1).reshape(-1)
        cgo[...] = jnp.concatenate([c_new[j:j + 1, :] for j in range(STEPS)], axis=1).reshape(-1)
        cuo[...] = jnp.concatenate([c_new[7 + j:8 + j, :] for j in range(STEPS)], axis=1).reshape(-1)
        cdo[...] = jnp.concatenate([c_new[14 + j:15 + j, 0:256] for j in range(5)], axis=1).reshape(-1)

    for t, (w, g, o) in enumerate(((wg, gg, ng), (wu, gu, nu))):
        c = column(cc[pl.ds(7 * t + k, 1), :])
        for j in range(w.shape[1] // 128):
            lanes = slice(128 * j, 128 * (j + 1))
            o[:, lanes] = w[:, lanes] - g[:, lanes] * rs[t:t + 1, lanes] * c
    r = column(rs[pl.ds(8 + k, 1), :])[0:mb]
    for j in range(wd.shape[1] // 128):
        lanes = slice(128 * j, 128 * (j + 1))
        c = cc[14 + j // 2:15 + j // 2, 128 * (j % 2):128 * (j % 2 + 1)]
        nd[:, lanes] = wd[:, lanes] - gd[:, lanes] * c * r


def run_step(r_new, c_new, rs, cc, wg, wu, wd, gg, gu, gd):
    f32 = lambda *s: jax.ShapeDtypeStruct(s, F32)
    n, i = wg.shape
    m, h = wd.shape
    whole = lambda a: pl.BlockSpec(a.shape, lambda k: (0, 0))
    flat = lambda s: pl.BlockSpec((s,), lambda k: (0,))
    by_n = pl.BlockSpec((n // STEPS, i), lambda k: (k, 0))
    by_m = pl.BlockSpec((m // STEPS, h), lambda k: (k, 0))
    return pl.pallas_call(
        step_kernel, grid=(STEPS,),
        out_shape=(f32(n, i), f32(n, i), f32(m, h), f32(i), f32(i), f32(m), f32(n), f32(n), f32(h)),
        in_specs=[whole(a) for a in (r_new, c_new, rs, cc)] + [by_n, by_n, by_m] * 2,
        out_specs=[by_n, by_n, by_m] + [flat(s) for s in (i, i, m, n, n, h)],
        compiler_params=pltpu.CompilerParams(vmem_limit_bytes=48 * 1024 * 1024),
        cost_estimate=pl.CostEstimate(flops=20_000_000_000, bytes_accessed=78_000_000, transcendentals=0),
        name="step",
    )(r_new, c_new, rs, cc, wg, wu, wd, gg, gu, gd)


TO_0 = [(1, 0)]
TO_1 = [(0, 1)]


def solution(mesh):
    row_size = mesh.shape['row']
    col_size = mesh.shape['col']
    weight_spec = P('row', 'col')
    act_spec = P(None, 'row')
    grad_spec = P(None, 'col')
    in_specs = (weight_spec,) * 3 + (act_spec, act_spec) + (grad_spec,) * 3 + (P('row'), P('col')) * 3 + (P(),)
    out_specs = (weight_spec,) * 3 + (P('row'), P('col')) * 3 + (act_spec, act_spec)

    def body(w_gate, w_up, w_down, x_norm, x_act, dy_gate, dy_up, dy_down, r_gate, c_gate, r_up, c_up, r_down, c_down, hyper_params):
        d_model = w_gate.shape[0] * row_size
        d_ff = w_gate.shape[1] * col_size
        col = lax.axis_index('col')
        gg, gu, gd, dxn, early, late, r_new, c_new, rs, cc = run_fused(
            col_size, row_size, (d_model, d_ff),
            w_gate.T, w_up.T, w_down, x_norm, x_act.T, dy_gate.T, dy_up.T, dy_down,
            r_gate, r_up, r_down, c_gate, c_up, c_down, hyper_params)
        late_in = lax.ppermute(late, 'col', TO_1)
        dxn_in = lax.ppermute(dxn, 'col', TO_0)
        ng, nu, nd, rgo, ruo, rdo, cgo, cuo, cdo = run_step(r_new, c_new, rs, cc, w_gate.T, w_up.T, w_down, gg, gu, gd)
        dx_norm = jnp.where(col == 1, dxn, dxn_in)
        dx_act = jnp.concatenate([early, jnp.where(col == 0, late, late_in)], axis=0).T
        return (ng.T, nu.T, nd, rgo, cgo, ruo, cuo, rdo, cdo, dx_norm, dx_act)

    return jax.shard_map(body, mesh=mesh, in_specs=in_specs, out_specs=out_specs, check_vma=False)
```

```python
import functools

import jax
import jax.numpy as jnp
from jax import lax
from jax.experimental import pallas as pl
from jax.experimental.pallas import tpu as pltpu
from jax.sharding import PartitionSpec as P

EPS_ONE = 1e-30
EPS_TWO = 1e-3
STEPS = 7
BF16 = jnp.bfloat16
F32 = jnp.float32
MESH = pl.DeviceIdType.MESH
VM = pl.BlockSpec(memory_space=pltpu.VMEM)

HBM = pl.BlockSpec(memory_space=pltpu.HBM)

P_SENT = (320, 184, 136)
W_SENT = (480, 288, 384, 384, 144)
A_ROWS = (768, 384, 384, 144)
R_SENT = (768, 240)
N_SENT = 224


def fold(v, width=128):
    acc = v[:, :width]
    for k in range(1, v.shape[1] // width):
        acc = acc + v[:, k * width:(k + 1) * width]
    return acc


def fold_rows(v):
    return jnp.sum(v.reshape(v.shape[0] // 8, 8, v.shape[1]), axis=0)


def lane_total(v):
    s = jnp.sum(jnp.sum(v, axis=0, keepdims=True), axis=1, keepdims=True)
    lane = lax.broadcasted_iota(jnp.int32, (1, 128), 1)
    return jnp.where(lane == 0, jnp.broadcast_to(s, (1, 128)), 0.0)


def column(row_vec):
    return jnp.broadcast_to(row_vec, (128, row_vec.shape[1])).T


def fused(nc, nr, sizes,
          wg, wu, wd, xn, xa, dg, du, dd, rg, ru, rd, cg, cu, cd, hyper,
          gg, gu, gd, dxn_early, dxn_late, dxa_early, dxa_late, r_out, c_out, rs_out, cc_out,
          xn_v, dd_v, dy_v, p_v, pin_v, wb_v, win_v, dxa_v, dxn_v,
          rg_v, ru_v, rd_v, cg_v, cu_v, cd_v, hyp,
          r_mine, r_peer, c_all, s_all, wsq, wsq_d, rr, cc, racc, cacc, sacc,
          loc, dsem, qsem, psem, wsem, asem, nsem, rsem, csem, ssem):
    col = lax.axis_index('col')
    row = lax.axis_index('row')
    me = col * nr + row
    d_model, d_ff = sizes
    nb = dg.shape[0] // STEPS
    mb = wd.shape[0] // STEPS
    quarter = dd.shape[0] // nr
    others = [(dc, dr) for dc in range(nc) for dr in range(nr) if (dc, dr) != (0, 0)]

    c_all[row] = jnp.zeros(c_all.shape[1:], F32)
    s_all[me] = jnp.zeros(s_all.shape[1:], F32)

    barrier = pltpu.get_barrier_semaphore()
    for dc, dr in others:
        pl.semaphore_signal(barrier, 1, device_id=(lax.rem(col + dc, nc), lax.rem(row + dr, nr)), device_id_type=MESH)

    loads = [pltpu.make_async_copy(a, b, loc.at[k]) for k, (a, b) in enumerate((
        (xn, xn_v), (dd, dd_v), (rg, rg_v), (ru, ru_v), (rd, rd_v), (cg, cg_v), (cu, cu_v), (cd, cd_v), (hyper, hyp)))]
    for load in loads:
        load.start()
    pl.semaphore_wait(barrier, len(others))

    def remote(src, dst, sems, k, target):
        return pltpu.make_async_remote_copy(src_ref=src, dst_ref=dst, send_sem=sems.at[0, k], recv_sem=sems.at[1, k],
                                            device_id=target, device_id_type=MESH)

    def ranged(src, dst, sems, counts):
        copies, at = [], 0
        for k, n in enumerate(counts):
            copies.append(remote(src.at[pl.ds(at, n)], dst.at[pl.ds(at, n)], sems, k, across))
            at += n
        return copies

    across = (1 - col, row)
    chip = (col, lax.rem(row + 2, nr))
    core = (col, row + 1 - 2 * lax.rem(row, 2))
    rows_of = lambda r: pl.ds(pl.multiple_of(r * quarter, quarter), quarter)
    dy_copy = remote(dd.at[rows_of(row)], dy_v.at[rows_of(row)], dsem, 0, across)
    p_copies = ranged(p_v, pin_v, psem, P_SENT)
    w_copies = ranged(wb_v, win_v, wsem, W_SENT)
    a_copies = ranged(dxa_v, dxa_v, asem, R_SENT)
    n_copy = ranged(dxn_v, dxn_v, nsem, (N_SENT,))[0]

    @pl.when(col == 1)
    def _():
        dy_copy.start()

    p_v[...] = jnp.zeros_like(p_v)
    wsq[...] = jnp.zeros_like(wsq)
    wsq_d[...] = jnp.zeros_like(wsq_d)

    def part_body(wg_b, wu_b, dg_b, du_b):
        for k, (w_b, d_b) in enumerate(((wg_b, dg_b), (wu_b, du_b))):
            w = w_b[...]
            wsq[pl.ds(8 * k, 8), :] += fold_rows(w * w)
            p_v[...] += lax.dot_general(w.astype(BF16), d_b[...], (((0,), (0,)), ((), ())), preferred_element_type=F32)

    by_n = lambda width: pl.BlockSpec((nb, width), lambda k: (k, 0))
    by_m = lambda width: pl.BlockSpec((mb, width), lambda k: (k, 0))
    pltpu.emit_pipeline(part_body, grid=(STEPS,), in_specs=[by_n(wg.shape[1])] * 2 + [by_n(dg.shape[1])] * 2)(wg, wu, dg, du)

    @pl.when(col == 0)
    def _():
        p_copies[0].start()

    first = W_SENT[0] // mb

    def cast_body(start, w_b):
        w = w_b[...]
        wsq_d[...] += fold_rows(w * w)
        wb_v[pl.ds(pl.multiple_of((start + pl.program_id(0)) * mb, mb), mb), :] = w.astype(BF16)

    def cast(start, count):
        pltpu.emit_pipeline(functools.partial(cast_body, start), grid=(count,), in_specs=[
            pl.BlockSpec((mb, wd.shape[1]), lambda k: (start + k, 0), pipeline_mode=pl.Buffered(4))])(wd)

    cast(0, first)

    @pl.when(col == 1)
    def _():
        w_copies[0].start()

    cast(first, STEPS - first)

    q_far = remote(dy_v.at[rows_of(row)], dy_v.at[rows_of(row)], qsem, 0, chip)
    q_near = remote(dy_v.at[rows_of(row)], dy_v.at[rows_of(row)], qsem, 1, core)
    q_both = remote(dy_v.at[rows_of(chip[1])], dy_v.at[rows_of(chip[1])], qsem, 2, core)

    @pl.when(col == 0)
    def _():
        dy_copy.wait_recv()
        q_far.start()
        q_near.start()

    for load in loads:
        load.wait()
    r_mine[...] = jnp.zeros_like(r_mine)
    racc[...] = jnp.zeros_like(racc)
    cacc[...] = jnp.zeros_like(cacc)

    def grad_body(dg_b, du_b, xa_b, gg_b, gu_b, gd_b):
        k = pl.program_id(0)
        for t, (d_b, g_b) in enumerate(((dg_b, gg_b), (du_b, gu_b))):
            g = jnp.dot(d_b[...], xn_v[...], preferred_element_type=F32)
            g_b[...] = g
            q = g * g + EPS_ONE
            racc[pl.ds(8 * t, 8), :] += fold_rows(q)
            c_all[row, pl.ds(7 * t + k, 1), :] = jnp.sum(fold(q).T, axis=0, keepdims=True)
        g = jnp.dot(xa_b[...], dd_v[...], preferred_element_type=F32)
        gd_b[...] = g
        q = g * g + EPS_ONE
        cacc[...] += fold_rows(q)
        r_mine[pl.ds(8 + k, 1), pl.ds(0, 240)] = jnp.sum(fold(q).T, axis=0, keepdims=True)

    pltpu.emit_pipeline(grad_body, grid=(STEPS,), in_specs=[by_n(dg.shape[1])] * 2 + [by_m(xa.shape[1])],
                        out_specs=[by_n(gg.shape[1])] * 2 + [by_m(gd.shape[1])])(dg, du, xa, gg, gu, gd)

    for t in range(2):
        r_mine[t:t + 1, :] = jnp.sum(racc[8 * t:8 * t + 8, :], axis=0, keepdims=True)
    c_down = jnp.sum(cacc[...], axis=0, keepdims=True)
    for k in range(5):
        c_all[row, 14 + k:15 + k, 0:256] = c_down[:, 256 * k:256 * (k + 1)]

    r_copy = remote(r_mine, r_peer, rsem, 0, across)
    r_copy.start()
    c_copies = [pltpu.make_async_remote_copy(
        src_ref=c_all.at[row], dst_ref=c_all.at[row], send_sem=csem.at[0, d], recv_sem=csem.at[1, row],
        device_id=(col, lax.rem(row + d, nr)), device_id_type=MESH) for d in range(1, nr)]
    for c in c_copies:
        c.start()

    @pl.when(col == 0)
    def _():
        p_copies[1].start()
        q_far.wait_recv()
        q_both.start()

    @pl.when(col == 1)
    def _():
        w_copies[1].start()

    beta = hyp[0]
    rr[...] = jnp.ones_like(rr)
    rr[0:1, :] = rg_v[...].reshape(1, -1)
    rr[1:2, :] = ru_v[...].reshape(1, -1)
    r_old, g_old, u_old, d_old = [v[...].reshape(1, -1) for v in (rd_v, cg_v, cu_v, cd_v)]
    for k in range(STEPS):
        cc[k:k + 1, :] = g_old[:, nb * k:nb * (k + 1)]
        cc[7 + k:8 + k, :] = u_old[:, nb * k:nb * (k + 1)]
        rr[8 + k:9 + k, 0:mb] = r_old[:, mb * k:mb * (k + 1)]
    for k in range(5):
        cc[14 + k:15 + k, 0:256] = d_old[:, 256 * k:256 * (k + 1)]
        cc[14 + k:15 + k, 256:480] = jnp.ones((1, 224), F32)
    cc[19:24, :] = jnp.ones((5, 480), F32)

    r_copy.wait()
    for d in range(1, nr):
        c_copies[d - 1].wait_send()
        s = lax.rem(row + d, nr)
        pltpu.make_async_remote_copy(src_ref=c_all.at[s], dst_ref=c_all.at[s], send_sem=csem.at[0, d], recv_sem=csem.at[1, s],
                                     device_id=(col, s), device_id_type=MESH).wait_recv()

    line = lax.broadcasted_iota(jnp.int32, rr.shape, 0)
    r_new = beta * rr[...] + (1.0 - beta) * ((r_mine[...] + r_peer[...]) / jnp.where(line < 8, float(d_ff), float(d_model)))
    line = lax.broadcasted_iota(jnp.int32, cc.shape, 0)
    c_sum = (c_all[0] + c_all[1]) + (c_all[2] + c_all[3])
    c_new = beta * cc[...] + (1.0 - beta) * (c_sum / jnp.where(line < 14, float(d_model), float(d_ff)))
    r_out[...] = r_new
    c_out[...] = c_new
    rr[...] = lax.rsqrt(r_new)
    cc[...] = lax.rsqrt(c_new)
    cc_out[...] = cc[...]

    sacc[...] = jnp.zeros_like(sacc)

    def square_body(gg_b, gu_b, gd_b):
        k = pl.program_id(0)
        for t, g_b in enumerate((gg_b, gu_b)):
            u = g_b[...] * rr[t:t + 1, :]
            s = fold(u * u)
            c = column(cc[pl.ds(7 * t + k, 1), :])
            sacc[pl.ds(8 * t, 8), :] += fold_rows(s * (c * c))
        c_row = jnp.concatenate([cc[14 + j:15 + j, 0:256] for j in range(5)], axis=1)
        u = gd_b[...] * c_row
        s = fold(u * u)
        r = column(rr[pl.ds(8 + k, 1), :])[0:mb]
        sacc[16:24, :] += fold_rows(s * (r * r))

    pltpu.emit_pipeline(square_body, grid=(STEPS,), in_specs=[by_n(gg.shape[1])] * 2 + [by_m(gd.shape[1])])(gg, gu, gd)

    for t in range(3):
        s_all[me, t:t + 1, :] = jnp.sum(sacc[8 * t:8 * t + 8, :], axis=0, keepdims=True)
    for t in range(2):
        s_all[me, 3 + t:4 + t, :] = jnp.sum(fold(wsq[8 * t:8 * t + 8, :]), axis=0, keepdims=True)
        s_all[me, 6 + t:7 + t, :] = lane_total(r_new[t:t + 1, :])
    s_all[me, 5:6, :] = jnp.sum(fold(wsq_d[...]), axis=0, keepdims=True)
    s_all[me, 8:9, :] = lane_total(r_new[8:15, 0:mb])
    s_copies = []
    for j, (dc, dr) in enumerate(others):
        s_copies.append(pltpu.make_async_remote_copy(
            src_ref=s_all.at[me], dst_ref=s_all.at[me], send_sem=ssem.at[0, j], recv_sem=ssem.at[1, me],
            device_id=(lax.rem(col + dc, nc), lax.rem(row + dr, nr)), device_id_type=MESH))
    for s in s_copies:
        s.start()

    @pl.when(col == 0)
    def _():
        p_copies[2].start()

    @pl.when(col == 1)
    def _():
        for w in w_copies[2:]:
            w.start()

    for j, (dc, dr) in enumerate(others):
        tc, tr = lax.rem(col + dc, nc), lax.rem(row + dr, nr)
        s_copies[j].wait_send()
        him = tc * nr + tr
        pltpu.make_async_remote_copy(src_ref=s_all.at[him], dst_ref=s_all.at[him], send_sem=ssem.at[0, j],
                                     recv_sem=ssem.at[1, him], device_id=(tc, tr), device_id_type=MESH).wait_recv()
    total = s_all[0]
    for j in range(1, nc * nr):
        total = total + s_all[j]
    sums = jnp.sum(total, axis=1, keepdims=True)
    scales = []
    for t, (m, n) in enumerate(((d_model, d_ff), (d_model, d_ff), (d_ff, d_model))):
        r_mean = sums[6 + t:7 + t] / float(m * nc)
        rms_u = jnp.sqrt(sums[t:t + 1] * r_mean / float(m * n))
        step = hyp[1] * jnp.maximum(EPS_TWO, jnp.sqrt(sums[3 + t:4 + t] / float(m * n)))
        scales.append(step * jnp.sqrt(r_mean) / jnp.maximum(1.0, rms_u / hyp[2]))
    rs_out[...] = rr[...]
    rs_out[0:1, :] = rr[0:1, :] * scales[0]
    rs_out[1:2, :] = rr[1:2, :] * scales[1]
    rs_out[8:16, :] = rr[8:16, :] * scales[2]

    early = sum(R_SENT)
    total_m = wd.shape[0]
    save_early = pltpu.make_async_copy(dxa_v.at[pl.ds(0, early)], dxa_early, loc.at[9])
    save_late = pltpu.make_async_copy(dxa_v.at[pl.ds(early, total_m - early)], dxa_late, loc.at[10])
    save_n_early = pltpu.make_async_copy(dxn_v.at[pl.ds(0, N_SENT)], dxn_early, loc.at[11])
    save_n_late = pltpu.make_async_copy(dxn_v.at[pl.ds(N_SENT, dxn_v.shape[0] - N_SENT)], dxn_late, loc.at[12])

    @pl.when(col == 0)
    def _():
        q_near.wait_recv()
        q_both.wait_recv()
        q_far.wait_send()
        q_near.wait_send()
        q_both.wait_send()
        w_copies[0].wait_recv()
        at = 0
        for k, n in enumerate(A_ROWS):
            w_copies[k + 1].wait_recv()
            dims = (((1,), (1,)), ((), ()))
            o = lax.dot_general(wb_v[at:at + n, :], dd_v[...], dims, preferred_element_type=F32)
            o = o + lax.dot_general(win_v[at:at + n, :], dy_v[...], dims, preferred_element_type=F32)
            dxa_v[at:at + n, :] = o.astype(BF16)
            at += n
            if k < len(R_SENT):
                a_copies[k].start()
        save_early.start()
        save_late.start()
        for p in p_copies:
            p.wait_send()
        n_copy.wait_recv()
        save_n_early.start()
        for a in a_copies:
            a.wait_send()
        save_n_early.wait()
        save_early.wait()
        save_late.wait()

    @pl.when(col == 1)
    def _():
        for p in p_copies:
            p.wait_recv()
        for j in range(p_v.shape[0] // 128):
            rows = slice(128 * j, 128 * (j + 1))
            dxn_v[:, rows] = (p_v[rows, :] + pin_v[rows, :]).T.astype(BF16)
        n_copy.start()
        save_n_early.start()
        save_n_late.start()
        dy_copy.wait_send()
        for w in w_copies:
            w.wait_send()
        for a in a_copies:
            a.wait_recv()
        save_early.start()
        n_copy.wait_send()
        save_n_early.wait()
        save_n_late.wait()
        save_early.wait()


def run_fused(nc, nr, sizes, wg, wu, wd, xn, xa, dg, du, dd, rg, ru, rd, cg, cu, cd, hyper):
    f32, b16 = (lambda *s: jax.ShapeDtypeStruct(s, F32)), (lambda *s: jax.ShapeDtypeStruct(s, BF16))
    n, i = wg.shape
    m, h = wd.shape
    t = dd.shape[0]
    early = sum(R_SENT)
    dma = lambda *s: pltpu.SemaphoreType.DMA(s)
    vf = lambda *s: pltpu.VMEM(s, F32)
    vb = lambda *s: pltpu.VMEM(s, BF16)
    return pl.pallas_call(
        functools.partial(fused, nc, nr, sizes),
        out_shape=(f32(n, i), f32(n, i), f32(m, h), b16(N_SENT, i), b16(t - N_SENT, i), b16(early, t), b16(m - early, t),
                   f32(16, 640), f32(24, 480), f32(16, 640), f32(24, 480)),
        in_specs=[HBM] * 15,
        out_specs=[HBM] * 7 + [VM] * 4,
        scratch_shapes=[
            vb(*xn.shape), vb(t, h), vb(t, h), vf(i, t), vf(i, t), vb(m, h), vb(m, h), vb(m, t), vb(t, i),
            vf(i), vf(i), vf(m), vf(n), vf(n), vf(h), pltpu.SMEM((3,), F32),
            vf(16, 640), vf(16, 640), vf(nr, 24, 480), vf(nc * nr, 16, 128), vf(16, i), vf(8, h),
            vf(16, 640), vf(24, 480), vf(16, i), vf(8, h), vf(24, 128),
            dma(13), dma(2, 1), dma(2, 3), dma(2, len(P_SENT)), dma(2, len(W_SENT)), dma(2, len(R_SENT)), dma(2, 1), dma(2, 1),
            dma(2, nr), dma(2, nc * nr)],
        compiler_params=pltpu.CompilerParams(collective_id=0, has_side_effects=True, vmem_limit_bytes=60 * 1024 * 1024),
        cost_estimate=pl.CostEstimate(flops=22_000_000_000, bytes_accessed=150_000_000, transcendentals=0),
        name="fused",
    )(wg, wu, wd, xn, xa, dg, du, dd, rg, ru, rd, cg, cu, cd, hyper)


def step_kernel(r_hbm, c_hbm, rs_hbm, cc_hbm, wg, wu, wd, gg, gu, gd, a_in, n_in, ng, nu, nd, a_out, n_out,
                rgo, ruo, rdo, cgo, cuo, cdo, r_new, c_new, rs, cc, a_v, n_v, sem):
    k = pl.program_id(0)
    nb, mb = wg.shape[0], wd.shape[0]
    pairs = ((r_hbm, r_new), (c_hbm, c_new), (rs_hbm, rs), (cc_hbm, cc), (a_in, a_v), (n_in, n_v),
             (a_v, a_out.at[pl.ds(0, a_v.shape[0])]), (n_v, n_out.at[pl.ds(0, n_v.shape[0])]))
    copies = [pltpu.make_async_copy(a, b, sem.at[j]) for j, (a, b) in enumerate(pairs)]

    @pl.when(k == 0)
    def _():
        for c in copies[:6]:
            c.start()
        for c in copies[:4]:
            c.wait()
        rgo[...] = r_new[0:1, :].reshape(-1)
        ruo[...] = r_new[1:2, :].reshape(-1)
        rdo[...] = jnp.concatenate([r_new[8 + j:9 + j, 0:mb] for j in range(STEPS)], axis=1).reshape(-1)
        cgo[...] = jnp.concatenate([c_new[j:j + 1, :] for j in range(STEPS)], axis=1).reshape(-1)
        cuo[...] = jnp.concatenate([c_new[7 + j:8 + j, :] for j in range(STEPS)], axis=1).reshape(-1)
        cdo[...] = jnp.concatenate([c_new[14 + j:15 + j, 0:256] for j in range(5)], axis=1).reshape(-1)

    @pl.when(k == 1)
    def _():
        for c in copies[4:6]:
            c.wait()
        for c in copies[6:]:
            c.start()

    @pl.when(k == STEPS - 1)
    def _():
        for c in copies[6:]:
            c.wait()

    for t, (w, g, o) in enumerate(((wg, gg, ng), (wu, gu, nu))):
        c = column(cc[pl.ds(7 * t + k, 1), :])
        for j in range(w.shape[1] // 128):
            lanes = slice(128 * j, 128 * (j + 1))
            o[:, lanes] = w[:, lanes] - g[:, lanes] * rs[t:t + 1, lanes] * c
    r = column(rs[pl.ds(8 + k, 1), :])[0:mb]
    for j in range(wd.shape[1] // 128):
        lanes = slice(128 * j, 128 * (j + 1))
        c = cc[14 + j // 2:15 + j // 2, 128 * (j % 2):128 * (j % 2 + 1)]
        nd[:, lanes] = wd[:, lanes] - gd[:, lanes] * c * r


def run_step(tokens, r_new, c_new, rs, cc, wg, wu, wd, gg, gu, gd, a_early, n_early):
    f32 = lambda *s: jax.ShapeDtypeStruct(s, F32)
    n, i = wg.shape
    m, h = wd.shape
    flat = lambda s: pl.BlockSpec((s,), lambda k: (0,))
    by_n = pl.BlockSpec((n // STEPS, i), lambda k: (k, 0))
    by_m = pl.BlockSpec((m // STEPS, h), lambda k: (k, 0))
    b16 = lambda *s: jax.ShapeDtypeStruct(s, BF16)
    return pl.pallas_call(
        step_kernel, grid=(STEPS,),
        out_shape=(f32(n, i), f32(n, i), f32(m, h), b16(m, tokens), b16(tokens, i), f32(i), f32(i), f32(m), f32(n), f32(n), f32(h)),
        in_specs=[HBM] * 4 + [by_n, by_n, by_m] * 2 + [HBM] * 2,
        out_specs=[by_n, by_n, by_m, HBM, HBM] + [flat(s) for s in (i, i, m, n, n, h)],
        scratch_shapes=[pltpu.VMEM(a.shape, a.dtype) for a in (r_new, c_new, rs, cc, a_early, n_early)] + [
            pltpu.SemaphoreType.DMA((8,))],
        compiler_params=pltpu.CompilerParams(vmem_limit_bytes=60 * 1024 * 1024),
        cost_estimate=pl.CostEstimate(flops=20_000_000_000, bytes_accessed=78_000_000, transcendentals=0),
        name="step",
    )(r_new, c_new, rs, cc, wg, wu, wd, gg, gu, gd, a_early, n_early)


TO_0 = [(1, 0)]
TO_1 = [(0, 1)]


def solution(mesh):
    row_size = mesh.shape['row']
    col_size = mesh.shape['col']
    weight_spec = P('row', 'col')
    act_spec = P(None, 'row')
    grad_spec = P(None, 'col')
    in_specs = (weight_spec,) * 3 + (act_spec, act_spec) + (grad_spec,) * 3 + (P('row'), P('col')) * 3 + (P(),)
    out_specs = (weight_spec,) * 3 + (P('row'), P('col')) * 3 + (act_spec, act_spec)

    def body(w_gate, w_up, w_down, x_norm, x_act, dy_gate, dy_up, dy_down, r_gate, c_gate, r_up, c_up, r_down, c_down, hyper_params):
        d_model = w_gate.shape[0] * row_size
        d_ff = w_gate.shape[1] * col_size
        col = lax.axis_index('col')
        gg, gu, gd, n_early, n_late, a_early, a_late, r_new, c_new, rs, cc = run_fused(
            col_size, row_size, (d_model, d_ff),
            w_gate.T, w_up.T, w_down, x_norm, x_act.T, dy_gate.T, dy_up.T, dy_down,
            r_gate, r_up, r_down, c_gate, c_up, c_down, hyper_params)
        a_in = lax.ppermute(a_late, 'col', TO_1)
        n_in = lax.ppermute(n_late, 'col', TO_0)
        ng, nu, nd, dxa, dxn, rgo, ruo, rdo, cgo, cuo, cdo = run_step(
            dy_down.shape[0], r_new, c_new, rs, cc, w_gate.T, w_up.T, w_down, gg, gu, gd, a_early, n_early)
        dx_norm = lax.dynamic_update_slice(dxn, jnp.where(col == 1, n_late, n_in), (n_early.shape[0], 0))
        dx_act = lax.dynamic_update_slice(dxa, jnp.where(col == 0, a_late, a_in), (a_early.shape[0], 0)).T
        return (ng.T, nu.T, nd, rgo, cgo, ruo, cuo, rdo, cdo, dx_norm, dx_act)

    return jax.shard_map(body, mesh=mesh, in_specs=in_specs, out_specs=out_specs, check_vma=False)
```

```python
import functools

import jax
import jax.numpy as jnp
from jax import lax
from jax.experimental import pallas as pl
from jax.experimental.pallas import tpu as pltpu
from jax.sharding import PartitionSpec as P

EPS_ONE = 1e-30
EPS_TWO = 1e-3
STEPS = 7
BF16 = jnp.bfloat16
F32 = jnp.float32
MESH = pl.DeviceIdType.MESH
VM = pl.BlockSpec(memory_space=pltpu.VMEM)

HBM = pl.BlockSpec(memory_space=pltpu.HBM)

E_ROWS = 208
P_SENT = (272, 176, 192)
W_SENT = (592, 256, 320, 304)
A_ROWS = (304, 288, 256, 320, 304)
A_NEEDS = (0, 0, 1, 2, 3)
R_SENT = (304, 288, 128)
N_SENT = 272


def fold(v, width=128):
    acc = v[:, :width]
    for k in range(1, v.shape[1] // width):
        acc = acc + v[:, k * width:(k + 1) * width]
    return acc


def fold_rows(v):
    return jnp.sum(v.reshape(v.shape[0] // 8, 8, v.shape[1]), axis=0)


def lane_total(v):
    s = jnp.sum(jnp.sum(v, axis=0, keepdims=True), axis=1, keepdims=True)
    lane = lax.broadcasted_iota(jnp.int32, (1, 128), 1)
    return jnp.where(lane == 0, jnp.broadcast_to(s, (1, 128)), 0.0)


def column(row_vec):
    return jnp.broadcast_to(row_vec, (128, row_vec.shape[1])).T


def fused(nc, nr, sizes,
          wg, wu, wd, xn, xa, dg, du, dd, rg, ru, rd, cg, cu, cd, hyper,
          gg, gu, gd, dxn_early, dxn_late, dxa_early, dxa_late, r_out, c_out, rs_out, cc_out,
          xn_v, dd_v, dy_v, e_v, ein_v, p_v, pin_v, wb_v, win_v, dxa_v, dxn_v,
          rg_v, ru_v, rd_v, cg_v, cu_v, cd_v, hyp,
          r_mine, r_peer, c_all, s_all, wsq, wsq_d, rr, cc, racc, cacc, sacc,
          loc, dsem, esem, qsem, psem, wsem, asem, nsem, rsem, csem, ssem):
    col = lax.axis_index('col')
    row = lax.axis_index('row')
    me = col * nr + row
    d_model, d_ff = sizes
    nb = dg.shape[0] // STEPS
    mb = wd.shape[0] // STEPS
    quarter = dd.shape[0] // nr
    others = [(dc, dr) for dc in range(nc) for dr in range(nr) if (dc, dr) != (0, 0)]

    c_all[row] = jnp.zeros(c_all.shape[1:], F32)
    s_all[me] = jnp.zeros(s_all.shape[1:], F32)

    barrier = pltpu.get_barrier_semaphore()
    for dc, dr in others:
        pl.semaphore_signal(barrier, 1, device_id=(lax.rem(col + dc, nc), lax.rem(row + dr, nr)), device_id_type=MESH)

    loads = [pltpu.make_async_copy(a, b, loc.at[k]) for k, (a, b) in enumerate((
        (xn, xn_v), (dd, dd_v), (rg, rg_v), (ru, ru_v), (rd, rd_v), (cg, cg_v), (cu, cu_v), (cd, cd_v), (hyper, hyp)))]
    for load in loads:
        load.start()
    pl.semaphore_wait(barrier, len(others))

    def remote(src, dst, sems, k, target):
        return pltpu.make_async_remote_copy(src_ref=src, dst_ref=dst, send_sem=sems.at[0, k], recv_sem=sems.at[1, k],
                                            device_id=target, device_id_type=MESH)

    def ranged(src, dst, sems, counts, at=0, to=0):
        copies = []
        for k, n in enumerate(counts):
            copies.append(remote(src.at[pl.ds(at, n)], dst.at[pl.ds(at + to, n)], sems, k, across))
            at += n
        return copies

    across = (1 - col, row)
    chip = (col, lax.rem(row + 2, nr))
    core = (col, row + 1 - 2 * lax.rem(row, 2))
    rows_of = lambda r: pl.ds(pl.multiple_of(r * quarter, quarter), quarter)
    dy_copy = remote(dd.at[rows_of(row)], dy_v.at[rows_of(row)], dsem, 0, across)
    p_copies = ranged(p_v, pin_v, psem, P_SENT)
    w_copies = ranged(wb_v, win_v, wsem, W_SENT, E_ROWS, -E_ROWS)
    a_copies = ranged(dxa_v, dxa_early, asem, R_SENT, E_ROWS)
    n_copy = ranged(dxn_v, dxn_early, nsem, (N_SENT,))[0]
    e_copy = remote(e_v, ein_v, esem, 0, across)
    e_back = remote(dxa_v.at[pl.ds(0, E_ROWS)], dxa_early.at[pl.ds(0, E_ROWS)], esem, 1, across)
    dims_t = (((1,), (1,)), ((), ()))

    def act_rows(at, n):
        o = lax.dot_general(wb_v[at:at + n, :], dd_v[...], dims_t, preferred_element_type=F32)
        o = o + lax.dot_general(win_v[at - E_ROWS:at - E_ROWS + n, :], dy_v[...], dims_t, preferred_element_type=F32)
        dxa_v[at:at + n, :] = o.astype(BF16)

    @pl.when(col == 1)
    def _():
        dy_copy.start()

    by_n = lambda width: pl.BlockSpec((nb, width), lambda k: (k, 0))
    by_m = lambda width: pl.BlockSpec((mb, width), lambda k: (k, 0))

    wsq_d[...] = jnp.zeros_like(wsq_d)

    def cast_body(start, w_b):
        w = w_b[...]
        wsq_d[...] += fold_rows(w * w)
        wb_v[pl.ds(pl.multiple_of((start + pl.program_id(0)) * mb, mb), mb), :] = w.astype(BF16)

    def cast(start, count):
        pltpu.emit_pipeline(functools.partial(cast_body, start), grid=(count,), in_specs=[
            pl.BlockSpec((mb, wd.shape[1]), lambda k: (start + k, 0), pipeline_mode=pl.Buffered(4))])(wd)

    cast(0, 1)
    loads[1].wait()
    e_v[...] = lax.dot_general(wb_v[0:E_ROWS, :], dd_v[...], dims_t, preferred_element_type=F32)

    @pl.when(col == 0)
    def _():
        e_copy.start()

    cast(1, STEPS - 1)

    @pl.when(col == 1)
    def _():
        w_copies[0].start()

    p_v[...] = jnp.zeros_like(p_v)
    wsq[...] = jnp.zeros_like(wsq)

    def part_body(wg_b, wu_b, dg_b, du_b):
        for k, (w_b, d_b) in enumerate(((wg_b, dg_b), (wu_b, du_b))):
            w = w_b[...]
            wsq[pl.ds(8 * k, 8), :] += fold_rows(w * w)
            p_v[...] += lax.dot_general(w.astype(BF16), d_b[...], (((0,), (0,)), ((), ())), preferred_element_type=F32)

    pltpu.emit_pipeline(part_body, grid=(STEPS,), in_specs=[by_n(wg.shape[1])] * 2 + [by_n(dg.shape[1])] * 2)(wg, wu, dg, du)

    @pl.when(col == 0)
    def _():
        p_copies[0].start()

    q_far = remote(dy_v.at[rows_of(row)], dy_v.at[rows_of(row)], qsem, 0, chip)
    q_near = remote(dy_v.at[rows_of(row)], dy_v.at[rows_of(row)], qsem, 1, core)
    q_both = remote(dy_v.at[rows_of(chip[1])], dy_v.at[rows_of(chip[1])], qsem, 2, core)

    @pl.when(col == 0)
    def _():
        dy_copy.wait_recv()
        q_far.start()
        q_near.start()

    for load in loads[:1] + loads[2:]:
        load.wait()
    r_mine[...] = jnp.zeros_like(r_mine)
    racc[...] = jnp.zeros_like(racc)
    cacc[...] = jnp.zeros_like(cacc)

    def grad_body(dg_b, du_b, xa_b, gg_b, gu_b, gd_b):
        k = pl.program_id(0)
        for t, (d_b, g_b) in enumerate(((dg_b, gg_b), (du_b, gu_b))):
            g = jnp.dot(d_b[...], xn_v[...], preferred_element_type=F32)
            g_b[...] = g
            q = g * g + EPS_ONE
            racc[pl.ds(8 * t, 8), :] += fold_rows(q)
            c_all[row, pl.ds(7 * t + k, 1), :] = jnp.sum(fold(q).T, axis=0, keepdims=True)
        g = jnp.dot(xa_b[...], dd_v[...], preferred_element_type=F32)
        gd_b[...] = g
        q = g * g + EPS_ONE
        cacc[...] += fold_rows(q)
        r_mine[pl.ds(8 + k, 1), pl.ds(0, 240)] = jnp.sum(fold(q).T, axis=0, keepdims=True)

    pltpu.emit_pipeline(grad_body, grid=(STEPS,), in_specs=[by_n(dg.shape[1])] * 2 + [by_m(xa.shape[1])],
                        out_specs=[by_n(gg.shape[1])] * 2 + [by_m(gd.shape[1])])(dg, du, xa, gg, gu, gd)

    for t in range(2):
        r_mine[t:t + 1, :] = jnp.sum(racc[8 * t:8 * t + 8, :], axis=0, keepdims=True)
    c_down = jnp.sum(cacc[...], axis=0, keepdims=True)
    for k in range(5):
        c_all[row, 14 + k:15 + k, 0:256] = c_down[:, 256 * k:256 * (k + 1)]

    r_copy = remote(r_mine, r_peer, rsem, 0, across)
    r_copy.start()
    c_copies = [pltpu.make_async_remote_copy(
        src_ref=c_all.at[row], dst_ref=c_all.at[row], send_sem=csem.at[0, d], recv_sem=csem.at[1, row],
        device_id=(col, lax.rem(row + d, nr)), device_id_type=MESH) for d in range(1, nr)]
    for c in c_copies:
        c.start()

    @pl.when(col == 0)
    def _():
        p_copies[1].start()
        q_far.wait_recv()
        q_both.start()
        w_copies[0].wait_recv()
        q_near.wait_recv()
        q_both.wait_recv()
        q_far.wait_send()
        q_near.wait_send()
        q_both.wait_send()
        act_rows(E_ROWS, A_ROWS[0])

    @pl.when(col == 1)
    def _():
        w_copies[1].start()
        e_copy.wait_recv()
        dxa_v[0:E_ROWS, :] = (e_v[...] + ein_v[...]).astype(BF16)

    beta = hyp[0]
    rr[...] = jnp.ones_like(rr)
    rr[0:1, :] = rg_v[...].reshape(1, -1)
    rr[1:2, :] = ru_v[...].reshape(1, -1)
    r_old, g_old, u_old, d_old = [v[...].reshape(1, -1) for v in (rd_v, cg_v, cu_v, cd_v)]
    for k in range(STEPS):
        cc[k:k + 1, :] = g_old[:, nb * k:nb * (k + 1)]
        cc[7 + k:8 + k, :] = u_old[:, nb * k:nb * (k + 1)]
        rr[8 + k:9 + k, 0:mb] = r_old[:, mb * k:mb * (k + 1)]
    for k in range(5):
        cc[14 + k:15 + k, 0:256] = d_old[:, 256 * k:256 * (k + 1)]
        cc[14 + k:15 + k, 256:480] = jnp.ones((1, 224), F32)
    cc[19:24, :] = jnp.ones((5, 480), F32)

    r_copy.wait()
    for d in range(1, nr):
        c_copies[d - 1].wait_send()
        s = lax.rem(row + d, nr)
        pltpu.make_async_remote_copy(src_ref=c_all.at[s], dst_ref=c_all.at[s], send_sem=csem.at[0, d], recv_sem=csem.at[1, s],
                                     device_id=(col, s), device_id_type=MESH).wait_recv()

    line = lax.broadcasted_iota(jnp.int32, rr.shape, 0)
    r_new = beta * rr[...] + (1.0 - beta) * ((r_mine[...] + r_peer[...]) / jnp.where(line < 8, float(d_ff), float(d_model)))
    line = lax.broadcasted_iota(jnp.int32, cc.shape, 0)
    c_sum = (c_all[0] + c_all[1]) + (c_all[2] + c_all[3])
    c_new = beta * cc[...] + (1.0 - beta) * (c_sum / jnp.where(line < 14, float(d_model), float(d_ff)))
    r_out[...] = r_new
    c_out[...] = c_new
    rr[...] = lax.rsqrt(r_new)
    cc[...] = lax.rsqrt(c_new)
    cc_out[...] = cc[...]

    sacc[...] = jnp.zeros_like(sacc)

    def square_body(gg_b, gu_b, gd_b):
        k = pl.program_id(0)
        for t, g_b in enumerate((gg_b, gu_b)):
            u = g_b[...] * rr[t:t + 1, :]
            s = fold(u * u)
            c = column(cc[pl.ds(7 * t + k, 1), :])
            sacc[pl.ds(8 * t, 8), :] += fold_rows(s * (c * c))
        c_row = jnp.concatenate([cc[14 + j:15 + j, 0:256] for j in range(5)], axis=1)
        u = gd_b[...] * c_row
        s = fold(u * u)
        r = column(rr[pl.ds(8 + k, 1), :])[0:mb]
        sacc[16:24, :] += fold_rows(s * (r * r))

    pltpu.emit_pipeline(square_body, grid=(STEPS,), in_specs=[by_n(gg.shape[1])] * 2 + [by_m(gd.shape[1])])(gg, gu, gd)

    for t in range(3):
        s_all[me, t:t + 1, :] = jnp.sum(sacc[8 * t:8 * t + 8, :], axis=0, keepdims=True)
    for t in range(2):
        s_all[me, 3 + t:4 + t, :] = jnp.sum(fold(wsq[8 * t:8 * t + 8, :]), axis=0, keepdims=True)
        s_all[me, 6 + t:7 + t, :] = lane_total(r_new[t:t + 1, :])
    s_all[me, 5:6, :] = jnp.sum(fold(wsq_d[...]), axis=0, keepdims=True)
    s_all[me, 8:9, :] = lane_total(r_new[8:15, 0:mb])
    s_copies = []
    for j, (dc, dr) in enumerate(others):
        s_copies.append(pltpu.make_async_remote_copy(
            src_ref=s_all.at[me], dst_ref=s_all.at[me], send_sem=ssem.at[0, j], recv_sem=ssem.at[1, me],
            device_id=(lax.rem(col + dc, nc), lax.rem(row + dr, nr)), device_id_type=MESH))
    for s in s_copies:
        s.start()

    @pl.when(col == 0)
    def _():
        p_copies[2].start()
        a_copies[0].start()

    @pl.when(col == 1)
    def _():
        for w in w_copies[2:]:
            w.start()
        e_back.start()

    for j, (dc, dr) in enumerate(others):
        tc, tr = lax.rem(col + dc, nc), lax.rem(row + dr, nr)
        s_copies[j].wait_send()
        him = tc * nr + tr
        pltpu.make_async_remote_copy(src_ref=s_all.at[him], dst_ref=s_all.at[him], send_sem=ssem.at[0, j],
                                     recv_sem=ssem.at[1, him], device_id=(tc, tr), device_id_type=MESH).wait_recv()
    total = s_all[0]
    for j in range(1, nc * nr):
        total = total + s_all[j]
    sums = jnp.sum(total, axis=1, keepdims=True)
    scales = []
    for t, (m, n) in enumerate(((d_model, d_ff), (d_model, d_ff), (d_ff, d_model))):
        r_mean = sums[6 + t:7 + t] / float(m * nc)
        rms_u = jnp.sqrt(sums[t:t + 1] * r_mean / float(m * n))
        step = hyp[1] * jnp.maximum(EPS_TWO, jnp.sqrt(sums[3 + t:4 + t] / float(m * n)))
        scales.append(step * jnp.sqrt(r_mean) / jnp.maximum(1.0, rms_u / hyp[2]))
    rs_out[...] = rr[...]
    rs_out[0:1, :] = rr[0:1, :] * scales[0]
    rs_out[1:2, :] = rr[1:2, :] * scales[1]
    rs_out[8:16, :] = rr[8:16, :] * scales[2]

    early = E_ROWS + sum(R_SENT)
    rows_n, rows_a = dxn_v.shape[0], dxa_v.shape[0]
    save_e = pltpu.make_async_copy(dxa_v.at[pl.ds(0, E_ROWS)], dxa_early.at[pl.ds(0, E_ROWS)], loc.at[9])
    save_a = pltpu.make_async_copy(dxa_v.at[pl.ds(E_ROWS, early - E_ROWS)], dxa_early.at[pl.ds(E_ROWS, early - E_ROWS)], loc.at[9])
    save_late = pltpu.make_async_copy(dxa_v.at[pl.ds(early, rows_a - early)], dxa_late, loc.at[10])
    save_n = pltpu.make_async_copy(dxn_v.at[pl.ds(0, N_SENT)], dxn_early, loc.at[11])
    save_n_late = pltpu.make_async_copy(dxn_v.at[pl.ds(N_SENT, rows_n - N_SENT)], dxn_late, loc.at[12])

    @pl.when(col == 0)
    def _():
        at = E_ROWS + A_ROWS[0]
        for k in range(1, len(A_ROWS)):
            if A_NEEDS[k] != A_NEEDS[k - 1]:
                w_copies[A_NEEDS[k]].wait_recv()
            act_rows(at, A_ROWS[k])
            at += A_ROWS[k]
            if k < len(R_SENT):
                a_copies[k].start()
            if k == len(R_SENT) - 1:
                save_a.start()
        save_late.start()
        e_copy.wait_send()
        for p in p_copies:
            p.wait_send()
        save_a.wait()
        save_late.wait()
        e_back.wait_recv()
        n_copy.wait_recv()
        for a in a_copies:
            a.wait_send()

    @pl.when(col == 1)
    def _():
        save_e.start()
        for p in p_copies:
            p.wait_recv()
        for j in range(p_v.shape[0] // 128):
            rows = slice(128 * j, 128 * (j + 1))
            dxn_v[:, rows] = (p_v[rows, :] + pin_v[rows, :]).T.astype(BF16)
        n_copy.start()
        save_n.start()
        save_n_late.start()
        save_e.wait()
        save_n.wait()
        save_n_late.wait()
        dy_copy.wait_send()
        for w in w_copies:
            w.wait_send()
        e_back.wait_send()
        for a in a_copies:
            a.wait_recv()
        n_copy.wait_send()


def run_fused(nc, nr, sizes, wg, wu, wd, xn, xa, dg, du, dd, rg, ru, rd, cg, cu, cd, hyper):
    f32, b16 = (lambda *s: jax.ShapeDtypeStruct(s, F32)), (lambda *s: jax.ShapeDtypeStruct(s, BF16))
    n, i = wg.shape
    m, h = wd.shape
    t = dd.shape[0]
    early = E_ROWS + sum(R_SENT)
    dma = lambda *s: pltpu.SemaphoreType.DMA(s)
    vf = lambda *s: pltpu.VMEM(s, F32)
    vb = lambda *s: pltpu.VMEM(s, BF16)
    return pl.pallas_call(
        functools.partial(fused, nc, nr, sizes),
        out_shape=(f32(n, i), f32(n, i), f32(m, h), b16(N_SENT, i), b16(t - N_SENT, i), b16(early, t), b16(m - early, t),
                   f32(16, 640), f32(24, 480), f32(16, 640), f32(24, 480)),
        in_specs=[HBM] * 15,
        out_specs=[HBM] * 7 + [VM] * 4,
        scratch_shapes=[
            vb(*xn.shape), vb(t, h), vb(t, h), vf(E_ROWS, t), vf(E_ROWS, t), vf(i, t), vf(i, t), vb(m, h), vb(m - E_ROWS, h),
            vb(m, t), vb(t, i),
            vf(i), vf(i), vf(m), vf(n), vf(n), vf(h), pltpu.SMEM((3,), F32),
            vf(16, 640), vf(16, 640), vf(nr, 24, 480), vf(nc * nr, 16, 128), vf(16, i), vf(8, h),
            vf(16, 640), vf(24, 480), vf(16, i), vf(8, h), vf(24, 128),
            dma(13), dma(2, 1), dma(2, 2), dma(2, 3), dma(2, len(P_SENT)), dma(2, len(W_SENT)), dma(2, len(R_SENT)), dma(2, 1), dma(2, 1),
            dma(2, nr), dma(2, nc * nr)],
        compiler_params=pltpu.CompilerParams(collective_id=0, has_side_effects=True, vmem_limit_bytes=60 * 1024 * 1024),
        cost_estimate=pl.CostEstimate(flops=22_000_000_000, bytes_accessed=150_000_000, transcendentals=0),
        name="fused",
    )(wg, wu, wd, xn, xa, dg, du, dd, rg, ru, rd, cg, cu, cd, hyper)


def step_kernel(r_hbm, c_hbm, rs_hbm, cc_hbm, wg, wu, wd, gg, gu, gd, a_in, n_in, ng, nu, nd, a_out, n_out,
                rgo, ruo, rdo, cgo, cuo, cdo, r_new, c_new, rs, cc, a_v, n_v, sem):
    k = pl.program_id(0)
    nb, mb = wg.shape[0], wd.shape[0]
    pairs = ((r_hbm, r_new), (c_hbm, c_new), (rs_hbm, rs), (cc_hbm, cc), (a_in, a_v), (n_in, n_v),
             (a_v, a_out.at[pl.ds(0, a_v.shape[0])]), (n_v, n_out.at[pl.ds(0, n_v.shape[0])]))
    copies = [pltpu.make_async_copy(a, b, sem.at[j]) for j, (a, b) in enumerate(pairs)]

    @pl.when(k == 0)
    def _():
        for c in copies[:6]:
            c.start()
        for c in copies[:4]:
            c.wait()
        rgo[...] = r_new[0:1, :].reshape(-1)
        ruo[...] = r_new[1:2, :].reshape(-1)
        rdo[...] = jnp.concatenate([r_new[8 + j:9 + j, 0:mb] for j in range(STEPS)], axis=1).reshape(-1)
        cgo[...] = jnp.concatenate([c_new[j:j + 1, :] for j in range(STEPS)], axis=1).reshape(-1)
        cuo[...] = jnp.concatenate([c_new[7 + j:8 + j, :] for j in range(STEPS)], axis=1).reshape(-1)
        cdo[...] = jnp.concatenate([c_new[14 + j:15 + j, 0:256] for j in range(5)], axis=1).reshape(-1)

    @pl.when(k == 1)
    def _():
        for c in copies[4:6]:
            c.wait()
        for c in copies[6:]:
            c.start()

    @pl.when(k == STEPS - 1)
    def _():
        for c in copies[6:]:
            c.wait()

    for t, (w, g, o) in enumerate(((wg, gg, ng), (wu, gu, nu))):
        c = column(cc[pl.ds(7 * t + k, 1), :])
        for j in range(w.shape[1] // 128):
            lanes = slice(128 * j, 128 * (j + 1))
            o[:, lanes] = w[:, lanes] - g[:, lanes] * rs[t:t + 1, lanes] * c
    r = column(rs[pl.ds(8 + k, 1), :])[0:mb]
    for j in range(wd.shape[1] // 128):
        lanes = slice(128 * j, 128 * (j + 1))
        c = cc[14 + j // 2:15 + j // 2, 128 * (j % 2):128 * (j % 2 + 1)]
        nd[:, lanes] = wd[:, lanes] - gd[:, lanes] * c * r


def run_step(tokens, r_new, c_new, rs, cc, wg, wu, wd, gg, gu, gd, a_early, n_early):
    f32 = lambda *s: jax.ShapeDtypeStruct(s, F32)
    n, i = wg.shape
    m, h = wd.shape
    flat = lambda s: pl.BlockSpec((s,), lambda k: (0,))
    by_n = pl.BlockSpec((n // STEPS, i), lambda k: (k, 0))
    by_m = pl.BlockSpec((m // STEPS, h), lambda k: (k, 0))
    b16 = lambda *s: jax.ShapeDtypeStruct(s, BF16)
    return pl.pallas_call(
        step_kernel, grid=(STEPS,),
        out_shape=(f32(n, i), f32(n, i), f32(m, h), b16(m, tokens), b16(tokens, i), f32(i), f32(i), f32(m), f32(n), f32(n), f32(h)),
        in_specs=[HBM] * 4 + [by_n, by_n, by_m] * 2 + [HBM] * 2,
        out_specs=[by_n, by_n, by_m, HBM, HBM] + [flat(s) for s in (i, i, m, n, n, h)],
        scratch_shapes=[pltpu.VMEM(a.shape, a.dtype) for a in (r_new, c_new, rs, cc, a_early, n_early)] + [
            pltpu.SemaphoreType.DMA((8,))],
        compiler_params=pltpu.CompilerParams(vmem_limit_bytes=60 * 1024 * 1024),
        cost_estimate=pl.CostEstimate(flops=20_000_000_000, bytes_accessed=78_000_000, transcendentals=0),
        name="step",
    )(r_new, c_new, rs, cc, wg, wu, wd, gg, gu, gd, a_early, n_early)


TO_0 = [(1, 0)]
TO_1 = [(0, 1)]


def solution(mesh):
    row_size = mesh.shape['row']
    col_size = mesh.shape['col']
    weight_spec = P('row', 'col')
    act_spec = P(None, 'row')
    grad_spec = P(None, 'col')
    in_specs = (weight_spec,) * 3 + (act_spec, act_spec) + (grad_spec,) * 3 + (P('row'), P('col')) * 3 + (P(),)
    out_specs = (weight_spec,) * 3 + (P('row'), P('col')) * 3 + (act_spec, act_spec)

    def body(w_gate, w_up, w_down, x_norm, x_act, dy_gate, dy_up, dy_down, r_gate, c_gate, r_up, c_up, r_down, c_down, hyper_params):
        d_model = w_gate.shape[0] * row_size
        d_ff = w_gate.shape[1] * col_size
        col = lax.axis_index('col')
        gg, gu, gd, n_early, n_late, a_early, a_late, r_new, c_new, rs, cc = run_fused(
            col_size, row_size, (d_model, d_ff),
            w_gate.T, w_up.T, w_down, x_norm, x_act.T, dy_gate.T, dy_up.T, dy_down,
            r_gate, r_up, r_down, c_gate, c_up, c_down, hyper_params)
        a_in = lax.ppermute(a_late, 'col', TO_1)
        n_in = lax.ppermute(n_late, 'col', TO_0)
        ng, nu, nd, dxa, dxn, rgo, ruo, rdo, cgo, cuo, cdo = run_step(
            dy_down.shape[0], r_new, c_new, rs, cc, w_gate.T, w_up.T, w_down, gg, gu, gd, a_early, n_early)
        dx_norm = lax.dynamic_update_slice(dxn, jnp.where(col == 1, n_late, n_in), (n_early.shape[0], 0))
        dx_act = lax.dynamic_update_slice(dxa, jnp.where(col == 0, a_late, a_in), (a_early.shape[0], 0)).T
        return (ng.T, nu.T, nd, rgo, cgo, ruo, cuo, rdo, cdo, dx_norm, dx_act)

    return jax.shard_map(body, mesh=mesh, in_specs=in_specs, out_specs=out_specs, check_vma=False)
```

```python
import functools

import jax
import jax.numpy as jnp
from jax import lax
from jax.experimental import pallas as pl
from jax.experimental.pallas import tpu as pltpu
from jax.sharding import PartitionSpec as P

EPS_ONE = 1e-30
EPS_TWO = 1e-3
STEPS = 7
BF16 = jnp.bfloat16
F32 = jnp.float32
MESH = pl.DeviceIdType.MESH
VM = pl.BlockSpec(memory_space=pltpu.VMEM)

HBM = pl.BlockSpec(memory_space=pltpu.HBM)

E_ROWS = 208
E_BACK = 80
Y_COLS = 128
P_SENT = (256, 192, 64)
W_SENT = (544, 288, 528, 112)
A_ROWS = (272, 272, 288, 528, 112)
A_NEEDS = (0, 0, 1, 2, 3)
R_SENT = (272, 272, 256)


def fold(v, width=128):
    acc = v[:, :width]
    for k in range(1, v.shape[1] // width):
        acc = acc + v[:, k * width:(k + 1) * width]
    return acc


def fold_rows(v):
    return jnp.sum(v.reshape(v.shape[0] // 8, 8, v.shape[1]), axis=0)


def lane_total(v):
    s = jnp.sum(jnp.sum(v, axis=0, keepdims=True), axis=1, keepdims=True)
    lane = lax.broadcasted_iota(jnp.int32, (1, 128), 1)
    return jnp.where(lane == 0, jnp.broadcast_to(s, (1, 128)), 0.0)


def column(row_vec):
    return jnp.broadcast_to(row_vec, (128, row_vec.shape[1])).T


def fused(nc, nr, sizes,
          wg, wu, wd, xn, xa, dg, du, dd, rg, ru, rd, cg, cu, cd, hyper,
          gg, gu, gd, n_cols, dxa_early, late, r_hbm, c_hbm, rs_hbm, cc_hbm,
          xn_v, dd_v, dy_v, e_v, ein_v, p_v, pin_v, wb_v, win_v, dxa_v, dxn_v,
          rg_v, ru_v, rd_v, cg_v, cu_v, cd_v, hyp,
          r_mine, r_peer, c_all, s_all, wsq, wsq_d, rr, cc, racc, cacc, sacc, r_out, c_out, rs_out,
          loc, dsem, esem, qsem, psem, wsem, asem, nsem, rsem, csem, ssem):
    col = lax.axis_index('col')
    row = lax.axis_index('row')
    me = col * nr + row
    d_model, d_ff = sizes
    nb = dg.shape[0] // STEPS
    mb = wd.shape[0] // STEPS
    quarter = dd.shape[0] // nr
    others = [(dc, dr) for dc in range(nc) for dr in range(nr) if (dc, dr) != (0, 0)]

    c_all[row] = jnp.zeros(c_all.shape[1:], F32)
    s_all[me] = jnp.zeros(s_all.shape[1:], F32)

    barrier = pltpu.get_barrier_semaphore()
    for dc, dr in others:
        pl.semaphore_signal(barrier, 1, device_id=(lax.rem(col + dc, nc), lax.rem(row + dr, nr)), device_id_type=MESH)

    loads = [pltpu.make_async_copy(a, b, loc.at[k]) for k, (a, b) in enumerate((
        (xn, xn_v), (dd, dd_v), (rg, rg_v), (ru, ru_v), (rd, rd_v), (cg, cg_v), (cu, cu_v), (cd, cd_v), (hyper, hyp)))]
    for load in loads:
        load.start()
    pl.semaphore_wait(barrier, len(others))

    def remote(src, dst, sems, k, target):
        return pltpu.make_async_remote_copy(src_ref=src, dst_ref=dst, send_sem=sems.at[0, k], recv_sem=sems.at[1, k],
                                            device_id=target, device_id_type=MESH)

    def ranged(src, dst, sems, counts, at=0, to=0):
        copies = []
        for k, n in enumerate(counts):
            copies.append(remote(src.at[pl.ds(at, n)], dst.at[pl.ds(at + to, n)], sems, k, across))
            at += n
        return copies

    across = (1 - col, row)
    chip = (col, lax.rem(row + 2, nr))
    core = (col, row + 1 - 2 * lax.rem(row, 2))
    rows_of = lambda r: pl.ds(pl.multiple_of(r * quarter, quarter), quarter)
    dy_copy = remote(dd.at[rows_of(row)], dy_v.at[rows_of(row)], dsem, 0, across)
    p_copies = ranged(p_v, pin_v, psem, P_SENT)
    w_copies = ranged(wb_v, win_v, wsem, W_SENT, E_ROWS, -E_ROWS)
    a_copies = ranged(dxa_v, dxa_early, asem, R_SENT, E_ROWS)
    split = p_v.shape[0] - Y_COLS
    own_cols = dxn_v.at[:, pl.ds(split, Y_COLS)]
    y_copy = ranged(p_v, pin_v, nsem, (Y_COLS,), split)[0]
    n_copy = remote(own_cols, n_cols, nsem, 1, across)
    e_copy = remote(e_v, ein_v, esem, 0, across)
    e_back = remote(dxa_v.at[pl.ds(0, E_BACK)], dxa_early.at[pl.ds(0, E_BACK)], esem, 1, across)
    dims_t = (((1,), (1,)), ((), ()))

    def act_rows(at, n):
        o = lax.dot_general(wb_v[at:at + n, :], dd_v[...], dims_t, preferred_element_type=F32)
        o = o + lax.dot_general(win_v[at - E_ROWS:at - E_ROWS + n, :], dy_v[...], dims_t, preferred_element_type=F32)
        dxa_v[at:at + n, :] = o.astype(BF16)

    @pl.when(col == 1)
    def _():
        dy_copy.start()

    by_n = lambda width: pl.BlockSpec((nb, width), lambda k: (k, 0))
    by_m = lambda width: pl.BlockSpec((mb, width), lambda k: (k, 0))

    wsq_d[...] = jnp.zeros_like(wsq_d)

    def cast_body(start, w_b):
        w = w_b[...]
        wsq_d[...] += fold_rows(w * w)
        wb_v[pl.ds(pl.multiple_of((start + pl.program_id(0)) * mb, mb), mb), :] = w.astype(BF16)

    def cast(start, count):
        pltpu.emit_pipeline(functools.partial(cast_body, start), grid=(count,), in_specs=[
            pl.BlockSpec((mb, wd.shape[1]), lambda k: (start + k, 0), pipeline_mode=pl.Buffered(4))])(wd)

    cast(0, 1)
    loads[1].wait()
    e_v[...] = lax.dot_general(wb_v[0:E_ROWS, :], dd_v[...], dims_t, preferred_element_type=F32)

    @pl.when(col == 0)
    def _():
        e_copy.start()

    cast(1, STEPS - 1)

    @pl.when(col == 1)
    def _():
        w_copies[0].start()

    p_v[...] = jnp.zeros_like(p_v)
    wsq[...] = jnp.zeros_like(wsq)

    def part_body(wg_b, wu_b, dg_b, du_b):
        for k, (w_b, d_b) in enumerate(((wg_b, dg_b), (wu_b, du_b))):
            w = w_b[...]
            wsq[pl.ds(8 * k, 8), :] += fold_rows(w * w)
            p_v[...] += lax.dot_general(w.astype(BF16), d_b[...], (((0,), (0,)), ((), ())), preferred_element_type=F32)

    deep_n = lambda width: pl.BlockSpec((nb, width), lambda k: (k, 0), pipeline_mode=pl.Buffered(3))
    pltpu.emit_pipeline(part_body, grid=(STEPS,), in_specs=[deep_n(wg.shape[1])] * 2 + [deep_n(dg.shape[1])] * 2)(wg, wu, dg, du)

    @pl.when(col == 0)
    def _():
        p_copies[0].start()

    q_far = remote(dy_v.at[rows_of(row)], dy_v.at[rows_of(row)], qsem, 0, chip)
    q_near = remote(dy_v.at[rows_of(row)], dy_v.at[rows_of(row)], qsem, 1, core)
    q_both = remote(dy_v.at[rows_of(chip[1])], dy_v.at[rows_of(chip[1])], qsem, 2, core)

    @pl.when(col == 0)
    def _():
        dy_copy.wait_recv()
        q_far.start()
        q_near.start()

    for load in loads[:1] + loads[2:]:
        load.wait()
    r_mine[...] = jnp.zeros_like(r_mine)
    racc[...] = jnp.zeros_like(racc)
    cacc[...] = jnp.zeros_like(cacc)

    def grad_body(dg_b, du_b, xa_b, gg_b, gu_b, gd_b):
        k = pl.program_id(0)
        for t, (d_b, g_b) in enumerate(((dg_b, gg_b), (du_b, gu_b))):
            g = jnp.dot(d_b[...], xn_v[...], preferred_element_type=F32)
            g_b[...] = g
            q = g * g + EPS_ONE
            racc[pl.ds(8 * t, 8), :] += fold_rows(q)
            c_all[row, pl.ds(7 * t + k, 1), :] = jnp.sum(fold(q).T, axis=0, keepdims=True)
        g = jnp.dot(xa_b[...], dd_v[...], preferred_element_type=F32)
        gd_b[...] = g
        q = g * g + EPS_ONE
        cacc[...] += fold_rows(q)
        r_mine[pl.ds(8 + k, 1), pl.ds(0, 240)] = jnp.sum(fold(q).T, axis=0, keepdims=True)

    pltpu.emit_pipeline(grad_body, grid=(STEPS,), in_specs=[by_n(dg.shape[1])] * 2 + [by_m(xa.shape[1])],
                        out_specs=[by_n(gg.shape[1])] * 2 + [by_m(gd.shape[1])])(dg, du, xa, gg, gu, gd)

    for t in range(2):
        r_mine[t:t + 1, :] = jnp.sum(racc[8 * t:8 * t + 8, :], axis=0, keepdims=True)
    c_down = jnp.sum(cacc[...], axis=0, keepdims=True)
    for k in range(5):
        c_all[row, 14 + k:15 + k, 0:256] = c_down[:, 256 * k:256 * (k + 1)]

    r_copy = remote(r_mine, r_peer, rsem, 0, across)
    r_copy.start()
    c_copies = [pltpu.make_async_remote_copy(
        src_ref=c_all.at[row], dst_ref=c_all.at[row], send_sem=csem.at[0, d], recv_sem=csem.at[1, row],
        device_id=(col, lax.rem(row + d, nr)), device_id_type=MESH) for d in range(1, nr)]
    for c in c_copies:
        c.start()

    @pl.when(col == 0)
    def _():
        p_copies[1].start()
        q_far.wait_recv()
        q_both.start()
        w_copies[0].wait_recv()
        q_near.wait_recv()
        q_both.wait_recv()
        q_far.wait_send()
        q_near.wait_send()
        q_both.wait_send()
        act_rows(E_ROWS, A_ROWS[0])

    @pl.when(col == 1)
    def _():
        w_copies[1].start()
        e_copy.wait_recv()
        dxa_v[0:E_ROWS, :] = (e_v[...] + ein_v[...]).astype(BF16)

    beta = hyp[0]
    rr[...] = jnp.ones_like(rr)
    rr[0:1, :] = rg_v[...].reshape(1, -1)
    rr[1:2, :] = ru_v[...].reshape(1, -1)
    r_old, g_old, u_old, d_old = [v[...].reshape(1, -1) for v in (rd_v, cg_v, cu_v, cd_v)]
    for k in range(STEPS):
        cc[k:k + 1, :] = g_old[:, nb * k:nb * (k + 1)]
        cc[7 + k:8 + k, :] = u_old[:, nb * k:nb * (k + 1)]
        rr[8 + k:9 + k, 0:mb] = r_old[:, mb * k:mb * (k + 1)]
    for k in range(5):
        cc[14 + k:15 + k, 0:256] = d_old[:, 256 * k:256 * (k + 1)]
        cc[14 + k:15 + k, 256:480] = jnp.ones((1, 224), F32)
    cc[19:24, :] = jnp.ones((5, 480), F32)

    r_copy.wait()
    for d in range(1, nr):
        c_copies[d - 1].wait_send()
        s = lax.rem(row + d, nr)
        pltpu.make_async_remote_copy(src_ref=c_all.at[s], dst_ref=c_all.at[s], send_sem=csem.at[0, d], recv_sem=csem.at[1, s],
                                     device_id=(col, s), device_id_type=MESH).wait_recv()

    line = lax.broadcasted_iota(jnp.int32, rr.shape, 0)
    r_new = beta * rr[...] + (1.0 - beta) * ((r_mine[...] + r_peer[...]) / jnp.where(line < 8, float(d_ff), float(d_model)))
    line = lax.broadcasted_iota(jnp.int32, cc.shape, 0)
    c_sum = (c_all[0] + c_all[1]) + (c_all[2] + c_all[3])
    c_new = beta * cc[...] + (1.0 - beta) * (c_sum / jnp.where(line < 14, float(d_model), float(d_ff)))
    r_out[...] = r_new
    c_out[...] = c_new
    rr[...] = lax.rsqrt(r_new)
    cc[...] = lax.rsqrt(c_new)
    save_r = pltpu.make_async_copy(r_out, r_hbm, loc.at[11])
    save_c = pltpu.make_async_copy(c_out, c_hbm, loc.at[12])
    save_cc = pltpu.make_async_copy(cc, cc_hbm, loc.at[13])

    sacc[...] = jnp.zeros_like(sacc)

    def square_body(gg_b, gu_b, gd_b):
        k = pl.program_id(0)
        for t, g_b in enumerate((gg_b, gu_b)):
            u = g_b[...] * rr[t:t + 1, :]
            s = fold(u * u)
            c = column(cc[pl.ds(7 * t + k, 1), :])
            sacc[pl.ds(8 * t, 8), :] += fold_rows(s * (c * c))
        c_row = jnp.concatenate([cc[14 + j:15 + j, 0:256] for j in range(5)], axis=1)
        u = gd_b[...] * c_row
        s = fold(u * u)
        r = column(rr[pl.ds(8 + k, 1), :])[0:mb]
        sacc[16:24, :] += fold_rows(s * (r * r))

    pltpu.emit_pipeline(square_body, grid=(STEPS,), in_specs=[by_n(gg.shape[1])] * 2 + [by_m(gd.shape[1])])(gg, gu, gd)

    for t in range(3):
        s_all[me, t:t + 1, :] = jnp.sum(sacc[8 * t:8 * t + 8, :], axis=0, keepdims=True)
    for t in range(2):
        s_all[me, 3 + t:4 + t, :] = jnp.sum(fold(wsq[8 * t:8 * t + 8, :]), axis=0, keepdims=True)
        s_all[me, 6 + t:7 + t, :] = lane_total(r_new[t:t + 1, :])
    s_all[me, 5:6, :] = jnp.sum(fold(wsq_d[...]), axis=0, keepdims=True)
    s_all[me, 8:9, :] = lane_total(r_new[8:15, 0:mb])
    s_copies = []
    for j, (dc, dr) in enumerate(others):
        s_copies.append(pltpu.make_async_remote_copy(
            src_ref=s_all.at[me], dst_ref=s_all.at[me], send_sem=ssem.at[0, j], recv_sem=ssem.at[1, me],
            device_id=(lax.rem(col + dc, nc), lax.rem(row + dr, nr)), device_id_type=MESH))
    for s in s_copies:
        s.start()

    @pl.when(col == 0)
    def _():
        p_copies[2].start()
        a_copies[0].start()

    @pl.when(col == 1)
    def _():
        y_copy.start()
        for w in w_copies[2:]:
            w.start()
        e_back.start()

    for j, (dc, dr) in enumerate(others):
        tc, tr = lax.rem(col + dc, nc), lax.rem(row + dr, nr)
        s_copies[j].wait_send()
        him = tc * nr + tr
        pltpu.make_async_remote_copy(src_ref=s_all.at[him], dst_ref=s_all.at[him], send_sem=ssem.at[0, j],
                                     recv_sem=ssem.at[1, him], device_id=(tc, tr), device_id_type=MESH).wait_recv()
    total = s_all[0]
    for j in range(1, nc * nr):
        total = total + s_all[j]
    sums = jnp.sum(total, axis=1, keepdims=True)
    scales = []
    for t, (m, n) in enumerate(((d_model, d_ff), (d_model, d_ff), (d_ff, d_model))):
        r_mean = sums[6 + t:7 + t] / float(m * nc)
        rms_u = jnp.sqrt(sums[t:t + 1] * r_mean / float(m * n))
        step = hyp[1] * jnp.maximum(EPS_TWO, jnp.sqrt(sums[3 + t:4 + t] / float(m * n)))
        scales.append(step * jnp.sqrt(r_mean) / jnp.maximum(1.0, rms_u / hyp[2]))
    rs_out[...] = rr[...]
    rs_out[0:1, :] = rr[0:1, :] * scales[0]
    rs_out[1:2, :] = rr[1:2, :] * scales[1]
    rs_out[8:16, :] = rr[8:16, :] * scales[2]
    save_rs = pltpu.make_async_copy(rs_out, rs_hbm, loc.at[14])
    save_stats = (save_r, save_c, save_cc, save_rs)
    for c in save_stats:
        c.start()

    early = E_ROWS + sum(R_SENT)
    rows_a, half = dxa_v.shape[0], dxn_v.shape[0] // 2
    save_e = pltpu.make_async_copy(dxa_v.at[pl.ds(0, E_ROWS)], dxa_early.at[pl.ds(0, E_ROWS)], loc.at[9])
    save_a = pltpu.make_async_copy(dxa_v.at[pl.ds(E_ROWS, early - E_ROWS)], dxa_early.at[pl.ds(E_ROWS, early - E_ROWS)], loc.at[9])
    save_late = pltpu.make_async_copy(dxa_v.at[pl.ds(early, rows_a - early)], late, loc.at[10])
    save_y = pltpu.make_async_copy(own_cols, n_cols, loc.at[15])
    save_pack = [pltpu.make_async_copy(a, b, loc.at[15 + k]) for k, (a, b) in enumerate((
        (dxn_v.at[pl.ds(0, half), pl.ds(0, split)], late.at[pl.ds(0, half), pl.ds(0, split)]),
        (dxn_v.at[pl.ds(half, half), pl.ds(0, split)], late.at[pl.ds(0, half), pl.ds(split, split)]),
        (dxa_v.at[pl.ds(E_BACK, E_ROWS - E_BACK)], late.at[pl.ds(half, E_ROWS - E_BACK)])))]

    def norm_columns(start, stop):
        for j in range(start, stop, 128):
            dxn_v[:, j:j + 128] = (p_v[j:j + 128, :] + pin_v[j:j + 128, :]).T.astype(BF16)

    @pl.when(col == 0)
    def _():
        at = E_ROWS + A_ROWS[0]
        for k in range(1, len(A_ROWS)):
            if k == 2:
                y_copy.wait_recv()
                norm_columns(split, split + Y_COLS)
                n_copy.start()
                save_y.start()
            if A_NEEDS[k] != A_NEEDS[k - 1]:
                w_copies[A_NEEDS[k]].wait_recv()
            act_rows(at, A_ROWS[k])
            at += A_ROWS[k]
            if k < len(R_SENT):
                a_copies[k].start()
            if k == len(R_SENT) - 1:
                save_a.start()
        save_late.start()
        e_copy.wait_send()
        for p in p_copies:
            p.wait_send()
        n_copy.wait_send()
        save_a.wait()
        save_y.wait()
        save_late.wait()
        e_back.wait_recv()
        for a in a_copies:
            a.wait_send()

    @pl.when(col == 1)
    def _():
        save_e.start()
        for p in p_copies:
            p.wait_recv()
        norm_columns(0, split)
        for c in save_pack:
            c.start()
        save_e.wait()
        for c in save_pack:
            c.wait()
        dy_copy.wait_send()
        y_copy.wait_send()
        for w in w_copies:
            w.wait_send()
        e_back.wait_send()
        n_copy.wait_recv()
        for a in a_copies:
            a.wait_recv()

    for c in save_stats:
        c.wait()


def run_fused(nc, nr, sizes, wg, wu, wd, xn, xa, dg, du, dd, rg, ru, rd, cg, cu, cd, hyper):
    f32, b16 = (lambda *s: jax.ShapeDtypeStruct(s, F32)), (lambda *s: jax.ShapeDtypeStruct(s, BF16))
    n, i = wg.shape
    m, h = wd.shape
    t = dd.shape[0]
    early = E_ROWS + sum(R_SENT)
    dma = lambda *s: pltpu.SemaphoreType.DMA(s)
    vf = lambda *s: pltpu.VMEM(s, F32)
    vb = lambda *s: pltpu.VMEM(s, BF16)
    return pl.pallas_call(
        functools.partial(fused, nc, nr, sizes),
        out_shape=(f32(n, i), f32(n, i), f32(m, h), b16(t, Y_COLS), b16(early, t), b16(m - early, t),
                   f32(16, 640), f32(24, 480), f32(16, 640), f32(24, 480)),
        in_specs=[HBM] * 15,
        out_specs=[HBM] * 10,
        scratch_shapes=[
            vb(*xn.shape), vb(t, h), vb(t, h), vf(E_ROWS, t), vf(E_ROWS, t), vf(i, t), vf(i, t), vb(m, h), vb(m - E_ROWS, h),
            vb(m, t), vb(t, i),
            vf(i), vf(i), vf(m), vf(n), vf(n), vf(h), pltpu.SMEM((3,), F32),
            vf(16, 640), vf(16, 640), vf(nr, 24, 480), vf(nc * nr, 16, 128), vf(16, i), vf(8, h),
            vf(16, 640), vf(24, 480), vf(16, i), vf(8, h), vf(24, 128),
            vf(16, 640), vf(24, 480), vf(16, 640),
            dma(18), dma(2, 1), dma(2, 2), dma(2, 3), dma(2, len(P_SENT)), dma(2, len(W_SENT)), dma(2, len(R_SENT)), dma(2, 2), dma(2, 1),
            dma(2, nr), dma(2, nc * nr)],
        compiler_params=pltpu.CompilerParams(collective_id=0, has_side_effects=True, vmem_limit_bytes=60 * 1024 * 1024),
        cost_estimate=pl.CostEstimate(flops=22_000_000_000, bytes_accessed=150_000_000, transcendentals=0),
        name="fused",
    )(wg, wu, wd, xn, xa, dg, du, dd, rg, ru, rd, cg, cu, cd, hyper)


def placements(col, buf, a_out, n_out, sending):
    half, split = n_out.shape[0] // 2, n_out.shape[1] - Y_COLS
    rows = a_out.shape[0] - buf.shape[0]
    act = [(buf, a_out.at[pl.ds(rows, buf.shape[0])])]
    norm = [(buf.at[pl.ds(0, half), pl.ds(0, split)], n_out.at[pl.ds(0, half), pl.ds(0, split)]),
            (buf.at[pl.ds(0, half), pl.ds(split, split)], n_out.at[pl.ds(half, half), pl.ds(0, split)])]
    back = [(buf.at[pl.ds(half, E_ROWS - E_BACK)], a_out.at[pl.ds(E_BACK, E_ROWS - E_BACK)])]
    return (act, norm) if sending else (norm + back, act)


def per_side(col, choices, sem, at, action):
    for side, pairs in enumerate(choices):
        @pl.when(col == side)
        def _(pairs=pairs):
            for j, (a, b) in enumerate(pairs):
                action(pltpu.make_async_copy(a, b, sem.at[at + j]))


def step_kernel(r_hbm, c_hbm, rs_hbm, cc_hbm, wg, wu, wd, gg, gu, gd, a_in, n_in, l_in, ng, nu, nd, a_out, n_out,
                rgo, ruo, rdo, cgo, cuo, cdo, r_new, c_new, rs, cc, a_v, n_v, l_v, sem):
    k = pl.program_id(0)
    col = lax.axis_index('col')
    nb, mb = wg.shape[0], wd.shape[0]
    cols = n_v.shape[1]
    pairs = ((r_hbm, r_new), (c_hbm, c_new), (rs_hbm, rs), (cc_hbm, cc), (a_in, a_v), (n_in, n_v), (l_in, l_v),
             (a_v, a_out.at[pl.ds(0, a_v.shape[0])]), (n_v, n_out.at[:, pl.ds(n_out.shape[1] - cols, cols)]))
    copies = [pltpu.make_async_copy(a, b, sem.at[j]) for j, (a, b) in enumerate(pairs)]
    own = placements(col, l_v, a_out, n_out, True)

    @pl.when(k == 0)
    def _():
        for c in copies[:7]:
            c.start()
        for c in copies[:4]:
            c.wait()
        rgo[...] = r_new[0:1, :].reshape(-1)
        ruo[...] = r_new[1:2, :].reshape(-1)
        rdo[...] = jnp.concatenate([r_new[8 + j:9 + j, 0:mb] for j in range(STEPS)], axis=1).reshape(-1)
        cgo[...] = jnp.concatenate([c_new[j:j + 1, :] for j in range(STEPS)], axis=1).reshape(-1)
        cuo[...] = jnp.concatenate([c_new[7 + j:8 + j, :] for j in range(STEPS)], axis=1).reshape(-1)
        cdo[...] = jnp.concatenate([c_new[14 + j:15 + j, 0:256] for j in range(5)], axis=1).reshape(-1)

    @pl.when(k == 1)
    def _():
        for c in copies[4:7]:
            c.wait()
        for c in copies[7:]:
            c.start()
        per_side(col, own, sem, len(pairs), lambda c: c.start())

    @pl.when(k == STEPS - 1)
    def _():
        for c in copies[7:]:
            c.wait()
        per_side(col, own, sem, len(pairs), lambda c: c.wait())

    for t, (w, g, o) in enumerate(((wg, gg, ng), (wu, gu, nu))):
        c = column(cc[pl.ds(7 * t + k, 1), :])
        for j in range(w.shape[1] // 128):
            lanes = slice(128 * j, 128 * (j + 1))
            o[:, lanes] = w[:, lanes] - g[:, lanes] * rs[t:t + 1, lanes] * c
    r = column(rs[pl.ds(8 + k, 1), :])[0:mb]
    for j in range(wd.shape[1] // 128):
        lanes = slice(128 * j, 128 * (j + 1))
        c = cc[14 + j // 2:15 + j // 2, 128 * (j % 2):128 * (j % 2 + 1)]
        nd[:, lanes] = wd[:, lanes] - gd[:, lanes] * c * r


def run_step(r_new, c_new, rs, cc, wg, wu, wd, gg, gu, gd, a_early, n_cols, late):
    f32 = lambda *s: jax.ShapeDtypeStruct(s, F32)
    b16 = lambda *s: jax.ShapeDtypeStruct(s, BF16)
    n, i = wg.shape
    m, h = wd.shape
    t = n_cols.shape[0]
    flat = lambda s: pl.BlockSpec((s,), lambda k: (0,))
    by_n = pl.BlockSpec((n // STEPS, i), lambda k: (k, 0))
    by_m = pl.BlockSpec((m // STEPS, h), lambda k: (k, 0))
    return pl.pallas_call(
        step_kernel, grid=(STEPS,),
        out_shape=(f32(n, i), f32(n, i), f32(m, h), b16(m, t), b16(t, i), f32(i), f32(i), f32(m), f32(n), f32(n), f32(h)),
        in_specs=[HBM] * 4 + [by_n, by_n, by_m] * 2 + [HBM] * 3,
        out_specs=[by_n, by_n, by_m, HBM, HBM] + [flat(s) for s in (i, i, m, n, n, h)],
        scratch_shapes=[pltpu.VMEM(a.shape, a.dtype) for a in (r_new, c_new, rs, cc, a_early, n_cols, late)] + [
            pltpu.SemaphoreType.DMA((12,))],
        compiler_params=pltpu.CompilerParams(vmem_limit_bytes=60 * 1024 * 1024),
        cost_estimate=pl.CostEstimate(flops=20_000_000_000, bytes_accessed=78_000_000, transcendentals=0),
        name="step",
    )(r_new, c_new, rs, cc, wg, wu, wd, gg, gu, gd, a_early, n_cols, late)


def place_kernel(late_in, a_in, n_in, a_out, n_out, sem):
    col = lax.axis_index('col')
    got = placements(col, late_in, a_out, n_out, False)
    per_side(col, got, sem, 0, lambda c: c.start())
    per_side(col, got, sem, 0, lambda c: c.wait())


def run_place(late_in, dxa, dxn):
    return pl.pallas_call(
        place_kernel,
        out_shape=(jax.ShapeDtypeStruct(dxa.shape, BF16), jax.ShapeDtypeStruct(dxn.shape, BF16)),
        in_specs=[pl.BlockSpec(memory_space=pl.ANY), HBM, HBM], out_specs=[HBM, HBM], input_output_aliases={1: 0, 2: 1},
        scratch_shapes=[pltpu.SemaphoreType.DMA((3,))],
        compiler_params=pltpu.CompilerParams(vmem_limit_bytes=1024 * 1024),
        name="place",
    )(late_in, dxa, dxn)


SWAP = [(0, 1), (1, 0)]


def solution(mesh):
    row_size = mesh.shape['row']
    col_size = mesh.shape['col']
    weight_spec = P('row', 'col')
    act_spec = P(None, 'row')
    grad_spec = P(None, 'col')
    in_specs = (weight_spec,) * 3 + (act_spec, act_spec) + (grad_spec,) * 3 + (P('row'), P('col')) * 3 + (P(),)
    out_specs = (weight_spec,) * 3 + (P('row'), P('col')) * 3 + (act_spec, act_spec)

    def body(w_gate, w_up, w_down, x_norm, x_act, dy_gate, dy_up, dy_down, r_gate, c_gate, r_up, c_up, r_down, c_down, hyper_params):
        d_model = w_gate.shape[0] * row_size
        d_ff = w_gate.shape[1] * col_size
        gg, gu, gd, n_cols, a_early, late, r_new, c_new, rs, cc = run_fused(
            col_size, row_size, (d_model, d_ff),
            w_gate.T, w_up.T, w_down, x_norm, x_act.T, dy_gate.T, dy_up.T, dy_down,
            r_gate, r_up, r_down, c_gate, c_up, c_down, hyper_params)
        late_in = lax.ppermute(late, 'col', SWAP)
        ng, nu, nd, dxa, dxn, rgo, ruo, rdo, cgo, cuo, cdo = run_step(
            r_new, c_new, rs, cc, w_gate.T, w_up.T, w_down, gg, gu, gd, a_early, n_cols, late)
        dx_act, dx_norm = run_place(late_in, dxa, dxn)
        return (ng.T, nu.T, nd, rgo, cgo, ruo, cuo, rdo, cdo, dx_norm, dx_act.T)

    return jax.shard_map(body, mesh=mesh, in_specs=in_specs, out_specs=out_specs, check_vma=False)
```

```python
import functools

import jax
import jax.numpy as jnp
from jax import lax
from jax.experimental import pallas as pl
from jax.experimental.pallas import tpu as pltpu
from jax.sharding import PartitionSpec as P

EPS_ONE = 1e-30
EPS_TWO = 1e-3
STEPS = 7
BF16 = jnp.bfloat16
F32 = jnp.float32
MESH = pl.DeviceIdType.MESH
VM = pl.BlockSpec(memory_space=pltpu.VMEM)

HBM = pl.BlockSpec(memory_space=pltpu.HBM)

E_ROWS = 240
Y_COLS = 128
P_SENT = (224, 192, 96)
W_SENT = (528, 288, 512, 112)
A_ROWS = (256, 272, 288, 512, 112)
A_NEEDS = (0, 0, 1, 2, 3)
R_SENT = (256, 272, 288, 112)
CAST_FIRST = 4


def fold(v, width=128):
    acc = v[:, :width]
    for k in range(1, v.shape[1] // width):
        acc = acc + v[:, k * width:(k + 1) * width]
    return acc


def fold_rows(v):
    return jnp.sum(v.reshape(v.shape[0] // 8, 8, v.shape[1]), axis=0)


def lane_total(v):
    s = jnp.sum(jnp.sum(v, axis=0, keepdims=True), axis=1, keepdims=True)
    lane = lax.broadcasted_iota(jnp.int32, (1, 128), 1)
    return jnp.where(lane == 0, jnp.broadcast_to(s, (1, 128)), 0.0)


def column(row_vec):
    return jnp.broadcast_to(row_vec, (128, row_vec.shape[1])).T


def fused(nc, nr, sizes,
          wg, wu, wd, xn, xa, dg, du, dd, rg, ru, rd, cg, cu, cd, hyper,
          gg, gu, gd, ng, nu, nd, n_cols, dxa_early, late, r_hbm, c_hbm,
          xn_v, dd_v, wf_v, dy_v, e_v, ein_v, p_v, pin_v, wb_v, win_v, dxa_v, dxn_v,
          rg_v, ru_v, rd_v, cg_v, cu_v, cd_v, hyp,
          r_mine, r_peer, c_all, s_all, s_mine, s_peer, wsq, wsq_d, rr, cc, racc, cacc, sacc, r_out, c_out, rs_v,
          loc, dsem, esem, qsem, psem, wsem, asem, nsem, rsem, csem, ssem):
    col = lax.axis_index('col')
    row = lax.axis_index('row')
    d_model, d_ff = sizes
    nb = dg.shape[0] // STEPS
    mb = wd.shape[0] // STEPS
    quarter = dd.shape[0] // nr
    others = [(1, 0)] + [(0, dr) for dr in range(1, nr)]

    c_all[row] = jnp.zeros(c_all.shape[1:], F32)
    s_all[row] = jnp.zeros(s_all.shape[1:], F32)

    barrier = pltpu.get_barrier_semaphore()
    for dc, dr in others:
        pl.semaphore_signal(barrier, 1, device_id=(lax.rem(col + dc, nc), lax.rem(row + dr, nr)), device_id_type=MESH)

    loads = [pltpu.make_async_copy(a, b, loc.at[k]) for k, (a, b) in enumerate((
        (wd.at[pl.ds(0, E_ROWS)], wf_v), (dd, dd_v), (xn, xn_v), (rg, rg_v), (ru, ru_v), (rd, rd_v), (cg, cg_v), (cu, cu_v), (cd, cd_v), (hyper, hyp)))]
    for load in loads:
        load.start()
    pl.semaphore_wait(barrier, len(others))

    def remote(src, dst, sems, k, target):
        return pltpu.make_async_remote_copy(src_ref=src, dst_ref=dst, send_sem=sems.at[0, k], recv_sem=sems.at[1, k],
                                            device_id=target, device_id_type=MESH)

    def ranged(src, dst, sems, counts, at=0, to=0):
        copies = []
        for k, n in enumerate(counts):
            copies.append(remote(src.at[pl.ds(at, n)], dst.at[pl.ds(at + to, n)], sems, k, across))
            at += n
        return copies

    across = (1 - col, row)
    chip = (col, lax.rem(row + 2, nr))
    core = (col, row + 1 - 2 * lax.rem(row, 2))
    rows_of = lambda r: pl.ds(pl.multiple_of(r * quarter, quarter), quarter)
    dy_copy = remote(dd.at[rows_of(row)], dy_v.at[rows_of(row)], dsem, 0, across)
    p_copies = ranged(p_v, pin_v, psem, P_SENT)
    w_copies = ranged(wb_v, win_v, wsem, W_SENT, E_ROWS, -E_ROWS)
    a_copies = ranged(dxa_v, dxa_early, asem, R_SENT, E_ROWS)
    split = p_v.shape[0] - Y_COLS
    own_cols = dxn_v.at[:, pl.ds(split, Y_COLS)]
    y_copy = ranged(p_v, pin_v, nsem, (Y_COLS,), split)[0]
    n_copy = remote(own_cols, n_cols, nsem, 1, across)
    e_copy = remote(e_v, ein_v, esem, 0, across)
    e_back = remote(dxa_v.at[pl.ds(0, E_ROWS)], dxa_early.at[pl.ds(0, E_ROWS)], esem, 1, across)
    dims_t = (((1,), (1,)), ((), ()))

    def act_rows(at, n, ready):
        o = lax.dot_general(wb_v[at:at + n, :], dd_v[...], dims_t, preferred_element_type=F32)
        ready()
        o = o + lax.dot_general(win_v[at - E_ROWS:at - E_ROWS + n, :], dy_v[...], dims_t, preferred_element_type=F32)
        dxa_v[at:at + n, :] = o.astype(BF16)

    @pl.when(col == 1)
    def _():
        dy_copy.start()

    by_n = lambda width: pl.BlockSpec((nb, width), lambda k: (k, 0))
    by_m = lambda width: pl.BlockSpec((mb, width), lambda k: (k, 0))

    wsq_d[...] = jnp.zeros_like(wsq_d)

    def cast_body(start, w_b):
        w = w_b[...]
        wsq_d[...] += fold_rows(w * w)
        wb_v[pl.ds(pl.multiple_of((start + pl.program_id(0)) * mb, mb), mb), :] = w.astype(BF16)

    def cast(start, count):
        pltpu.emit_pipeline(functools.partial(cast_body, start), grid=(count,), in_specs=[
            pl.BlockSpec((mb, wd.shape[1]), lambda k: (start + k, 0), pipeline_mode=pl.Buffered(4))])(wd)

    for load in loads[:2]:
        load.wait()
    e_v[...] = lax.dot_general(wf_v[...].astype(BF16), dd_v[...], dims_t, preferred_element_type=F32)

    @pl.when(col == 0)
    def _():
        e_copy.start()

    cast(0, CAST_FIRST)

    @pl.when(col == 1)
    def _():
        w_copies[0].start()

    p_v[...] = jnp.zeros_like(p_v)
    wsq[...] = jnp.zeros_like(wsq)

    def part_body(wg_b, wu_b, dg_b, du_b):
        for k, (w_b, d_b) in enumerate(((wg_b, dg_b), (wu_b, du_b))):
            w = w_b[...]
            wsq[pl.ds(8 * k, 8), :] += fold_rows(w * w)
            p_v[...] += lax.dot_general(w.astype(BF16), d_b[...], (((0,), (0,)), ((), ())), preferred_element_type=F32)

    deep_n = lambda width: pl.BlockSpec((nb, width), lambda k: (k, 0), pipeline_mode=pl.Buffered(3))
    pltpu.emit_pipeline(part_body, grid=(STEPS,), in_specs=[deep_n(wg.shape[1])] * 2 + [deep_n(dg.shape[1])] * 2)(wg, wu, dg, du)

    @pl.when(col == 0)
    def _():
        p_copies[0].start()

    cast(CAST_FIRST, STEPS - CAST_FIRST)

    q_far = remote(dy_v.at[rows_of(row)], dy_v.at[rows_of(row)], qsem, 0, chip)
    q_near = remote(dy_v.at[rows_of(row)], dy_v.at[rows_of(row)], qsem, 1, core)
    q_both = remote(dy_v.at[rows_of(chip[1])], dy_v.at[rows_of(chip[1])], qsem, 2, core)

    @pl.when(col == 0)
    def _():
        dy_copy.wait_recv()
        q_far.start()
        q_near.start()

    for load in loads[2:]:
        load.wait()
    r_mine[...] = jnp.zeros_like(r_mine)
    racc[...] = jnp.zeros_like(racc)
    cacc[...] = jnp.zeros_like(cacc)

    def grad_body(dg_b, du_b, xa_b, gg_b, gu_b, gd_b):
        k = pl.program_id(0)
        for t, (d_b, g_b) in enumerate(((dg_b, gg_b), (du_b, gu_b))):
            g = jnp.dot(d_b[...], xn_v[...], preferred_element_type=F32)
            g_b[...] = g
            q = g * g + EPS_ONE
            racc[pl.ds(8 * t, 8), :] += fold_rows(q)
            c_all[row, pl.ds(7 * t + k, 1), :] = jnp.sum(fold(q).T, axis=0, keepdims=True)
        g = jnp.dot(xa_b[...], dd_v[...], preferred_element_type=F32)
        gd_b[...] = g
        q = g * g + EPS_ONE
        cacc[...] += fold_rows(q)
        r_mine[pl.ds(8 + k, 1), pl.ds(0, 240)] = jnp.sum(fold(q).T, axis=0, keepdims=True)

    pltpu.emit_pipeline(grad_body, grid=(STEPS,), in_specs=[by_n(dg.shape[1])] * 2 + [by_m(xa.shape[1])],
                        out_specs=[by_n(gg.shape[1])] * 2 + [by_m(gd.shape[1])])(dg, du, xa, gg, gu, gd)

    for t in range(2):
        r_mine[t:t + 1, :] = jnp.sum(racc[8 * t:8 * t + 8, :], axis=0, keepdims=True)
    c_down = jnp.sum(cacc[...], axis=0, keepdims=True)
    for k in range(5):
        c_all[row, 14 + k:15 + k, 0:256] = c_down[:, 256 * k:256 * (k + 1)]

    r_copy = remote(r_mine, r_peer, rsem, 0, across)
    r_copy.start()
    c_copies = [pltpu.make_async_remote_copy(
        src_ref=c_all.at[row], dst_ref=c_all.at[row], send_sem=csem.at[0, d], recv_sem=csem.at[1, row],
        device_id=(col, lax.rem(row + d, nr)), device_id_type=MESH) for d in range(1, nr)]
    for c in c_copies:
        c.start()

    @pl.when(col == 0)
    def _():
        p_copies[1].start()
        q_far.wait_recv()
        q_both.start()

        def first_ready():
            w_copies[0].wait_recv()
            q_near.wait_recv()
            q_both.wait_recv()
            q_far.wait_send()
            q_near.wait_send()
            q_both.wait_send()

        act_rows(E_ROWS, A_ROWS[0], first_ready)

    @pl.when(col == 1)
    def _():
        w_copies[1].start()
        e_copy.wait_recv()
        dxa_v[0:E_ROWS, :] = (e_v[...] + ein_v[...]).astype(BF16)

    beta = hyp[0]
    rr[...] = jnp.ones_like(rr)
    rr[0:1, :] = rg_v[...].reshape(1, -1)
    rr[1:2, :] = ru_v[...].reshape(1, -1)
    r_old, g_old, u_old, d_old = [v[...].reshape(1, -1) for v in (rd_v, cg_v, cu_v, cd_v)]
    for k in range(STEPS):
        cc[k:k + 1, :] = g_old[:, nb * k:nb * (k + 1)]
        cc[7 + k:8 + k, :] = u_old[:, nb * k:nb * (k + 1)]
        rr[8 + k:9 + k, 0:mb] = r_old[:, mb * k:mb * (k + 1)]
    for k in range(5):
        cc[14 + k:15 + k, 0:256] = d_old[:, 256 * k:256 * (k + 1)]
        cc[14 + k:15 + k, 256:480] = jnp.ones((1, 224), F32)
    cc[19:24, :] = jnp.ones((5, 480), F32)

    r_copy.wait()
    for d in range(1, nr):
        c_copies[d - 1].wait_send()
        s = lax.rem(row + d, nr)
        pltpu.make_async_remote_copy(src_ref=c_all.at[s], dst_ref=c_all.at[s], send_sem=csem.at[0, d], recv_sem=csem.at[1, s],
                                     device_id=(col, s), device_id_type=MESH).wait_recv()

    line = lax.broadcasted_iota(jnp.int32, rr.shape, 0)
    r_new = beta * rr[...] + (1.0 - beta) * ((r_mine[...] + r_peer[...]) / jnp.where(line < 8, float(d_ff), float(d_model)))
    line = lax.broadcasted_iota(jnp.int32, cc.shape, 0)
    c_sum = (c_all[0] + c_all[1]) + (c_all[2] + c_all[3])
    c_new = beta * cc[...] + (1.0 - beta) * (c_sum / jnp.where(line < 14, float(d_model), float(d_ff)))
    r_out[...] = r_new
    c_out[...] = c_new
    rr[...] = lax.rsqrt(r_new)
    cc[...] = lax.rsqrt(c_new)
    save_r = pltpu.make_async_copy(r_out, r_hbm, loc.at[12])
    save_c = pltpu.make_async_copy(c_out, c_hbm, loc.at[13])

    sacc[...] = jnp.zeros_like(sacc)

    def square_body(gg_b, gu_b, gd_b):
        k = pl.program_id(0)
        for t, g_b in enumerate((gg_b, gu_b)):
            u = g_b[...] * rr[t:t + 1, :]
            s = fold(u * u)
            c = column(cc[pl.ds(7 * t + k, 1), :])
            sacc[pl.ds(8 * t, 8), :] += fold_rows(s * (c * c))
        c_row = jnp.concatenate([cc[14 + j:15 + j, 0:256] for j in range(5)], axis=1)
        u = gd_b[...] * c_row
        s = fold(u * u)
        r = column(rr[pl.ds(8 + k, 1), :])[0:mb]
        sacc[16:24, :] += fold_rows(s * (r * r))

    pltpu.emit_pipeline(square_body, grid=(STEPS,), in_specs=[by_n(gg.shape[1])] * 2 + [by_m(gd.shape[1])])(gg, gu, gd)

    for t in range(3):
        s_all[row, t:t + 1, :] = jnp.sum(sacc[8 * t:8 * t + 8, :], axis=0, keepdims=True)
    for t in range(2):
        s_all[row, 3 + t:4 + t, :] = jnp.sum(fold(wsq[8 * t:8 * t + 8, :]), axis=0, keepdims=True)
        s_all[row, 6 + t:7 + t, :] = lane_total(r_new[t:t + 1, :])
    s_all[row, 5:6, :] = jnp.sum(fold(wsq_d[...]), axis=0, keepdims=True)
    s_all[row, 8:9, :] = lane_total(r_new[8:15, 0:mb])
    s_copies = [pltpu.make_async_remote_copy(
        src_ref=s_all.at[row], dst_ref=s_all.at[row], send_sem=ssem.at[0, d], recv_sem=ssem.at[1, row],
        device_id=(col, lax.rem(row + d, nr)), device_id_type=MESH) for d in range(1, nr)]
    for s in s_copies:
        s.start()
    for d in range(1, nr):
        s_copies[d - 1].wait_send()
        him = lax.rem(row + d, nr)
        pltpu.make_async_remote_copy(src_ref=s_all.at[him], dst_ref=s_all.at[him], send_sem=ssem.at[0, d],
                                     recv_sem=ssem.at[1, him], device_id=(col, him), device_id_type=MESH).wait_recv()
    s_mine[...] = (s_all[0] + s_all[1]) + (s_all[2] + s_all[3])
    s_copy = remote(s_mine, s_peer, ssem, nr, across)
    s_copy.start()

    @pl.when(col == 0)
    def _():
        p_copies[2].start()
        a_copies[0].start()

    @pl.when(col == 1)
    def _():
        y_copy.start()
        for w in w_copies[2:]:
            w.start()
        e_back.start()

    s_copy.wait()
    total = s_mine[...] + s_peer[...]
    sums = jnp.sum(total, axis=1, keepdims=True)
    scales = []
    for t, (m, n) in enumerate(((d_model, d_ff), (d_model, d_ff), (d_ff, d_model))):
        r_mean = sums[6 + t:7 + t] / float(m * nc)
        rms_u = jnp.sqrt(sums[t:t + 1] * r_mean / float(m * n))
        step = hyp[1] * jnp.maximum(EPS_TWO, jnp.sqrt(sums[3 + t:4 + t] / float(m * n)))
        scales.append(step * jnp.sqrt(r_mean) / jnp.maximum(1.0, rms_u / hyp[2]))
    rs_v[...] = rr[...]
    rs_v[0:1, :] = rr[0:1, :] * scales[0]
    rs_v[1:2, :] = rr[1:2, :] * scales[1]
    rs_v[8:16, :] = rr[8:16, :] * scales[2]
    save_stats = (save_r, save_c)
    for c in save_stats:
        c.start()

    def wide_body(wg_b, wu_b, gg_b, gu_b, ng_b, nu_b):
        k = pl.program_id(0)
        for t, (w, g, o) in enumerate(((wg_b, gg_b, ng_b), (wu_b, gu_b, nu_b))):
            c = column(cc[pl.ds(7 * t + k, 1), :])
            for j in range(w.shape[1] // 128):
                lanes = slice(128 * j, 128 * (j + 1))
                o[:, lanes] = w[:, lanes] - g[:, lanes] * rs_v[t:t + 1, lanes] * c

    def down_body(w, g, o):
        r = column(rs_v[pl.ds(8 + pl.program_id(0), 1), :])[0:mb]
        for j in range(w.shape[1] // 128):
            lanes = slice(128 * j, 128 * (j + 1))
            c = cc[14 + j // 2:15 + j // 2, 128 * (j % 2):128 * (j % 2 + 1)]
            o[:, lanes] = w[:, lanes] - g[:, lanes] * c * r

    early = E_ROWS + sum(R_SENT)
    rows_a, half = dxa_v.shape[0], dxn_v.shape[0] // 2
    save_e = pltpu.make_async_copy(dxa_v.at[pl.ds(0, E_ROWS)], dxa_early.at[pl.ds(0, E_ROWS)], loc.at[10])
    save_a = pltpu.make_async_copy(dxa_v.at[pl.ds(E_ROWS, early - E_ROWS)], dxa_early.at[pl.ds(E_ROWS, early - E_ROWS)], loc.at[10])
    save_late = pltpu.make_async_copy(dxa_v.at[pl.ds(early, rows_a - early)], late, loc.at[11])
    save_y = pltpu.make_async_copy(own_cols, n_cols, loc.at[16])
    save_pack = [pltpu.make_async_copy(a, b, loc.at[16 + k]) for k, (a, b) in enumerate((
        (dxn_v.at[pl.ds(0, half), pl.ds(0, split)], late.at[pl.ds(0, half), pl.ds(0, split)]),
        (dxn_v.at[pl.ds(half, half), pl.ds(0, split)], late.at[pl.ds(0, half), pl.ds(split, split)])))]

    def norm_columns(start, stop):
        for j in range(start, stop, 128):
            dxn_v[:, j:j + 128] = (p_v[j:j + 128, :] + pin_v[j:j + 128, :]).T.astype(BF16)

    def act_chunk(k):
        new = A_NEEDS[k] != A_NEEDS[k - 1]
        act_rows(E_ROWS + sum(A_ROWS[:k]), A_ROWS[k], w_copies[A_NEEDS[k]].wait_recv if new else lambda: None)
        if k < len(R_SENT):
            a_copies[k].start()

    @pl.when(col == 0)
    def _():
        act_chunk(1)

    pltpu.emit_pipeline(wide_body, grid=(STEPS,), in_specs=[by_n(wg.shape[1])] * 4,
                        out_specs=[by_n(wg.shape[1])] * 2)(wg, wu, gg, gu, ng, nu)

    @pl.when(col == 0)
    def _():
        y_copy.wait_recv()
        norm_columns(split, split + Y_COLS)
        n_copy.start()
        save_y.start()
        act_chunk(2)

    @pl.when(col == 1)
    def _():
        save_e.start()
        for p in p_copies:
            p.wait_recv()
        norm_columns(0, split)
        for c in save_pack:
            c.start()

    pltpu.emit_pipeline(down_body, grid=(STEPS,), in_specs=[by_m(wd.shape[1])] * 2,
                        out_specs=[by_m(wd.shape[1])])(wd, gd, nd)

    @pl.when(col == 0)
    def _():
        act_chunk(3)
        save_a.start()
        act_chunk(4)
        save_late.start()
        e_copy.wait_send()
        for p in p_copies:
            p.wait_send()
        n_copy.wait_send()
        save_a.wait()
        save_y.wait()
        save_late.wait()
        e_back.wait_recv()
        for a in a_copies:
            a.wait_send()

    @pl.when(col == 1)
    def _():
        save_e.wait()
        for c in save_pack:
            c.wait()
        dy_copy.wait_send()
        y_copy.wait_send()
        for w in w_copies:
            w.wait_send()
        e_back.wait_send()
        n_copy.wait_recv()
        for a in a_copies:
            a.wait_recv()

    for c in save_stats:
        c.wait()


def run_fused(nc, nr, sizes, wg, wu, wd, xn, xa, dg, du, dd, rg, ru, rd, cg, cu, cd, hyper):
    f32, b16 = (lambda *s: jax.ShapeDtypeStruct(s, F32)), (lambda *s: jax.ShapeDtypeStruct(s, BF16))
    n, i = wg.shape
    m, h = wd.shape
    t = dd.shape[0]
    early = E_ROWS + sum(R_SENT)
    dma = lambda *s: pltpu.SemaphoreType.DMA(s)
    vf = lambda *s: pltpu.VMEM(s, F32)
    vb = lambda *s: pltpu.VMEM(s, BF16)
    return pl.pallas_call(
        functools.partial(fused, nc, nr, sizes),
        out_shape=(f32(n, i), f32(n, i), f32(m, h), f32(n, i), f32(n, i), f32(m, h), b16(t, Y_COLS), b16(early, t), b16(m - early, t),
                   f32(16, 640), f32(24, 480)),
        in_specs=[HBM] * 15,
        out_specs=[HBM] * 11,
        scratch_shapes=[
            vb(*xn.shape), vb(t, h), vf(E_ROWS, h), vb(t, h), vf(E_ROWS, t), vf(E_ROWS, t), vf(i, t), vf(i, t), vb(m, h), vb(m - E_ROWS, h),
            vb(m, t), vb(t, i),
            vf(i), vf(i), vf(m), vf(n), vf(n), vf(h), pltpu.SMEM((3,), F32),
            vf(16, 640), vf(16, 640), vf(nr, 24, 480), vf(nr, 16, 128), vf(16, 128), vf(16, 128), vf(16, i), vf(8, h),
            vf(16, 640), vf(24, 480), vf(16, i), vf(8, h), vf(24, 128),
            vf(16, 640), vf(24, 480), vf(16, 640),
            dma(19), dma(2, 1), dma(2, 2), dma(2, 3), dma(2, len(P_SENT)), dma(2, len(W_SENT)), dma(2, len(R_SENT)), dma(2, 2), dma(2, 1),
            dma(2, nr), dma(2, nr + 1)],
        compiler_params=pltpu.CompilerParams(collective_id=0, has_side_effects=True, vmem_limit_bytes=60 * 1024 * 1024),
        cost_estimate=pl.CostEstimate(flops=22_000_000_000, bytes_accessed=150_000_000, transcendentals=0),
        name="fused",
    )(wg, wu, wd, xn, xa, dg, du, dd, rg, ru, rd, cg, cu, cd, hyper)


def placements(col, buf, a_out, n_out, sending):
    half, split = n_out.shape[0] // 2, n_out.shape[1] - Y_COLS
    rows = a_out.shape[0] - buf.shape[0]
    act = [(buf, a_out.at[pl.ds(rows, buf.shape[0])])]
    norm = [(buf.at[pl.ds(0, half), pl.ds(0, split)], n_out.at[pl.ds(0, half), pl.ds(0, split)]),
            (buf.at[pl.ds(0, half), pl.ds(split, split)], n_out.at[pl.ds(half, half), pl.ds(0, split)])]
    return (act, norm) if sending else (norm, act)


def per_side(col, choices, sem, at, action):
    for side, pairs in enumerate(choices):
        @pl.when(col == side)
        def _(pairs=pairs):
            for j, (a, b) in enumerate(pairs):
                action(pltpu.make_async_copy(a, b, sem.at[at + j]))


def publish_kernel(r_hbm, c_hbm, wg, wu, wd, a_in, n_in, l_in, ng, nu, nd, a_out, n_out,
                   rgo, ruo, rdo, cgo, cuo, cdo, r_new, c_new, a_v, n_v, l_v, sem):
    k = pl.program_id(0)
    col = lax.axis_index('col')
    mb = wd.shape[0]
    cols = n_v.shape[1]
    pairs = ((r_hbm, r_new), (c_hbm, c_new), (a_in, a_v), (n_in, n_v), (l_in, l_v),
             (a_v, a_out.at[pl.ds(0, a_v.shape[0])]), (n_v, n_out.at[:, pl.ds(n_out.shape[1] - cols, cols)]))
    copies = [pltpu.make_async_copy(a, b, sem.at[j]) for j, (a, b) in enumerate(pairs)]
    own = placements(col, l_v, a_out, n_out, True)

    @pl.when(k == 0)
    def _():
        for c in copies[:5]:
            c.start()

    @pl.when(k == 1)
    def _():
        for c in copies[:5]:
            c.wait()
        for c in copies[5:]:
            c.start()
        per_side(col, own, sem, len(pairs), lambda c: c.start())
        rgo[...] = r_new[0:1, :].reshape(-1)
        ruo[...] = r_new[1:2, :].reshape(-1)
        rdo[...] = jnp.concatenate([r_new[8 + j:9 + j, 0:mb] for j in range(STEPS)], axis=1).reshape(-1)
        cgo[...] = jnp.concatenate([c_new[j:j + 1, :] for j in range(STEPS)], axis=1).reshape(-1)
        cuo[...] = jnp.concatenate([c_new[7 + j:8 + j, :] for j in range(STEPS)], axis=1).reshape(-1)
        cdo[...] = jnp.concatenate([c_new[14 + j:15 + j, 0:256] for j in range(5)], axis=1).reshape(-1)

    @pl.when(k == STEPS - 1)
    def _():
        for c in copies[5:]:
            c.wait()
        per_side(col, own, sem, len(pairs), lambda c: c.wait())

    ng[...] = wg[...]
    nu[...] = wu[...]
    nd[...] = wd[...]


def run_publish(r_new, c_new, wg, wu, wd, a_early, n_cols, late):
    f32 = lambda *s: jax.ShapeDtypeStruct(s, F32)
    b16 = lambda *s: jax.ShapeDtypeStruct(s, BF16)
    n, i = wg.shape
    m, h = wd.shape
    t = n_cols.shape[0]
    flat = lambda s: pl.BlockSpec((s,), lambda k: (0,))
    by_n = pl.BlockSpec((n // STEPS, i), lambda k: (k, 0))
    by_m = pl.BlockSpec((m // STEPS, h), lambda k: (k, 0))
    return pl.pallas_call(
        publish_kernel, grid=(STEPS,),
        out_shape=(f32(n, i), f32(n, i), f32(m, h), b16(m, t), b16(t, i), f32(i), f32(i), f32(m), f32(n), f32(n), f32(h)),
        in_specs=[HBM] * 2 + [by_n, by_n, by_m] + [HBM] * 3,
        out_specs=[by_n, by_n, by_m, HBM, HBM] + [flat(s) for s in (i, i, m, n, n, h)],
        scratch_shapes=[pltpu.VMEM(a.shape, a.dtype) for a in (r_new, c_new, a_early, n_cols, late)] + [
            pltpu.SemaphoreType.DMA((10,))],
        compiler_params=pltpu.CompilerParams(vmem_limit_bytes=60 * 1024 * 1024),
        cost_estimate=pl.CostEstimate(flops=20_000_000_000, bytes_accessed=58_000_000, transcendentals=0),
        name="publish",
    )(r_new, c_new, wg, wu, wd, a_early, n_cols, late)


def place_kernel(late_in, a_in, n_in, a_out, n_out, sem):
    col = lax.axis_index('col')
    got = placements(col, late_in, a_out, n_out, False)
    per_side(col, got, sem, 0, lambda c: c.start())
    per_side(col, got, sem, 0, lambda c: c.wait())


def run_place(late_in, dxa, dxn):
    return pl.pallas_call(
        place_kernel,
        out_shape=(jax.ShapeDtypeStruct(dxa.shape, BF16), jax.ShapeDtypeStruct(dxn.shape, BF16)),
        in_specs=[pl.BlockSpec(memory_space=pl.ANY), HBM, HBM], out_specs=[HBM, HBM], input_output_aliases={1: 0, 2: 1},
        scratch_shapes=[pltpu.SemaphoreType.DMA((3,))],
        compiler_params=pltpu.CompilerParams(vmem_limit_bytes=1024 * 1024),
        name="place",
    )(late_in, dxa, dxn)


SWAP = [(0, 1), (1, 0)]


def solution(mesh):
    row_size = mesh.shape['row']
    col_size = mesh.shape['col']
    weight_spec = P('row', 'col')
    act_spec = P(None, 'row')
    grad_spec = P(None, 'col')
    in_specs = (weight_spec,) * 3 + (act_spec, act_spec) + (grad_spec,) * 3 + (P('row'), P('col')) * 3 + (P(),)
    out_specs = (weight_spec,) * 3 + (P('row'), P('col')) * 3 + (act_spec, act_spec)

    def body(w_gate, w_up, w_down, x_norm, x_act, dy_gate, dy_up, dy_down, r_gate, c_gate, r_up, c_up, r_down, c_down, hyper_params):
        d_model = w_gate.shape[0] * row_size
        d_ff = w_gate.shape[1] * col_size
        _, _, _, ng, nu, nd, n_cols, a_early, late, r_new, c_new = run_fused(
            col_size, row_size, (d_model, d_ff),
            w_gate.T, w_up.T, w_down, x_norm, x_act.T, dy_gate.T, dy_up.T, dy_down,
            r_gate, r_up, r_down, c_gate, c_up, c_down, hyper_params)
        late_in = lax.ppermute(late, 'col', SWAP)
        ng, nu, nd, dxa, dxn, rgo, ruo, rdo, cgo, cuo, cdo = run_publish(r_new, c_new, ng, nu, nd, a_early, n_cols, late)
        dx_act, dx_norm = run_place(late_in, dxa, dxn)
        return (ng.T, nu.T, nd, rgo, cgo, ruo, cuo, rdo, cdo, dx_norm, dx_act.T)

    return jax.shard_map(body, mesh=mesh, in_specs=in_specs, out_specs=out_specs, check_vma=False)
```

```python
import functools

import jax
import jax.numpy as jnp
from jax import lax
from jax.experimental import pallas as pl
from jax.experimental.pallas import tpu as pltpu
from jax.sharding import PartitionSpec as P

EPS_ONE = 1e-30
EPS_TWO = 1e-3
STEPS = 7
BF16 = jnp.bfloat16
F32 = jnp.float32
MESH = pl.DeviceIdType.MESH
VM = pl.BlockSpec(memory_space=pltpu.VMEM)

HBM = pl.BlockSpec(memory_space=pltpu.HBM)

E_ROWS = 112
P_FIRST = 256
P_SENT = (256, 176, 176, 32)
W_SENT = (592, 304, 560, 112)
A_ROWS = (304, 288, 304, 560, 112)
A_NEEDS = (0, 0, 1, 2, 3)
R_SENT = (304, 288, 304, 32)
CAST_FIRST = 4


def fold(v, width=128):
    acc = v[:, :width]
    for k in range(1, v.shape[1] // width):
        acc = acc + v[:, k * width:(k + 1) * width]
    return acc


def fold_rows(v):
    return jnp.sum(v.reshape(v.shape[0] // 8, 8, v.shape[1]), axis=0)


def lane_total(v):
    s = jnp.sum(jnp.sum(v, axis=0, keepdims=True), axis=1, keepdims=True)
    lane = lax.broadcasted_iota(jnp.int32, (1, 128), 1)
    return jnp.where(lane == 0, jnp.broadcast_to(s, (1, 128)), 0.0)


def column(row_vec):
    return jnp.broadcast_to(row_vec, (128, row_vec.shape[1])).T


def norm_pairs(norm, buf):
    t, i = norm.shape
    half, wide, last = t // 2, i - 128, t // 2
    pairs = [(norm.at[pl.ds(0, half), pl.ds(0, wide)], buf.at[pl.ds(0, half), pl.ds(0, wide)]),
             (norm.at[pl.ds(half, half), pl.ds(0, wide)], buf.at[pl.ds(0, half), pl.ds(wide, wide)])]
    for b in range(t // 128):
        pairs.append((norm.at[pl.ds(128 * b, 128), pl.ds(wide, 128)], buf.at[pl.ds(last, 128), pl.ds(128 * b, 128)]))
    return pairs


def fused(nc, nr, sizes,
          wg, wu, wd, xn, xa, dg, du, dd, rg, ru, rd, cg, cu, cd, hyper,
          gg, gu, gd, ng, nu, nd, dxa_early, late, r_hbm, c_hbm,
          xn_v, dd_v, wf_v, dy_v, e_v, ein_v, p_v, pin_v, wb_v, win_v, dxa_v, dxn_v,
          rg_v, ru_v, rd_v, cg_v, cu_v, cd_v, hyp,
          r_mine, r_peer, c_all, s_all, s_mine, s_peer, wsq, wsq_d, rr, cc, racc, cacc, sacc, r_out, c_out, rs_v,
          loc, dsem, esem, qsem, psem, wsem, asem, rsem, csem, ssem):
    col = lax.axis_index('col')
    row = lax.axis_index('row')
    d_model, d_ff = sizes
    nb = dg.shape[0] // STEPS
    mb = wd.shape[0] // STEPS
    quarter = dd.shape[0] // nr
    others = [(1, 0)] + [(0, dr) for dr in range(1, nr)]

    c_all[row] = jnp.zeros(c_all.shape[1:], F32)
    s_all[row] = jnp.zeros(s_all.shape[1:], F32)

    barrier = pltpu.get_barrier_semaphore()
    for dc, dr in others:
        pl.semaphore_signal(barrier, 1, device_id=(lax.rem(col + dc, nc), lax.rem(row + dr, nr)), device_id_type=MESH)

    loads = [pltpu.make_async_copy(a, b, loc.at[k]) for k, (a, b) in enumerate((
        (wd.at[pl.ds(0, E_ROWS)], wf_v), (dd, dd_v), (xn, xn_v), (rg, rg_v), (ru, ru_v), (rd, rd_v), (cg, cg_v), (cu, cu_v), (cd, cd_v), (hyper, hyp)))]
    for load in loads:
        load.start()

    def first_partial():
        for load in loads[:2]:
            load.wait()
        e_v[...] = lax.dot_general(wf_v[...].astype(BF16), dd_v[...], (((1,), (1,)), ((), ())), preferred_element_type=F32)

    @pl.when(col == 0)
    def _():
        first_partial()

    pl.semaphore_wait(barrier, len(others))

    def remote(src, dst, sems, k, target):
        return pltpu.make_async_remote_copy(src_ref=src, dst_ref=dst, send_sem=sems.at[0, k], recv_sem=sems.at[1, k],
                                            device_id=target, device_id_type=MESH)

    def ranged(src, dst, sems, counts, at=0, to=0):
        copies = []
        for k, n in enumerate(counts):
            copies.append(remote(src.at[pl.ds(at, n)], dst.at[pl.ds(at + to, n)], sems, k, across))
            at += n
        return copies

    across = (1 - col, row)
    chip = (col, lax.rem(row + 2, nr))
    core = (col, row + 1 - 2 * lax.rem(row, 2))
    rows_of = lambda r: pl.ds(pl.multiple_of(r * quarter, quarter), quarter)
    dy_copy = remote(dd.at[rows_of(row)], dy_v.at[rows_of(row)], dsem, 0, across)
    p_copies = ranged(p_v, pin_v, psem, P_SENT)
    w_copies = ranged(wb_v, win_v, wsem, W_SENT, E_ROWS, -E_ROWS)
    a_copies = ranged(dxa_v, dxa_early, asem, R_SENT, E_ROWS)
    e_copy = remote(e_v, ein_v, esem, 0, across)
    e_back = remote(dxa_v.at[pl.ds(0, E_ROWS)], dxa_early.at[pl.ds(0, E_ROWS)], esem, 1, across)
    dims_t = (((1,), (1,)), ((), ()))

    def act_rows(at, n, ready):
        o = lax.dot_general(wb_v[at:at + n, :], dd_v[...], dims_t, preferred_element_type=F32)
        ready()
        o = o + lax.dot_general(win_v[at - E_ROWS:at - E_ROWS + n, :], dy_v[...], dims_t, preferred_element_type=F32)
        dxa_v[at:at + n, :] = o.astype(BF16)

    @pl.when(col == 0)
    def _():
        e_copy.start()

    @pl.when(col == 1)
    def _():
        dy_copy.start()
        first_partial()

    by_n = lambda width: pl.BlockSpec((nb, width), lambda k: (k, 0))
    by_m = lambda width: pl.BlockSpec((mb, width), lambda k: (k, 0))

    wsq_d[...] = jnp.zeros_like(wsq_d)

    def cast_body(start, w_b):
        w = w_b[...]
        wsq_d[...] += fold_rows(w * w)
        wb_v[pl.ds(pl.multiple_of((start + pl.program_id(0)) * mb, mb), mb), :] = w.astype(BF16)

    def cast(start, count):
        pltpu.emit_pipeline(functools.partial(cast_body, start), grid=(count,), in_specs=[
            pl.BlockSpec((mb, wd.shape[1]), lambda k: (start + k, 0), pipeline_mode=pl.Buffered(4))])(wd)

    p_v[...] = jnp.zeros_like(p_v)
    wsq[...] = jnp.zeros_like(wsq)

    def part_body(start, wg_b, wu_b, dg_b, du_b):
        rows = slice(start, start + wg_b.shape[1])
        for k, (w_b, d_b) in enumerate(((wg_b, dg_b), (wu_b, du_b))):
            w = w_b[...]
            wsq[8 * k:8 * k + 8, rows] += fold_rows(w * w)
            p_v[rows, :] += lax.dot_general(w.astype(BF16), d_b[...], (((0,), (0,)), ((), ())), preferred_element_type=F32)

    def partial_rows(start, count):
        deep_n = lambda width: pl.BlockSpec((nb, width), lambda k: (k, 0), pipeline_mode=pl.Buffered(3))
        cols = pl.ds(start, count)
        pltpu.emit_pipeline(functools.partial(part_body, start), grid=(STEPS,),
                            in_specs=[deep_n(count)] * 2 + [deep_n(dg.shape[1])] * 2)(wg.at[:, cols], wu.at[:, cols], dg, du)

    partial_rows(0, P_FIRST)

    @pl.when(col == 0)
    def _():
        p_copies[0].start()

    cast(0, CAST_FIRST)

    @pl.when(col == 1)
    def _():
        w_copies[0].start()

    partial_rows(P_FIRST, wg.shape[1] - P_FIRST)

    @pl.when(col == 0)
    def _():
        p_copies[1].start()

    cast(CAST_FIRST, STEPS - CAST_FIRST)

    q_far = remote(dy_v.at[rows_of(row)], dy_v.at[rows_of(row)], qsem, 0, chip)
    q_near = remote(dy_v.at[rows_of(row)], dy_v.at[rows_of(row)], qsem, 1, core)
    q_both = remote(dy_v.at[rows_of(chip[1])], dy_v.at[rows_of(chip[1])], qsem, 2, core)

    @pl.when(col == 0)
    def _():
        dy_copy.wait_recv()
        q_far.start()
        q_near.start()

    for load in loads[2:]:
        load.wait()
    r_mine[...] = jnp.zeros_like(r_mine)
    racc[...] = jnp.zeros_like(racc)
    cacc[...] = jnp.zeros_like(cacc)

    def grad_body(dg_b, du_b, xa_b, gg_b, gu_b, gd_b):
        k = pl.program_id(0)
        for t, (d_b, g_b) in enumerate(((dg_b, gg_b), (du_b, gu_b))):
            g = jnp.dot(d_b[...], xn_v[...], preferred_element_type=F32)
            g_b[...] = g
            q = g * g + EPS_ONE
            racc[pl.ds(8 * t, 8), :] += fold_rows(q)
            c_all[row, pl.ds(7 * t + k, 1), :] = jnp.sum(fold(q).T, axis=0, keepdims=True)
        g = jnp.dot(xa_b[...], dd_v[...], preferred_element_type=F32)
        gd_b[...] = g
        q = g * g + EPS_ONE
        cacc[...] += fold_rows(q)
        r_mine[pl.ds(8 + k, 1), pl.ds(0, 240)] = jnp.sum(fold(q).T, axis=0, keepdims=True)

    pltpu.emit_pipeline(grad_body, grid=(STEPS,), in_specs=[by_n(dg.shape[1])] * 2 + [by_m(xa.shape[1])],
                        out_specs=[by_n(gg.shape[1])] * 2 + [by_m(gd.shape[1])])(dg, du, xa, gg, gu, gd)

    for t in range(2):
        r_mine[t:t + 1, :] = jnp.sum(racc[8 * t:8 * t + 8, :], axis=0, keepdims=True)
    c_down = jnp.sum(cacc[...], axis=0, keepdims=True)
    for k in range(5):
        c_all[row, 14 + k:15 + k, 0:256] = c_down[:, 256 * k:256 * (k + 1)]

    r_copy = remote(r_mine, r_peer, rsem, 0, across)
    r_copy.start()
    c_copies = [pltpu.make_async_remote_copy(
        src_ref=c_all.at[row], dst_ref=c_all.at[row], send_sem=csem.at[0, d], recv_sem=csem.at[1, row],
        device_id=(col, lax.rem(row + d, nr)), device_id_type=MESH) for d in range(1, nr)]
    for c in c_copies:
        c.start()

    @pl.when(col == 0)
    def _():
        p_copies[2].start()
        q_far.wait_recv()
        q_both.start()

        def first_ready():
            w_copies[0].wait_recv()
            q_near.wait_recv()
            q_both.wait_recv()
            q_far.wait_send()
            q_near.wait_send()
            q_both.wait_send()

        act_rows(E_ROWS, A_ROWS[0], first_ready)

    @pl.when(col == 1)
    def _():
        w_copies[1].start()
        e_copy.wait_recv()
        dxa_v[0:E_ROWS, :] = (e_v[...] + ein_v[...]).astype(BF16)

    beta = hyp[0]
    rr[...] = jnp.ones_like(rr)
    rr[0:1, :] = rg_v[...].reshape(1, -1)
    rr[1:2, :] = ru_v[...].reshape(1, -1)
    r_old, g_old, u_old, d_old = [v[...].reshape(1, -1) for v in (rd_v, cg_v, cu_v, cd_v)]
    for k in range(STEPS):
        cc[k:k + 1, :] = g_old[:, nb * k:nb * (k + 1)]
        cc[7 + k:8 + k, :] = u_old[:, nb * k:nb * (k + 1)]
        rr[8 + k:9 + k, 0:mb] = r_old[:, mb * k:mb * (k + 1)]
    for k in range(5):
        cc[14 + k:15 + k, 0:256] = d_old[:, 256 * k:256 * (k + 1)]
        cc[14 + k:15 + k, 256:480] = jnp.ones((1, 224), F32)
    cc[19:24, :] = jnp.ones((5, 480), F32)

    r_copy.wait()
    for d in range(1, nr):
        c_copies[d - 1].wait_send()
        s = lax.rem(row + d, nr)
        pltpu.make_async_remote_copy(src_ref=c_all.at[s], dst_ref=c_all.at[s], send_sem=csem.at[0, d], recv_sem=csem.at[1, s],
                                     device_id=(col, s), device_id_type=MESH).wait_recv()

    line = lax.broadcasted_iota(jnp.int32, rr.shape, 0)
    r_new = beta * rr[...] + (1.0 - beta) * ((r_mine[...] + r_peer[...]) / jnp.where(line < 8, float(d_ff), float(d_model)))
    line = lax.broadcasted_iota(jnp.int32, cc.shape, 0)
    c_sum = (c_all[0] + c_all[1]) + (c_all[2] + c_all[3])
    c_new = beta * cc[...] + (1.0 - beta) * (c_sum / jnp.where(line < 14, float(d_model), float(d_ff)))
    r_out[...] = r_new
    c_out[...] = c_new
    rr[...] = lax.rsqrt(r_new)
    cc[...] = lax.rsqrt(c_new)
    save_r = pltpu.make_async_copy(r_out, r_hbm, loc.at[12])
    save_c = pltpu.make_async_copy(c_out, c_hbm, loc.at[13])

    sacc[...] = jnp.zeros_like(sacc)

    def square_body(gg_b, gu_b, gd_b):
        k = pl.program_id(0)
        for t, g_b in enumerate((gg_b, gu_b)):
            u = g_b[...] * rr[t:t + 1, :]
            s = fold(u * u)
            c = column(cc[pl.ds(7 * t + k, 1), :])
            sacc[pl.ds(8 * t, 8), :] += fold_rows(s * (c * c))
        c_row = jnp.concatenate([cc[14 + j:15 + j, 0:256] for j in range(5)], axis=1)
        u = gd_b[...] * c_row
        s = fold(u * u)
        r = column(rr[pl.ds(8 + k, 1), :])[0:mb]
        sacc[16:24, :] += fold_rows(s * (r * r))

    pltpu.emit_pipeline(square_body, grid=(STEPS,), in_specs=[by_n(gg.shape[1])] * 2 + [by_m(gd.shape[1])])(gg, gu, gd)

    for t in range(3):
        s_all[row, t:t + 1, :] = jnp.sum(sacc[8 * t:8 * t + 8, :], axis=0, keepdims=True)
    for t in range(2):
        s_all[row, 3 + t:4 + t, :] = jnp.sum(fold(wsq[8 * t:8 * t + 8, :]), axis=0, keepdims=True)
        s_all[row, 6 + t:7 + t, :] = lane_total(r_new[t:t + 1, :])
    s_all[row, 5:6, :] = jnp.sum(fold(wsq_d[...]), axis=0, keepdims=True)
    s_all[row, 8:9, :] = lane_total(r_new[8:15, 0:mb])
    s_copies = [pltpu.make_async_remote_copy(
        src_ref=s_all.at[row], dst_ref=s_all.at[row], send_sem=ssem.at[0, d], recv_sem=ssem.at[1, row],
        device_id=(col, lax.rem(row + d, nr)), device_id_type=MESH) for d in range(1, nr)]
    for s in s_copies:
        s.start()
    for d in range(1, nr):
        s_copies[d - 1].wait_send()
        him = lax.rem(row + d, nr)
        pltpu.make_async_remote_copy(src_ref=s_all.at[him], dst_ref=s_all.at[him], send_sem=ssem.at[0, d],
                                     recv_sem=ssem.at[1, him], device_id=(col, him), device_id_type=MESH).wait_recv()
    s_mine[...] = (s_all[0] + s_all[1]) + (s_all[2] + s_all[3])
    s_copy = remote(s_mine, s_peer, ssem, nr, across)
    s_copy.start()

    @pl.when(col == 0)
    def _():
        p_copies[3].start()
        a_copies[0].start()

    @pl.when(col == 1)
    def _():
        for w in w_copies[2:]:
            w.start()
        e_back.start()

    s_copy.wait()
    total = s_mine[...] + s_peer[...]
    sums = jnp.sum(total, axis=1, keepdims=True)
    scales = []
    for t, (m, n) in enumerate(((d_model, d_ff), (d_model, d_ff), (d_ff, d_model))):
        r_mean = sums[6 + t:7 + t] / float(m * nc)
        rms_u = jnp.sqrt(sums[t:t + 1] * r_mean / float(m * n))
        step = hyp[1] * jnp.maximum(EPS_TWO, jnp.sqrt(sums[3 + t:4 + t] / float(m * n)))
        scales.append(step * jnp.sqrt(r_mean) / jnp.maximum(1.0, rms_u / hyp[2]))
    rs_v[...] = rr[...]
    rs_v[0:1, :] = rr[0:1, :] * scales[0]
    rs_v[1:2, :] = rr[1:2, :] * scales[1]
    rs_v[8:16, :] = rr[8:16, :] * scales[2]
    save_stats = (save_r, save_c)
    for c in save_stats:
        c.start()

    def wide_body(wg_b, wu_b, gg_b, gu_b, ng_b, nu_b):
        k = pl.program_id(0)
        for t, (w, g, o) in enumerate(((wg_b, gg_b, ng_b), (wu_b, gu_b, nu_b))):
            c = column(cc[pl.ds(7 * t + k, 1), :])
            for j in range(w.shape[1] // 128):
                lanes = slice(128 * j, 128 * (j + 1))
                o[:, lanes] = w[:, lanes] - g[:, lanes] * rs_v[t:t + 1, lanes] * c

    def down_body(w, g, o):
        r = column(rs_v[pl.ds(8 + pl.program_id(0), 1), :])[0:mb]
        for j in range(w.shape[1] // 128):
            lanes = slice(128 * j, 128 * (j + 1))
            c = cc[14 + j // 2:15 + j // 2, 128 * (j % 2):128 * (j % 2 + 1)]
            o[:, lanes] = w[:, lanes] - g[:, lanes] * c * r

    early = E_ROWS + sum(R_SENT)
    rows_a = dxa_v.shape[0]
    save_e = pltpu.make_async_copy(dxa_v.at[pl.ds(0, E_ROWS)], dxa_early.at[pl.ds(0, E_ROWS)], loc.at[10])
    save_a = pltpu.make_async_copy(dxa_v.at[pl.ds(E_ROWS, early - E_ROWS)], dxa_early.at[pl.ds(E_ROWS, early - E_ROWS)], loc.at[10])
    save_late = pltpu.make_async_copy(dxa_v.at[pl.ds(early, rows_a - early)], late, loc.at[11])
    save_pack = [pltpu.make_async_copy(a, b, loc.at[16 + k]) for k, (a, b) in enumerate(norm_pairs(dxn_v, late))]

    def norm_columns(start, stop):
        for j in range(start, stop, 128):
            dxn_v[:, j:j + 128] = (p_v[j:j + 128, :] + pin_v[j:j + 128, :]).T.astype(BF16)

    def act_chunk(k):
        new = A_NEEDS[k] != A_NEEDS[k - 1]
        act_rows(E_ROWS + sum(A_ROWS[:k]), A_ROWS[k], w_copies[A_NEEDS[k]].wait_recv if new else lambda: None)
        if k < len(R_SENT):
            a_copies[k].start()

    @pl.when(col == 0)
    def _():
        act_chunk(1)

    pltpu.emit_pipeline(wide_body, grid=(STEPS,), in_specs=[by_n(wg.shape[1])] * 4,
                        out_specs=[by_n(wg.shape[1])] * 2)(wg, wu, gg, gu, ng, nu)

    @pl.when(col == 0)
    def _():
        act_chunk(2)

    @pl.when(col == 1)
    def _():
        save_e.start()
        for p in p_copies:
            p.wait_recv()
        norm_columns(0, dxn_v.shape[1])
        for c in save_pack:
            c.start()

    pltpu.emit_pipeline(down_body, grid=(STEPS,), in_specs=[by_m(wd.shape[1])] * 2,
                        out_specs=[by_m(wd.shape[1])])(wd, gd, nd)

    @pl.when(col == 0)
    def _():
        act_chunk(3)
        save_a.start()
        act_chunk(4)
        save_late.start()
        e_copy.wait_send()
        for p in p_copies:
            p.wait_send()
        save_a.wait()
        save_late.wait()
        e_back.wait_recv()
        for a in a_copies:
            a.wait_send()

    @pl.when(col == 1)
    def _():
        save_e.wait()
        for c in save_pack:
            c.wait()
        dy_copy.wait_send()
        for w in w_copies:
            w.wait_send()
        e_back.wait_send()
        for a in a_copies:
            a.wait_recv()

    for c in save_stats:
        c.wait()


def run_fused(nc, nr, sizes, wg, wu, wd, xn, xa, dg, du, dd, rg, ru, rd, cg, cu, cd, hyper):
    f32, b16 = (lambda *s: jax.ShapeDtypeStruct(s, F32)), (lambda *s: jax.ShapeDtypeStruct(s, BF16))
    n, i = wg.shape
    m, h = wd.shape
    t = dd.shape[0]
    early = E_ROWS + sum(R_SENT)
    dma = lambda *s: pltpu.SemaphoreType.DMA(s)
    vf = lambda *s: pltpu.VMEM(s, F32)
    vb = lambda *s: pltpu.VMEM(s, BF16)
    return pl.pallas_call(
        functools.partial(fused, nc, nr, sizes),
        out_shape=(f32(n, i), f32(n, i), f32(m, h), f32(n, i), f32(n, i), f32(m, h), b16(early, t), b16(m - early, t),
                   f32(16, 640), f32(24, 480)),
        in_specs=[HBM] * 15,
        out_specs=[HBM] * 10,
        scratch_shapes=[
            vb(*xn.shape), vb(t, h), vf(E_ROWS, h), vb(t, h), vf(E_ROWS, t), vf(E_ROWS, t), vf(i, t), vf(i, t), vb(m, h), vb(m - E_ROWS, h),
            vb(m, t), vb(t, i),
            vf(i), vf(i), vf(m), vf(n), vf(n), vf(h), pltpu.SMEM((3,), F32),
            vf(16, 640), vf(16, 640), vf(nr, 24, 480), vf(nr, 16, 128), vf(16, 128), vf(16, 128), vf(16, i), vf(8, h),
            vf(16, 640), vf(24, 480), vf(16, i), vf(8, h), vf(24, 128),
            vf(16, 640), vf(24, 480), vf(16, 640),
            dma(26), dma(2, 1), dma(2, 2), dma(2, 3), dma(2, len(P_SENT)), dma(2, len(W_SENT)), dma(2, len(R_SENT)), dma(2, 1),
            dma(2, nr), dma(2, nr + 1)],
        compiler_params=pltpu.CompilerParams(collective_id=0, has_side_effects=True, vmem_limit_bytes=60 * 1024 * 1024),
        cost_estimate=pl.CostEstimate(flops=22_000_000_000, bytes_accessed=150_000_000, transcendentals=0),
        name="fused",
    )(wg, wu, wd, xn, xa, dg, du, dd, rg, ru, rd, cg, cu, cd, hyper)


def placements(col, buf, a_out, n_out, sending):
    rows = a_out.shape[0] - buf.shape[0]
    act = [(buf, a_out.at[pl.ds(rows, buf.shape[0])])]
    norm = [(b, a) for a, b in norm_pairs(n_out, buf)]
    return (act, norm) if sending else (norm, act)


def per_side(col, choices, sem, at, action):
    for side, pairs in enumerate(choices):
        @pl.when(col == side)
        def _(pairs=pairs):
            for j, (a, b) in enumerate(pairs):
                action(pltpu.make_async_copy(a, b, sem.at[at + j]))


def publish_kernel(r_hbm, c_hbm, wg, wu, wd, a_in, l_in, ng, nu, nd, a_out, n_out,
                   rgo, ruo, rdo, cgo, cuo, cdo, r_new, c_new, a_v, l_v, sem):
    k = pl.program_id(0)
    col = lax.axis_index('col')
    mb = wd.shape[0]
    pairs = ((r_hbm, r_new), (c_hbm, c_new), (a_in, a_v), (l_in, l_v),
             (a_v, a_out.at[pl.ds(0, a_v.shape[0])]))
    copies = [pltpu.make_async_copy(a, b, sem.at[j]) for j, (a, b) in enumerate(pairs)]
    own = placements(col, l_v, a_out, n_out, True)

    @pl.when(k == 0)
    def _():
        for c in copies[:4]:
            c.start()

    @pl.when(k == 1)
    def _():
        for c in copies[:4]:
            c.wait()
        for c in copies[4:]:
            c.start()
        per_side(col, own, sem, len(pairs), lambda c: c.start())
        rgo[...] = r_new[0:1, :].reshape(-1)
        ruo[...] = r_new[1:2, :].reshape(-1)
        rdo[...] = jnp.concatenate([r_new[8 + j:9 + j, 0:mb] for j in range(STEPS)], axis=1).reshape(-1)
        cgo[...] = jnp.concatenate([c_new[j:j + 1, :] for j in range(STEPS)], axis=1).reshape(-1)
        cuo[...] = jnp.concatenate([c_new[7 + j:8 + j, :] for j in range(STEPS)], axis=1).reshape(-1)
        cdo[...] = jnp.concatenate([c_new[14 + j:15 + j, 0:256] for j in range(5)], axis=1).reshape(-1)

    @pl.when(k == STEPS - 1)
    def _():
        for c in copies[4:]:
            c.wait()
        per_side(col, own, sem, len(pairs), lambda c: c.wait())

    ng[...] = wg[...]
    nu[...] = wu[...]
    nd[...] = wd[...]


def run_publish(r_new, c_new, wg, wu, wd, a_early, late):
    f32 = lambda *s: jax.ShapeDtypeStruct(s, F32)
    b16 = lambda *s: jax.ShapeDtypeStruct(s, BF16)
    n, i = wg.shape
    m, h = wd.shape
    t = late.shape[1]
    flat = lambda s: pl.BlockSpec((s,), lambda k: (0,))
    by_n = pl.BlockSpec((n // STEPS, i), lambda k: (k, 0))
    by_m = pl.BlockSpec((m // STEPS, h), lambda k: (k, 0))
    return pl.pallas_call(
        publish_kernel, grid=(STEPS,),
        out_shape=(f32(n, i), f32(n, i), f32(m, h), b16(m, t), b16(t, i), f32(i), f32(i), f32(m), f32(n), f32(n), f32(h)),
        in_specs=[HBM] * 2 + [by_n, by_n, by_m] + [HBM] * 2,
        out_specs=[by_n, by_n, by_m, HBM, HBM] + [flat(s) for s in (i, i, m, n, n, h)],
        scratch_shapes=[pltpu.VMEM(a.shape, a.dtype) for a in (r_new, c_new, a_early, late)] + [
            pltpu.SemaphoreType.DMA((16,))],
        compiler_params=pltpu.CompilerParams(vmem_limit_bytes=60 * 1024 * 1024),
        cost_estimate=pl.CostEstimate(flops=20_000_000_000, bytes_accessed=58_000_000, transcendentals=0),
        name="publish",
    )(r_new, c_new, wg, wu, wd, a_early, late)


def place_kernel(late_in, a_in, n_in, a_out, n_out, sem):
    col = lax.axis_index('col')
    got = placements(col, late_in, a_out, n_out, False)
    per_side(col, got, sem, 0, lambda c: c.start())
    per_side(col, got, sem, 0, lambda c: c.wait())


def run_place(late_in, dxa, dxn):
    return pl.pallas_call(
        place_kernel,
        out_shape=(jax.ShapeDtypeStruct(dxa.shape, BF16), jax.ShapeDtypeStruct(dxn.shape, BF16)),
        in_specs=[pl.BlockSpec(memory_space=pl.ANY), HBM, HBM], out_specs=[HBM, HBM], input_output_aliases={1: 0, 2: 1},
        scratch_shapes=[pltpu.SemaphoreType.DMA((10,))],
        compiler_params=pltpu.CompilerParams(vmem_limit_bytes=1024 * 1024),
        name="place",
    )(late_in, dxa, dxn)


SWAP = [(0, 1), (1, 0)]


def solution(mesh):
    row_size = mesh.shape['row']
    col_size = mesh.shape['col']
    weight_spec = P('row', 'col')
    act_spec = P(None, 'row')
    grad_spec = P(None, 'col')
    in_specs = (weight_spec,) * 3 + (act_spec, act_spec) + (grad_spec,) * 3 + (P('row'), P('col')) * 3 + (P(),)
    out_specs = (weight_spec,) * 3 + (P('row'), P('col')) * 3 + (act_spec, act_spec)

    def body(w_gate, w_up, w_down, x_norm, x_act, dy_gate, dy_up, dy_down, r_gate, c_gate, r_up, c_up, r_down, c_down, hyper_params):
        d_model = w_gate.shape[0] * row_size
        d_ff = w_gate.shape[1] * col_size
        _, _, _, ng, nu, nd, a_early, late, r_new, c_new = run_fused(
            col_size, row_size, (d_model, d_ff),
            w_gate.T, w_up.T, w_down, x_norm, x_act.T, dy_gate.T, dy_up.T, dy_down,
            r_gate, r_up, r_down, c_gate, c_up, c_down, hyper_params)
        late_in = lax.ppermute(late, 'col', SWAP)
        ng, nu, nd, dxa, dxn, rgo, ruo, rdo, cgo, cuo, cdo = run_publish(r_new, c_new, ng, nu, nd, a_early, late)
        dx_act, dx_norm = run_place(late_in, dxa, dxn)
        return (ng.T, nu.T, nd, rgo, cgo, ruo, cuo, rdo, cdo, dx_norm, dx_act.T)

    return jax.shard_map(body, mesh=mesh, in_specs=in_specs, out_specs=out_specs, check_vma=False)
```

```python
import functools

import jax
import jax.numpy as jnp
from jax import lax
from jax.experimental import pallas as pl
from jax.experimental.pallas import tpu as pltpu
from jax.sharding import PartitionSpec as P

EPS_ONE = 1e-30
EPS_TWO = 1e-3
STEPS = 7
BF16 = jnp.bfloat16
F32 = jnp.float32
MESH = pl.DeviceIdType.MESH
VM = pl.BlockSpec(memory_space=pltpu.VMEM)

HBM = pl.BlockSpec(memory_space=pltpu.HBM)

E_ROWS = 112
P_FIRST = 256
P_SENT = (256, 176, 176, 32)
W_SENT = (592, 304, 560, 112)
A_ROWS = (304, 288, 304, 560, 112)
A_NEEDS = (0, 0, 1, 2, 3)
R_SENT = (304, 288, 304, 32)
CAST_FIRST = 4


def fold(v, width=128):
    acc = v[:, :width]
    for k in range(1, v.shape[1] // width):
        acc = acc + v[:, k * width:(k + 1) * width]
    return acc


def fold_rows(v):
    return jnp.sum(v.reshape(v.shape[0] // 8, 8, v.shape[1]), axis=0)


def lane_total(v):
    s = jnp.sum(jnp.sum(v, axis=0, keepdims=True), axis=1, keepdims=True)
    lane = lax.broadcasted_iota(jnp.int32, (1, 128), 1)
    return jnp.where(lane == 0, jnp.broadcast_to(s, (1, 128)), 0.0)


def column(row_vec):
    return jnp.broadcast_to(row_vec, (128, row_vec.shape[1])).T


def norm_pairs(norm, buf):
    t, i = norm.shape
    half, wide, last = t // 2, i - 128, t // 2
    pairs = [(norm.at[pl.ds(0, half), pl.ds(0, wide)], buf.at[pl.ds(0, half), pl.ds(0, wide)]),
             (norm.at[pl.ds(half, half), pl.ds(0, wide)], buf.at[pl.ds(0, half), pl.ds(wide, wide)])]
    for b in range(t // 128):
        pairs.append((norm.at[pl.ds(128 * b, 128), pl.ds(wide, 128)], buf.at[pl.ds(last, 128), pl.ds(128 * b, 128)]))
    return pairs


def fused(nc, nr, sizes,
          wg, wu, wd, xn, xa, dg, du, dd, rg, ru, rd, cg, cu, cd, hyper,
          gg, gu, gd, ng, nu, nd, dxa_early, late, r_hbm, c_hbm,
          xn_v, dd_v, wf_v, dy_v, e_v, ein_v, p_v, pin_v, wb_v, win_v, dxa_v, dxn_v,
          rg_v, ru_v, rd_v, cg_v, cu_v, cd_v, hyp,
          r_mine, r_peer, r_send, r_got, c_all, s_all, s_mine, s_peer, wsq, wsq_d, rr, cc, racc, cacc, sacc, r_out, c_out, rs_v,
          loc, dsem, esem, qsem, psem, wsem, asem, rsem, csem, ssem):
    col = lax.axis_index('col')
    row = lax.axis_index('row')
    d_model, d_ff = sizes
    nb = dg.shape[0] // STEPS
    mb = wd.shape[0] // STEPS
    quarter = dd.shape[0] // nr
    others = [(1, 0)] + [(0, dr) for dr in range(1, nr)]

    c_all[row] = jnp.zeros(c_all.shape[1:], F32)
    s_all[row] = jnp.zeros(s_all.shape[1:], F32)

    barrier = pltpu.get_barrier_semaphore()
    for dc, dr in others:
        pl.semaphore_signal(barrier, 1, device_id=(lax.rem(col + dc, nc), lax.rem(row + dr, nr)), device_id_type=MESH)

    loads = [pltpu.make_async_copy(a, b, loc.at[k]) for k, (a, b) in enumerate((
        (wd.at[pl.ds(0, E_ROWS)], wf_v), (dd, dd_v), (xn, xn_v), (rg, rg_v), (ru, ru_v), (rd, rd_v), (cg, cg_v), (cu, cu_v), (cd, cd_v), (hyper, hyp)))]
    for load in loads:
        load.start()

    def first_partial():
        for load in loads[:2]:
            load.wait()
        e_v[...] = lax.dot_general(wf_v[...].astype(BF16), dd_v[...], (((1,), (1,)), ((), ())), preferred_element_type=F32)

    @pl.when(col == 0)
    def _():
        first_partial()

    pl.semaphore_wait(barrier, len(others))

    def remote(src, dst, sems, k, target):
        return pltpu.make_async_remote_copy(src_ref=src, dst_ref=dst, send_sem=sems.at[0, k], recv_sem=sems.at[1, k],
                                            device_id=target, device_id_type=MESH)

    def ranged(src, dst, sems, counts, at=0, to=0):
        copies = []
        for k, n in enumerate(counts):
            copies.append(remote(src.at[pl.ds(at, n)], dst.at[pl.ds(at + to, n)], sems, k, across))
            at += n
        return copies

    across = (1 - col, row)
    chip = (col, lax.rem(row + 2, nr))
    core = (col, row + 1 - 2 * lax.rem(row, 2))
    rows_of = lambda r: pl.ds(pl.multiple_of(r * quarter, quarter), quarter)
    dy_copy = remote(dd.at[rows_of(row)], dy_v.at[rows_of(row)], dsem, 0, across)
    p_copies = ranged(p_v, pin_v, psem, P_SENT)
    w_copies = ranged(wb_v, win_v, wsem, W_SENT, E_ROWS, -E_ROWS)
    a_copies = ranged(dxa_v, dxa_early, asem, R_SENT, E_ROWS)
    e_copy = remote(e_v, ein_v, esem, 0, across)
    e_back = remote(dxa_v.at[pl.ds(0, E_ROWS)], dxa_early.at[pl.ds(0, E_ROWS)], esem, 1, across)
    dims_t = (((1,), (1,)), ((), ()))

    def act_rows(at, n, ready):
        o = lax.dot_general(wb_v[at:at + n, :], dd_v[...], dims_t, preferred_element_type=F32)
        ready()
        o = o + lax.dot_general(win_v[at - E_ROWS:at - E_ROWS + n, :], dy_v[...], dims_t, preferred_element_type=F32)
        dxa_v[at:at + n, :] = o.astype(BF16)

    @pl.when(col == 0)
    def _():
        e_copy.start()

    @pl.when(col == 1)
    def _():
        dy_copy.start()
        first_partial()

    by_n = lambda width: pl.BlockSpec((nb, width), lambda k: (k, 0))
    by_m = lambda width: pl.BlockSpec((mb, width), lambda k: (k, 0))

    wsq_d[...] = jnp.zeros_like(wsq_d)

    def cast_body(start, w_b):
        w = w_b[...]
        wsq_d[...] += fold_rows(w * w)
        wb_v[pl.ds(pl.multiple_of((start + pl.program_id(0)) * mb, mb), mb), :] = w.astype(BF16)

    def cast(start, count):
        pltpu.emit_pipeline(functools.partial(cast_body, start), grid=(count,), in_specs=[
            pl.BlockSpec((mb, wd.shape[1]), lambda k: (start + k, 0), pipeline_mode=pl.Buffered(4))])(wd)

    p_v[...] = jnp.zeros_like(p_v)
    wsq[...] = jnp.zeros_like(wsq)

    def part_body(start, wg_b, wu_b, dg_b, du_b):
        rows = slice(start, start + wg_b.shape[1])
        for k, (w_b, d_b) in enumerate(((wg_b, dg_b), (wu_b, du_b))):
            w = w_b[...]
            wsq[8 * k:8 * k + 8, rows] += fold_rows(w * w)
            p_v[rows, :] += lax.dot_general(w.astype(BF16), d_b[...], (((0,), (0,)), ((), ())), preferred_element_type=F32)

    def partial_rows(start, count):
        deep_n = lambda width: pl.BlockSpec((nb, width), lambda k: (k, 0), pipeline_mode=pl.Buffered(3))
        cols = pl.ds(start, count)
        pltpu.emit_pipeline(functools.partial(part_body, start), grid=(STEPS,),
                            in_specs=[deep_n(count)] * 2 + [deep_n(dg.shape[1])] * 2)(wg.at[:, cols], wu.at[:, cols], dg, du)

    partial_rows(0, P_FIRST)

    @pl.when(col == 0)
    def _():
        p_copies[0].start()

    cast(0, CAST_FIRST)

    @pl.when(col == 1)
    def _():
        w_copies[0].start()

    partial_rows(P_FIRST, wg.shape[1] - P_FIRST)

    @pl.when(col == 0)
    def _():
        p_copies[1].start()

    cast(CAST_FIRST, STEPS - CAST_FIRST)

    q_far = remote(dy_v.at[rows_of(row)], dy_v.at[rows_of(row)], qsem, 0, chip)
    q_near = remote(dy_v.at[rows_of(row)], dy_v.at[rows_of(row)], qsem, 1, core)
    q_both = remote(dy_v.at[rows_of(chip[1])], dy_v.at[rows_of(chip[1])], qsem, 2, core)

    @pl.when(col == 0)
    def _():
        dy_copy.wait_recv()
        q_far.start()
        q_near.start()

    for load in loads[2:]:
        load.wait()
    r_mine[...] = jnp.zeros_like(r_mine)
    racc[...] = jnp.zeros_like(racc)
    cacc[...] = jnp.zeros_like(cacc)

    def grad_body(dg_b, du_b, xa_b, gg_b, gu_b, gd_b):
        k = pl.program_id(0)
        for t, (d_b, g_b) in enumerate(((dg_b, gg_b), (du_b, gu_b))):
            g = jnp.dot(d_b[...], xn_v[...], preferred_element_type=F32)
            g_b[...] = g
            q = g * g + EPS_ONE
            racc[pl.ds(8 * t, 8), :] += fold_rows(q)
            c_all[row, pl.ds(7 * t + k, 1), :] = jnp.sum(fold(q).T, axis=0, keepdims=True)
        g = jnp.dot(xa_b[...], dd_v[...], preferred_element_type=F32)
        gd_b[...] = g
        q = g * g + EPS_ONE
        cacc[...] += fold_rows(q)
        r_mine[pl.ds(8 + k, 1), pl.ds(0, 240)] = jnp.sum(fold(q).T, axis=0, keepdims=True)

    pltpu.emit_pipeline(grad_body, grid=(STEPS,), in_specs=[by_n(dg.shape[1])] * 2 + [by_m(xa.shape[1])],
                        out_specs=[by_n(gg.shape[1])] * 2 + [by_m(gd.shape[1])])(dg, du, xa, gg, gu, gd)

    for t in range(2):
        r_mine[t:t + 1, :] = jnp.sum(racc[8 * t:8 * t + 8, :], axis=0, keepdims=True)
    c_down = jnp.sum(cacc[...], axis=0, keepdims=True)
    for k in range(5):
        c_all[row, 14 + k:15 + k, 0:256] = c_down[:, 256 * k:256 * (k + 1)]

    r_send[...] = jnp.zeros_like(r_send)
    r_send[:, 0:256] = r_mine[8:16, 0:256]
    for t in range(2):
        for j in range(5):
            r_send[j:j + 1, 128 * (2 + t):128 * (3 + t)] = r_mine[t:t + 1, 128 * j:128 * (j + 1)]
    r_copy = remote(r_send, r_got, rsem, 0, across)
    r_copy.start()
    c_copies = [pltpu.make_async_remote_copy(
        src_ref=c_all.at[row], dst_ref=c_all.at[row], send_sem=csem.at[0, d], recv_sem=csem.at[1, row],
        device_id=(col, lax.rem(row + d, nr)), device_id_type=MESH) for d in range(1, nr)]
    for c in c_copies:
        c.start()

    @pl.when(col == 0)
    def _():
        p_copies[2].start()
        q_far.wait_recv()
        q_both.start()

        def first_ready():
            w_copies[0].wait_recv()
            q_near.wait_recv()
            q_both.wait_recv()
            q_far.wait_send()
            q_near.wait_send()
            q_both.wait_send()

        act_rows(E_ROWS, A_ROWS[0], first_ready)

    @pl.when(col == 1)
    def _():
        w_copies[1].start()
        e_copy.wait_recv()
        dxa_v[0:E_ROWS, :] = (e_v[...] + ein_v[...]).astype(BF16)

    beta = hyp[0]
    rr[...] = jnp.ones_like(rr)
    rr[0:1, :] = rg_v[...].reshape(1, -1)
    rr[1:2, :] = ru_v[...].reshape(1, -1)
    r_old, g_old, u_old, d_old = [v[...].reshape(1, -1) for v in (rd_v, cg_v, cu_v, cd_v)]
    for k in range(STEPS):
        cc[k:k + 1, :] = g_old[:, nb * k:nb * (k + 1)]
        cc[7 + k:8 + k, :] = u_old[:, nb * k:nb * (k + 1)]
        rr[8 + k:9 + k, 0:mb] = r_old[:, mb * k:mb * (k + 1)]
    for k in range(5):
        cc[14 + k:15 + k, 0:256] = d_old[:, 256 * k:256 * (k + 1)]
        cc[14 + k:15 + k, 256:480] = jnp.ones((1, 224), F32)
    cc[19:24, :] = jnp.ones((5, 480), F32)

    r_peer[...] = jnp.zeros_like(r_peer)
    r_copy.wait()
    r_peer[8:16, 0:256] = r_got[:, 0:256]
    for t in range(2):
        for j in range(5):
            r_peer[t:t + 1, 128 * j:128 * (j + 1)] = r_got[j:j + 1, 128 * (2 + t):128 * (3 + t)]
    for d in range(1, nr):
        c_copies[d - 1].wait_send()
        s = lax.rem(row + d, nr)
        pltpu.make_async_remote_copy(src_ref=c_all.at[s], dst_ref=c_all.at[s], send_sem=csem.at[0, d], recv_sem=csem.at[1, s],
                                     device_id=(col, s), device_id_type=MESH).wait_recv()

    line = lax.broadcasted_iota(jnp.int32, rr.shape, 0)
    r_new = beta * rr[...] + (1.0 - beta) * ((r_mine[...] + r_peer[...]) / jnp.where(line < 8, float(d_ff), float(d_model)))
    line = lax.broadcasted_iota(jnp.int32, cc.shape, 0)
    c_sum = (c_all[0] + c_all[1]) + (c_all[2] + c_all[3])
    c_new = beta * cc[...] + (1.0 - beta) * (c_sum / jnp.where(line < 14, float(d_model), float(d_ff)))
    r_out[...] = r_new
    c_out[...] = c_new
    rr[...] = lax.rsqrt(r_new)
    cc[...] = lax.rsqrt(c_new)
    save_r = pltpu.make_async_copy(r_out, r_hbm, loc.at[12])
    save_c = pltpu.make_async_copy(c_out, c_hbm, loc.at[13])

    sacc[...] = jnp.zeros_like(sacc)

    def square_body(gg_b, gu_b, gd_b):
        k = pl.program_id(0)
        for t, g_b in enumerate((gg_b, gu_b)):
            u = g_b[...] * rr[t:t + 1, :]
            s = fold(u * u)
            c = column(cc[pl.ds(7 * t + k, 1), :])
            sacc[pl.ds(8 * t, 8), :] += fold_rows(s * (c * c))
        c_row = jnp.concatenate([cc[14 + j:15 + j, 0:256] for j in range(5)], axis=1)
        u = gd_b[...] * c_row
        s = fold(u * u)
        r = column(rr[pl.ds(8 + k, 1), :])[0:mb]
        sacc[16:24, :] += fold_rows(s * (r * r))

    pltpu.emit_pipeline(square_body, grid=(STEPS,), in_specs=[by_n(gg.shape[1])] * 2 + [by_m(gd.shape[1])])(gg, gu, gd)

    for t in range(3):
        s_all[row, t:t + 1, :] = jnp.sum(sacc[8 * t:8 * t + 8, :], axis=0, keepdims=True)
    for t in range(2):
        s_all[row, 3 + t:4 + t, :] = jnp.sum(fold(wsq[8 * t:8 * t + 8, :]), axis=0, keepdims=True)
        s_all[row, 6 + t:7 + t, :] = lane_total(r_new[t:t + 1, :])
    s_all[row, 5:6, :] = jnp.sum(fold(wsq_d[...]), axis=0, keepdims=True)
    s_all[row, 8:9, :] = lane_total(r_new[8:15, 0:mb])
    s_copies = [pltpu.make_async_remote_copy(
        src_ref=s_all.at[row], dst_ref=s_all.at[row], send_sem=ssem.at[0, d], recv_sem=ssem.at[1, row],
        device_id=(col, lax.rem(row + d, nr)), device_id_type=MESH) for d in range(1, nr)]
    for s in s_copies:
        s.start()
    for d in range(1, nr):
        s_copies[d - 1].wait_send()
        him = lax.rem(row + d, nr)
        pltpu.make_async_remote_copy(src_ref=s_all.at[him], dst_ref=s_all.at[him], send_sem=ssem.at[0, d],
                                     recv_sem=ssem.at[1, him], device_id=(col, him), device_id_type=MESH).wait_recv()
    s_mine[...] = (s_all[0] + s_all[1]) + (s_all[2] + s_all[3])
    s_copy = remote(s_mine, s_peer, ssem, nr, across)
    s_copy.start()

    @pl.when(col == 0)
    def _():
        p_copies[3].start()
        a_copies[0].start()

    @pl.when(col == 1)
    def _():
        for w in w_copies[2:]:
            w.start()
        e_back.start()

    s_copy.wait()
    total = s_mine[...] + s_peer[...]
    sums = jnp.sum(total, axis=1, keepdims=True)
    scales = []
    for t, (m, n) in enumerate(((d_model, d_ff), (d_model, d_ff), (d_ff, d_model))):
        r_mean = sums[6 + t:7 + t] / float(m * nc)
        rms_u = jnp.sqrt(sums[t:t + 1] * r_mean / float(m * n))
        step = hyp[1] * jnp.maximum(EPS_TWO, jnp.sqrt(sums[3 + t:4 + t] / float(m * n)))
        scales.append(step * jnp.sqrt(r_mean) / jnp.maximum(1.0, rms_u / hyp[2]))
    rs_v[...] = rr[...]
    rs_v[0:1, :] = rr[0:1, :] * scales[0]
    rs_v[1:2, :] = rr[1:2, :] * scales[1]
    rs_v[8:16, :] = rr[8:16, :] * scales[2]
    save_stats = (save_r, save_c)
    for c in save_stats:
        c.start()

    def wide_body(wg_b, wu_b, gg_b, gu_b, ng_b, nu_b):
        k = pl.program_id(0)
        for t, (w, g, o) in enumerate(((wg_b, gg_b, ng_b), (wu_b, gu_b, nu_b))):
            c = column(cc[pl.ds(7 * t + k, 1), :])
            for j in range(w.shape[1] // 128):
                lanes = slice(128 * j, 128 * (j + 1))
                o[:, lanes] = w[:, lanes] - g[:, lanes] * rs_v[t:t + 1, lanes] * c

    def down_body(w, g, o):
        r = column(rs_v[pl.ds(8 + pl.program_id(0), 1), :])[0:mb]
        for j in range(w.shape[1] // 128):
            lanes = slice(128 * j, 128 * (j + 1))
            c = cc[14 + j // 2:15 + j // 2, 128 * (j % 2):128 * (j % 2 + 1)]
            o[:, lanes] = w[:, lanes] - g[:, lanes] * c * r

    early = E_ROWS + sum(R_SENT)
    rows_a = dxa_v.shape[0]
    save_e = pltpu.make_async_copy(dxa_v.at[pl.ds(0, E_ROWS)], dxa_early.at[pl.ds(0, E_ROWS)], loc.at[10])
    save_a = pltpu.make_async_copy(dxa_v.at[pl.ds(E_ROWS, early - E_ROWS)], dxa_early.at[pl.ds(E_ROWS, early - E_ROWS)], loc.at[10])
    save_late = pltpu.make_async_copy(dxa_v.at[pl.ds(early, rows_a - early)], late, loc.at[11])
    save_pack = [pltpu.make_async_copy(a, b, loc.at[16 + k]) for k, (a, b) in enumerate(norm_pairs(dxn_v, late))]

    def norm_columns(start, stop):
        for j in range(start, stop, 128):
            dxn_v[:, j:j + 128] = (p_v[j:j + 128, :] + pin_v[j:j + 128, :]).T.astype(BF16)

    def act_chunk(k):
        new = A_NEEDS[k] != A_NEEDS[k - 1]
        act_rows(E_ROWS + sum(A_ROWS[:k]), A_ROWS[k], w_copies[A_NEEDS[k]].wait_recv if new else lambda: None)
        if k < len(R_SENT):
            a_copies[k].start()

    @pl.when(col == 0)
    def _():
        act_chunk(1)

    pltpu.emit_pipeline(wide_body, grid=(STEPS,), in_specs=[by_n(wg.shape[1])] * 4,
                        out_specs=[by_n(wg.shape[1])] * 2)(wg, wu, gg, gu, ng, nu)

    @pl.when(col == 0)
    def _():
        act_chunk(2)

    @pl.when(col == 1)
    def _():
        save_e.start()
        for p in p_copies:
            p.wait_recv()
        norm_columns(0, dxn_v.shape[1])
        for c in save_pack:
            c.start()

    pltpu.emit_pipeline(down_body, grid=(STEPS,), in_specs=[by_m(wd.shape[1])] * 2,
                        out_specs=[by_m(wd.shape[1])])(wd, gd, nd)

    @pl.when(col == 0)
    def _():
        act_chunk(3)
        save_a.start()
        act_chunk(4)
        save_late.start()
        e_copy.wait_send()
        for p in p_copies:
            p.wait_send()
        save_a.wait()
        save_late.wait()
        e_back.wait_recv()
        for a in a_copies:
            a.wait_send()

    @pl.when(col == 1)
    def _():
        save_e.wait()
        for c in save_pack:
            c.wait()
        dy_copy.wait_send()
        for w in w_copies:
            w.wait_send()
        e_back.wait_send()
        for a in a_copies:
            a.wait_recv()

    for c in save_stats:
        c.wait()


def run_fused(nc, nr, sizes, wg, wu, wd, xn, xa, dg, du, dd, rg, ru, rd, cg, cu, cd, hyper):
    f32, b16 = (lambda *s: jax.ShapeDtypeStruct(s, F32)), (lambda *s: jax.ShapeDtypeStruct(s, BF16))
    n, i = wg.shape
    m, h = wd.shape
    t = dd.shape[0]
    early = E_ROWS + sum(R_SENT)
    dma = lambda *s: pltpu.SemaphoreType.DMA(s)
    vf = lambda *s: pltpu.VMEM(s, F32)
    vb = lambda *s: pltpu.VMEM(s, BF16)
    return pl.pallas_call(
        functools.partial(fused, nc, nr, sizes),
        out_shape=(f32(n, i), f32(n, i), f32(m, h), f32(n, i), f32(n, i), f32(m, h), b16(early, t), b16(m - early, t),
                   f32(16, 640), f32(24, 480)),
        in_specs=[HBM] * 15,
        out_specs=[HBM] * 10,
        scratch_shapes=[
            vb(*xn.shape), vb(t, h), vf(E_ROWS, h), vb(t, h), vf(E_ROWS, t), vf(E_ROWS, t), vf(i, t), vf(i, t), vb(m, h), vb(m - E_ROWS, h),
            vb(m, t), vb(t, i),
            vf(i), vf(i), vf(m), vf(n), vf(n), vf(h), pltpu.SMEM((3,), F32),
            vf(16, 640), vf(16, 640), vf(8, 512), vf(8, 512), vf(nr, 24, 480), vf(nr, 16, 128), vf(16, 128), vf(16, 128), vf(16, i), vf(8, h),
            vf(16, 640), vf(24, 480), vf(16, i), vf(8, h), vf(24, 128),
            vf(16, 640), vf(24, 480), vf(16, 640),
            dma(26), dma(2, 1), dma(2, 2), dma(2, 3), dma(2, len(P_SENT)), dma(2, len(W_SENT)), dma(2, len(R_SENT)), dma(2, 1),
            dma(2, nr), dma(2, nr + 1)],
        compiler_params=pltpu.CompilerParams(collective_id=0, has_side_effects=True, vmem_limit_bytes=60 * 1024 * 1024),
        cost_estimate=pl.CostEstimate(flops=22_000_000_000, bytes_accessed=150_000_000, transcendentals=0),
        name="fused",
    )(wg, wu, wd, xn, xa, dg, du, dd, rg, ru, rd, cg, cu, cd, hyper)


def placements(col, buf, a_out, n_out, sending):
    rows = a_out.shape[0] - buf.shape[0]
    act = [(buf, a_out.at[pl.ds(rows, buf.shape[0])])]
    norm = [(b, a) for a, b in norm_pairs(n_out, buf)]
    return (act, norm) if sending else (norm, act)


def per_side(col, choices, sem, at, action):
    for side, pairs in enumerate(choices):
        @pl.when(col == side)
        def _(pairs=pairs):
            for j, (a, b) in enumerate(pairs):
                action(pltpu.make_async_copy(a, b, sem.at[at + j]))


def publish_kernel(r_hbm, c_hbm, wg, wu, wd, a_in, l_in, ng, nu, nd, a_out, n_out,
                   rgo, ruo, rdo, cgo, cuo, cdo, r_new, c_new, a_v, l_v, sem):
    k = pl.program_id(0)
    col = lax.axis_index('col')
    mb = wd.shape[0]
    pairs = ((r_hbm, r_new), (c_hbm, c_new), (a_in, a_v), (l_in, l_v),
             (a_v, a_out.at[pl.ds(0, a_v.shape[0])]))
    copies = [pltpu.make_async_copy(a, b, sem.at[j]) for j, (a, b) in enumerate(pairs)]
    own = placements(col, l_v, a_out, n_out, True)

    @pl.when(k == 0)
    def _():
        for c in copies[:4]:
            c.start()

    @pl.when(k == 1)
    def _():
        for c in copies[:4]:
            c.wait()
        for c in copies[4:]:
            c.start()
        per_side(col, own, sem, len(pairs), lambda c: c.start())
        rgo[...] = r_new[0:1, :].reshape(-1)
        ruo[...] = r_new[1:2, :].reshape(-1)
        rdo[...] = jnp.concatenate([r_new[8 + j:9 + j, 0:mb] for j in range(STEPS)], axis=1).reshape(-1)
        cgo[...] = jnp.concatenate([c_new[j:j + 1, :] for j in range(STEPS)], axis=1).reshape(-1)
        cuo[...] = jnp.concatenate([c_new[7 + j:8 + j, :] for j in range(STEPS)], axis=1).reshape(-1)
        cdo[...] = jnp.concatenate([c_new[14 + j:15 + j, 0:256] for j in range(5)], axis=1).reshape(-1)

    @pl.when(k == STEPS - 1)
    def _():
        for c in copies[4:]:
            c.wait()
        per_side(col, own, sem, len(pairs), lambda c: c.wait())

    ng[...] = wg[...]
    nu[...] = wu[...]
    nd[...] = wd[...]


def run_publish(r_new, c_new, wg, wu, wd, a_early, late):
    f32 = lambda *s: jax.ShapeDtypeStruct(s, F32)
    b16 = lambda *s: jax.ShapeDtypeStruct(s, BF16)
    n, i = wg.shape
    m, h = wd.shape
    t = late.shape[1]
    flat = lambda s: pl.BlockSpec((s,), lambda k: (0,))
    by_n = pl.BlockSpec((n // STEPS, i), lambda k: (k, 0))
    by_m = pl.BlockSpec((m // STEPS, h), lambda k: (k, 0))
    return pl.pallas_call(
        publish_kernel, grid=(STEPS,),
        out_shape=(f32(n, i), f32(n, i), f32(m, h), b16(m, t), b16(t, i), f32(i), f32(i), f32(m), f32(n), f32(n), f32(h)),
        in_specs=[HBM] * 2 + [by_n, by_n, by_m] + [HBM] * 2,
        out_specs=[by_n, by_n, by_m, HBM, HBM] + [flat(s) for s in (i, i, m, n, n, h)],
        scratch_shapes=[pltpu.VMEM(a.shape, a.dtype) for a in (r_new, c_new, a_early, late)] + [
            pltpu.SemaphoreType.DMA((16,))],
        compiler_params=pltpu.CompilerParams(vmem_limit_bytes=60 * 1024 * 1024),
        cost_estimate=pl.CostEstimate(flops=20_000_000_000, bytes_accessed=58_000_000, transcendentals=0),
        name="publish",
    )(r_new, c_new, wg, wu, wd, a_early, late)


def place_kernel(late_in, a_in, n_in, a_out, n_out, sem):
    col = lax.axis_index('col')
    got = placements(col, late_in, a_out, n_out, False)
    per_side(col, got, sem, 0, lambda c: c.start())
    per_side(col, got, sem, 0, lambda c: c.wait())


def run_place(late_in, dxa, dxn):
    return pl.pallas_call(
        place_kernel,
        out_shape=(jax.ShapeDtypeStruct(dxa.shape, BF16), jax.ShapeDtypeStruct(dxn.shape, BF16)),
        in_specs=[pl.BlockSpec(memory_space=pl.ANY), HBM, HBM], out_specs=[HBM, HBM], input_output_aliases={1: 0, 2: 1},
        scratch_shapes=[pltpu.SemaphoreType.DMA((10,))],
        compiler_params=pltpu.CompilerParams(vmem_limit_bytes=1024 * 1024),
        name="place",
    )(late_in, dxa, dxn)


SWAP = [(0, 1), (1, 0)]


def solution(mesh):
    row_size = mesh.shape['row']
    col_size = mesh.shape['col']
    weight_spec = P('row', 'col')
    act_spec = P(None, 'row')
    grad_spec = P(None, 'col')
    in_specs = (weight_spec,) * 3 + (act_spec, act_spec) + (grad_spec,) * 3 + (P('row'), P('col')) * 3 + (P(),)
    out_specs = (weight_spec,) * 3 + (P('row'), P('col')) * 3 + (act_spec, act_spec)

    def body(w_gate, w_up, w_down, x_norm, x_act, dy_gate, dy_up, dy_down, r_gate, c_gate, r_up, c_up, r_down, c_down, hyper_params):
        d_model = w_gate.shape[0] * row_size
        d_ff = w_gate.shape[1] * col_size
        _, _, _, ng, nu, nd, a_early, late, r_new, c_new = run_fused(
            col_size, row_size, (d_model, d_ff),
            w_gate.T, w_up.T, w_down, x_norm, x_act.T, dy_gate.T, dy_up.T, dy_down,
            r_gate, r_up, r_down, c_gate, c_up, c_down, hyper_params)
        late_in = lax.ppermute(late, 'col', SWAP)
        ng, nu, nd, dxa, dxn, rgo, ruo, rdo, cgo, cuo, cdo = run_publish(r_new, c_new, ng, nu, nd, a_early, late)
        dx_act, dx_norm = run_place(late_in, dxa, dxn)
        return (ng.T, nu.T, nd, rgo, cgo, ruo, cuo, rdo, cdo, dx_norm, dx_act.T)

    return jax.shard_map(body, mesh=mesh, in_specs=in_specs, out_specs=out_specs, check_vma=False)
```

```python
import functools

import jax
import jax.numpy as jnp
from jax import lax
from jax.experimental import pallas as pl
from jax.experimental.pallas import tpu as pltpu
from jax.sharding import PartitionSpec as P

EPS_ONE = 1e-30
EPS_TWO = 1e-3
STEPS = 7
BF16 = jnp.bfloat16
F32 = jnp.float32
MESH = pl.DeviceIdType.MESH
VM = pl.BlockSpec(memory_space=pltpu.VMEM)

HBM = pl.BlockSpec(memory_space=pltpu.HBM)

E_ROWS = 96
P_FIRST = 256
P_SENT = (256, 192, 176, 16)
W_SENT = (592, 304, 576, 112)
A_ROWS = (304, 288, 304, 576, 112)
A_NEEDS = (0, 0, 1, 2, 3)
R_SENT = (304, 288, 304, 48)
CAST_FIRST = 4


def fold(v, width=128):
    acc = v[:, :width]
    for k in range(1, v.shape[1] // width):
        acc = acc + v[:, k * width:(k + 1) * width]
    return acc


def fold_rows(v):
    return jnp.sum(v.reshape(v.shape[0] // 8, 8, v.shape[1]), axis=0)


def lane_total(v):
    s = jnp.sum(jnp.sum(v, axis=0, keepdims=True), axis=1, keepdims=True)
    lane = lax.broadcasted_iota(jnp.int32, (1, 128), 1)
    return jnp.where(lane == 0, jnp.broadcast_to(s, (1, 128)), 0.0)


def column(row_vec):
    return jnp.broadcast_to(row_vec, (128, row_vec.shape[1])).T


def norm_pairs(norm, buf):
    t, i = norm.shape
    half, wide, last = t // 2, i - 128, t // 2
    pairs = [(norm.at[pl.ds(0, half), pl.ds(0, wide)], buf.at[pl.ds(0, half), pl.ds(0, wide)]),
             (norm.at[pl.ds(half, half), pl.ds(0, wide)], buf.at[pl.ds(0, half), pl.ds(wide, wide)])]
    for b in range(t // 128):
        pairs.append((norm.at[pl.ds(128 * b, 128), pl.ds(wide, 128)], buf.at[pl.ds(last, 128), pl.ds(128 * b, 128)]))
    return pairs


def fused(nc, nr, sizes,
          wg, wu, wd, xn, xa, dg, du, dd, rg, ru, rd, cg, cu, cd, hyper,
          gg, gu, gd, ng, nu, nd, dxa_early, late, r_hbm, c_hbm,
          xn_v, dd_v, wf_v, dy_v, e_v, ein_v, p_v, pin_v, wb_v, win_v, dxa_v, dxn_v,
          rg_v, ru_v, rd_v, cg_v, cu_v, cd_v, hyp,
          r_mine, r_peer, r_send, r_got, c_all, s_all, s_mine, s_peer, wsq, wsq_d, rr, cc, racc, cacc, sacc, r_out, c_out, rs_v,
          loc, dsem, esem, qsem, psem, wsem, asem, rsem, csem, ssem):
    col = lax.axis_index('col')
    row = lax.axis_index('row')
    d_model, d_ff = sizes
    nb = dg.shape[0] // STEPS
    mb = wd.shape[0] // STEPS
    quarter = dd.shape[0] // nr
    others = [(1, 0)] + [(0, dr) for dr in range(1, nr)]

    c_all[row] = jnp.zeros(c_all.shape[1:], F32)
    s_all[row] = jnp.zeros(s_all.shape[1:], F32)

    barrier = pltpu.get_barrier_semaphore()
    for dc, dr in others:
        pl.semaphore_signal(barrier, 1, device_id=(lax.rem(col + dc, nc), lax.rem(row + dr, nr)), device_id_type=MESH)

    loads = [pltpu.make_async_copy(a, b, loc.at[k]) for k, (a, b) in enumerate((
        (wd.at[pl.ds(0, E_ROWS)], wf_v), (dd, dd_v), (xn, xn_v), (rg, rg_v), (ru, ru_v), (rd, rd_v), (cg, cg_v), (cu, cu_v), (cd, cd_v), (hyper, hyp)))]
    for load in loads:
        load.start()

    def first_partial():
        for load in loads[:2]:
            load.wait()
        e_v[...] = lax.dot_general(wf_v[...].astype(BF16), dd_v[...], (((1,), (1,)), ((), ())), preferred_element_type=F32)

    @pl.when(col == 0)
    def _():
        first_partial()

    pl.semaphore_wait(barrier, len(others))

    def remote(src, dst, sems, k, target):
        return pltpu.make_async_remote_copy(src_ref=src, dst_ref=dst, send_sem=sems.at[0, k], recv_sem=sems.at[1, k],
                                            device_id=target, device_id_type=MESH)

    def ranged(src, dst, sems, counts, at=0, to=0):
        copies = []
        for k, n in enumerate(counts):
            copies.append(remote(src.at[pl.ds(at, n)], dst.at[pl.ds(at + to, n)], sems, k, across))
            at += n
        return copies

    across = (1 - col, row)
    chip = (col, lax.rem(row + 2, nr))
    core = (col, row + 1 - 2 * lax.rem(row, 2))
    rows_of = lambda r: pl.ds(pl.multiple_of(r * quarter, quarter), quarter)
    dy_copy = remote(dd.at[rows_of(row)], dy_v.at[rows_of(row)], dsem, 0, across)
    p_copies = ranged(p_v, pin_v, psem, P_SENT)
    w_copies = ranged(wb_v, win_v, wsem, W_SENT, E_ROWS, -E_ROWS)
    a_copies = ranged(dxa_v, dxa_early, asem, R_SENT, E_ROWS)
    e_copy = remote(e_v, ein_v, esem, 0, across)
    e_back = remote(dxa_v.at[pl.ds(0, E_ROWS)], dxa_early.at[pl.ds(0, E_ROWS)], esem, 1, across)
    dims_t = (((1,), (1,)), ((), ()))

    def act_rows(at, n, ready):
        o = lax.dot_general(wb_v[at:at + n, :], dd_v[...], dims_t, preferred_element_type=F32)
        ready()
        o = o + lax.dot_general(win_v[at - E_ROWS:at - E_ROWS + n, :], dy_v[...], dims_t, preferred_element_type=F32)
        dxa_v[at:at + n, :] = o.astype(BF16)

    @pl.when(col == 0)
    def _():
        e_copy.start()

    @pl.when(col == 1)
    def _():
        dy_copy.start()
        first_partial()

    by_n = lambda width: pl.BlockSpec((nb, width), lambda k: (k, 0))
    by_m = lambda width: pl.BlockSpec((mb, width), lambda k: (k, 0))

    wsq_d[...] = jnp.zeros_like(wsq_d)

    def cast_body(start, w_b):
        w = w_b[...]
        wsq_d[...] += fold_rows(w * w)
        wb_v[pl.ds(pl.multiple_of((start + pl.program_id(0)) * mb, mb), mb), :] = w.astype(BF16)

    def cast(start, count):
        pltpu.emit_pipeline(functools.partial(cast_body, start), grid=(count,), in_specs=[
            pl.BlockSpec((mb, wd.shape[1]), lambda k: (start + k, 0), pipeline_mode=pl.Buffered(4))])(wd)

    p_v[...] = jnp.zeros_like(p_v)
    wsq[...] = jnp.zeros_like(wsq)

    def part_body(start, wg_b, wu_b, dg_b, du_b):
        rows = slice(start, start + wg_b.shape[1])
        for k, (w_b, d_b) in enumerate(((wg_b, dg_b), (wu_b, du_b))):
            w = w_b[...]
            wsq[8 * k:8 * k + 8, rows] += fold_rows(w * w)
            p_v[rows, :] += lax.dot_general(w.astype(BF16), d_b[...], (((0,), (0,)), ((), ())), preferred_element_type=F32)

    def partial_rows(start, count):
        deep_n = lambda width: pl.BlockSpec((nb, width), lambda k: (k, 0), pipeline_mode=pl.Buffered(3))
        cols = pl.ds(start, count)
        pltpu.emit_pipeline(functools.partial(part_body, start), grid=(STEPS,),
                            in_specs=[deep_n(count)] * 2 + [deep_n(dg.shape[1])] * 2)(wg.at[:, cols], wu.at[:, cols], dg, du)

    partial_rows(0, P_FIRST)

    @pl.when(col == 0)
    def _():
        p_copies[0].start()

    cast(0, CAST_FIRST)

    @pl.when(col == 1)
    def _():
        w_copies[0].start()

    partial_rows(P_FIRST, wg.shape[1] - P_FIRST)

    @pl.when(col == 0)
    def _():
        p_copies[1].start()

    cast(CAST_FIRST, STEPS - CAST_FIRST)

    q_far = remote(dy_v.at[rows_of(row)], dy_v.at[rows_of(row)], qsem, 0, chip)
    q_near = remote(dy_v.at[rows_of(row)], dy_v.at[rows_of(row)], qsem, 1, core)
    q_both = remote(dy_v.at[rows_of(chip[1])], dy_v.at[rows_of(chip[1])], qsem, 2, core)

    @pl.when(col == 0)
    def _():
        dy_copy.wait_recv()
        q_far.start()
        q_near.start()

    for load in loads[2:]:
        load.wait()
    r_mine[...] = jnp.zeros_like(r_mine)
    racc[...] = jnp.zeros_like(racc)
    cacc[...] = jnp.zeros_like(cacc)

    def grad_body(dg_b, du_b, xa_b, gg_b, gu_b, gd_b):
        k = pl.program_id(0)
        for t, (d_b, g_b) in enumerate(((dg_b, gg_b), (du_b, gu_b))):
            g = jnp.dot(d_b[...], xn_v[...], preferred_element_type=F32)
            g_b[...] = g
            q = g * g + EPS_ONE
            racc[pl.ds(8 * t, 8), :] += fold_rows(q)
            c_all[row, pl.ds(7 * t + k, 1), :] = jnp.sum(fold(q).T, axis=0, keepdims=True)
        g = jnp.dot(xa_b[...], dd_v[...], preferred_element_type=F32)
        gd_b[...] = g
        q = g * g + EPS_ONE
        cacc[...] += fold_rows(q)
        r_mine[pl.ds(8 + k, 1), pl.ds(0, 240)] = jnp.sum(fold(q).T, axis=0, keepdims=True)

    pltpu.emit_pipeline(grad_body, grid=(STEPS,), in_specs=[by_n(dg.shape[1])] * 2 + [by_m(xa.shape[1])],
                        out_specs=[by_n(gg.shape[1])] * 2 + [by_m(gd.shape[1])])(dg, du, xa, gg, gu, gd)

    for t in range(2):
        r_mine[t:t + 1, :] = jnp.sum(racc[8 * t:8 * t + 8, :], axis=0, keepdims=True)
    c_down = jnp.sum(cacc[...], axis=0, keepdims=True)
    for k in range(5):
        c_all[row, 14 + k:15 + k, 0:256] = c_down[:, 256 * k:256 * (k + 1)]

    r_send[...] = jnp.zeros_like(r_send)
    r_send[:, 0:256] = r_mine[8:16, 0:256]
    for t in range(2):
        for j in range(5):
            r_send[j:j + 1, 128 * (2 + t):128 * (3 + t)] = r_mine[t:t + 1, 128 * j:128 * (j + 1)]
    r_copy = remote(r_send, r_got, rsem, 0, across)
    r_copy.start()
    c_copies = [pltpu.make_async_remote_copy(
        src_ref=c_all.at[row], dst_ref=c_all.at[row], send_sem=csem.at[0, d], recv_sem=csem.at[1, row],
        device_id=(col, lax.rem(row + d, nr)), device_id_type=MESH) for d in range(1, nr)]
    for c in c_copies:
        c.start()

    @pl.when(col == 0)
    def _():
        p_copies[2].start()
        q_far.wait_recv()
        q_both.start()

        def first_ready():
            w_copies[0].wait_recv()
            q_near.wait_recv()
            q_both.wait_recv()
            q_far.wait_send()
            q_near.wait_send()
            q_both.wait_send()

        act_rows(E_ROWS, A_ROWS[0], first_ready)

    @pl.when(col == 1)
    def _():
        w_copies[1].start()
        e_copy.wait_recv()
        dxa_v[0:E_ROWS, :] = (e_v[...] + ein_v[...]).astype(BF16)

    beta = hyp[0]
    rr[...] = jnp.ones_like(rr)
    rr[0:1, :] = rg_v[...].reshape(1, -1)
    rr[1:2, :] = ru_v[...].reshape(1, -1)
    r_old, g_old, u_old, d_old = [v[...].reshape(1, -1) for v in (rd_v, cg_v, cu_v, cd_v)]
    for k in range(STEPS):
        cc[k:k + 1, :] = g_old[:, nb * k:nb * (k + 1)]
        cc[7 + k:8 + k, :] = u_old[:, nb * k:nb * (k + 1)]
        rr[8 + k:9 + k, 0:mb] = r_old[:, mb * k:mb * (k + 1)]
    for k in range(5):
        cc[14 + k:15 + k, 0:256] = d_old[:, 256 * k:256 * (k + 1)]
        cc[14 + k:15 + k, 256:480] = jnp.ones((1, 224), F32)
    cc[19:24, :] = jnp.ones((5, 480), F32)

    r_peer[...] = jnp.zeros_like(r_peer)
    r_copy.wait()
    r_peer[8:16, 0:256] = r_got[:, 0:256]
    for t in range(2):
        for j in range(5):
            r_peer[t:t + 1, 128 * j:128 * (j + 1)] = r_got[j:j + 1, 128 * (2 + t):128 * (3 + t)]
    for d in range(1, nr):
        c_copies[d - 1].wait_send()
        s = lax.rem(row + d, nr)
        pltpu.make_async_remote_copy(src_ref=c_all.at[s], dst_ref=c_all.at[s], send_sem=csem.at[0, d], recv_sem=csem.at[1, s],
                                     device_id=(col, s), device_id_type=MESH).wait_recv()

    line = lax.broadcasted_iota(jnp.int32, rr.shape, 0)
    r_new = beta * rr[...] + (1.0 - beta) * ((r_mine[...] + r_peer[...]) / jnp.where(line < 8, float(d_ff), float(d_model)))
    line = lax.broadcasted_iota(jnp.int32, cc.shape, 0)
    c_sum = (c_all[0] + c_all[1]) + (c_all[2] + c_all[3])
    c_new = beta * cc[...] + (1.0 - beta) * (c_sum / jnp.where(line < 14, float(d_model), float(d_ff)))
    r_out[...] = r_new
    c_out[...] = c_new
    rr[...] = lax.rsqrt(r_new)
    cc[...] = lax.rsqrt(c_new)
    save_r = pltpu.make_async_copy(r_out, r_hbm, loc.at[12])
    save_c = pltpu.make_async_copy(c_out, c_hbm, loc.at[13])

    sacc[...] = jnp.zeros_like(sacc)

    def square_body(gg_b, gu_b, gd_b):
        k = pl.program_id(0)
        for t, g_b in enumerate((gg_b, gu_b)):
            u = g_b[...] * rr[t:t + 1, :]
            s = fold(u * u)
            c = column(cc[pl.ds(7 * t + k, 1), :])
            sacc[pl.ds(8 * t, 8), :] += fold_rows(s * (c * c))
        c_row = jnp.concatenate([cc[14 + j:15 + j, 0:256] for j in range(5)], axis=1)
        u = gd_b[...] * c_row
        s = fold(u * u)
        r = column(rr[pl.ds(8 + k, 1), :])[0:mb]
        sacc[16:24, :] += fold_rows(s * (r * r))

    pltpu.emit_pipeline(square_body, grid=(STEPS,), in_specs=[by_n(gg.shape[1])] * 2 + [by_m(gd.shape[1])])(gg, gu, gd)

    for t in range(3):
        s_all[row, t:t + 1, :] = jnp.sum(sacc[8 * t:8 * t + 8, :], axis=0, keepdims=True)
    for t in range(2):
        s_all[row, 3 + t:4 + t, :] = jnp.sum(fold(wsq[8 * t:8 * t + 8, :]), axis=0, keepdims=True)
        s_all[row, 6 + t:7 + t, :] = lane_total(r_new[t:t + 1, :])
    s_all[row, 5:6, :] = jnp.sum(fold(wsq_d[...]), axis=0, keepdims=True)
    s_all[row, 8:9, :] = lane_total(r_new[8:15, 0:mb])
    s_copies = [pltpu.make_async_remote_copy(
        src_ref=s_all.at[row], dst_ref=s_all.at[row], send_sem=ssem.at[0, d], recv_sem=ssem.at[1, row],
        device_id=(col, lax.rem(row + d, nr)), device_id_type=MESH) for d in range(1, nr)]
    for s in s_copies:
        s.start()
    for d in range(1, nr):
        s_copies[d - 1].wait_send()
        him = lax.rem(row + d, nr)
        pltpu.make_async_remote_copy(src_ref=s_all.at[him], dst_ref=s_all.at[him], send_sem=ssem.at[0, d],
                                     recv_sem=ssem.at[1, him], device_id=(col, him), device_id_type=MESH).wait_recv()
    s_mine[...] = (s_all[0] + s_all[1]) + (s_all[2] + s_all[3])
    s_copy = remote(s_mine, s_peer, ssem, nr, across)
    s_copy.start()

    @pl.when(col == 0)
    def _():
        p_copies[3].start()
        a_copies[0].start()

    @pl.when(col == 1)
    def _():
        for w in w_copies[2:]:
            w.start()
        e_back.start()

    s_copy.wait()
    total = s_mine[...] + s_peer[...]
    sums = jnp.sum(total, axis=1, keepdims=True)
    scales = []
    for t, (m, n) in enumerate(((d_model, d_ff), (d_model, d_ff), (d_ff, d_model))):
        r_mean = sums[6 + t:7 + t] / float(m * nc)
        rms_u = jnp.sqrt(sums[t:t + 1] * r_mean / float(m * n))
        step = hyp[1] * jnp.maximum(EPS_TWO, jnp.sqrt(sums[3 + t:4 + t] / float(m * n)))
        scales.append(step * jnp.sqrt(r_mean) / jnp.maximum(1.0, rms_u / hyp[2]))
    rs_v[...] = rr[...]
    rs_v[0:1, :] = rr[0:1, :] * scales[0]
    rs_v[1:2, :] = rr[1:2, :] * scales[1]
    rs_v[8:16, :] = rr[8:16, :] * scales[2]
    save_stats = (save_r, save_c)
    for c in save_stats:
        c.start()

    def wide_body(wg_b, wu_b, gg_b, gu_b, ng_b, nu_b):
        k = pl.program_id(0)
        for t, (w, g, o) in enumerate(((wg_b, gg_b, ng_b), (wu_b, gu_b, nu_b))):
            c = column(cc[pl.ds(7 * t + k, 1), :])
            for j in range(w.shape[1] // 128):
                lanes = slice(128 * j, 128 * (j + 1))
                o[:, lanes] = w[:, lanes] - g[:, lanes] * rs_v[t:t + 1, lanes] * c

    def down_body(w, g, o):
        r = column(rs_v[pl.ds(8 + pl.program_id(0), 1), :])[0:mb]
        for j in range(w.shape[1] // 128):
            lanes = slice(128 * j, 128 * (j + 1))
            c = cc[14 + j // 2:15 + j // 2, 128 * (j % 2):128 * (j % 2 + 1)]
            o[:, lanes] = w[:, lanes] - g[:, lanes] * c * r

    early = E_ROWS + sum(R_SENT)
    rows_a = dxa_v.shape[0]
    save_e = pltpu.make_async_copy(dxa_v.at[pl.ds(0, E_ROWS)], dxa_early.at[pl.ds(0, E_ROWS)], loc.at[10])
    save_a = pltpu.make_async_copy(dxa_v.at[pl.ds(E_ROWS, early - E_ROWS)], dxa_early.at[pl.ds(E_ROWS, early - E_ROWS)], loc.at[10])
    save_late = pltpu.make_async_copy(dxa_v.at[pl.ds(early, rows_a - early)], late, loc.at[11])
    save_pack = [pltpu.make_async_copy(a, b, loc.at[16 + k]) for k, (a, b) in enumerate(norm_pairs(dxn_v, late))]

    def norm_columns(start, stop):
        for j in range(start, stop, 128):
            dxn_v[:, j:j + 128] = (p_v[j:j + 128, :] + pin_v[j:j + 128, :]).T.astype(BF16)

    def act_chunk(k):
        new = A_NEEDS[k] != A_NEEDS[k - 1]
        act_rows(E_ROWS + sum(A_ROWS[:k]), A_ROWS[k], w_copies[A_NEEDS[k]].wait_recv if new else lambda: None)
        if k < len(R_SENT):
            a_copies[k].start()

    @pl.when(col == 0)
    def _():
        act_chunk(1)

    pltpu.emit_pipeline(wide_body, grid=(STEPS,), in_specs=[by_n(wg.shape[1])] * 4,
                        out_specs=[by_n(wg.shape[1])] * 2)(wg, wu, gg, gu, ng, nu)

    @pl.when(col == 0)
    def _():
        act_chunk(2)

    @pl.when(col == 1)
    def _():
        save_e.start()
        for p in p_copies:
            p.wait_recv()
        norm_columns(0, dxn_v.shape[1])
        for c in save_pack:
            c.start()

    pltpu.emit_pipeline(down_body, grid=(STEPS,), in_specs=[by_m(wd.shape[1])] * 2,
                        out_specs=[by_m(wd.shape[1])])(wd, gd, nd)

    @pl.when(col == 0)
    def _():
        act_chunk(3)
        save_a.start()
        act_chunk(4)
        save_late.start()
        e_copy.wait_send()
        for p in p_copies:
            p.wait_send()
        save_a.wait()
        save_late.wait()
        e_back.wait_recv()
        for a in a_copies:
            a.wait_send()

    @pl.when(col == 1)
    def _():
        save_e.wait()
        for c in save_pack:
            c.wait()
        dy_copy.wait_send()
        for w in w_copies:
            w.wait_send()
        e_back.wait_send()
        for a in a_copies:
            a.wait_recv()

    for c in save_stats:
        c.wait()


def run_fused(nc, nr, sizes, wg, wu, wd, xn, xa, dg, du, dd, rg, ru, rd, cg, cu, cd, hyper):
    f32, b16 = (lambda *s: jax.ShapeDtypeStruct(s, F32)), (lambda *s: jax.ShapeDtypeStruct(s, BF16))
    n, i = wg.shape
    m, h = wd.shape
    t = dd.shape[0]
    early = E_ROWS + sum(R_SENT)
    dma = lambda *s: pltpu.SemaphoreType.DMA(s)
    vf = lambda *s: pltpu.VMEM(s, F32)
    vb = lambda *s: pltpu.VMEM(s, BF16)
    return pl.pallas_call(
        functools.partial(fused, nc, nr, sizes),
        out_shape=(f32(n, i), f32(n, i), f32(m, h), f32(n, i), f32(n, i), f32(m, h), b16(early, t), b16(m - early, t),
                   f32(16, 640), f32(24, 480)),
        in_specs=[HBM] * 15,
        out_specs=[HBM] * 10,
        scratch_shapes=[
            vb(*xn.shape), vb(t, h), vf(E_ROWS, h), vb(t, h), vf(E_ROWS, t), vf(E_ROWS, t), vf(i, t), vf(i, t), vb(m, h), vb(m - E_ROWS, h),
            vb(m, t), vb(t, i),
            vf(i), vf(i), vf(m), vf(n), vf(n), vf(h), pltpu.SMEM((3,), F32),
            vf(16, 640), vf(16, 640), vf(8, 512), vf(8, 512), vf(nr, 24, 480), vf(nr, 16, 128), vf(16, 128), vf(16, 128), vf(16, i), vf(8, h),
            vf(16, 640), vf(24, 480), vf(16, i), vf(8, h), vf(24, 128),
            vf(16, 640), vf(24, 480), vf(16, 640),
            dma(26), dma(2, 1), dma(2, 2), dma(2, 3), dma(2, len(P_SENT)), dma(2, len(W_SENT)), dma(2, len(R_SENT)), dma(2, 1),
            dma(2, nr), dma(2, nr + 1)],
        compiler_params=pltpu.CompilerParams(collective_id=0, has_side_effects=True, vmem_limit_bytes=60 * 1024 * 1024),
        cost_estimate=pl.CostEstimate(flops=22_000_000_000, bytes_accessed=150_000_000, transcendentals=0),
        name="fused",
    )(wg, wu, wd, xn, xa, dg, du, dd, rg, ru, rd, cg, cu, cd, hyper)


def placements(col, buf, a_out, n_out, sending):
    rows = a_out.shape[0] - buf.shape[0]
    act = [(buf, a_out.at[pl.ds(rows, buf.shape[0])])]
    norm = [(b, a) for a, b in norm_pairs(n_out, buf)]
    return (act, norm) if sending else (norm, act)


def per_side(col, choices, sem, at, action):
    for side, pairs in enumerate(choices):
        @pl.when(col == side)
        def _(pairs=pairs):
            for j, (a, b) in enumerate(pairs):
                action(pltpu.make_async_copy(a, b, sem.at[at + j]))


def publish_kernel(r_hbm, c_hbm, wg, wu, wd, a_in, l_in, ng, nu, nd, a_out, n_out,
                   rgo, ruo, rdo, cgo, cuo, cdo, r_new, c_new, a_v, l_v, sem):
    k = pl.program_id(0)
    col = lax.axis_index('col')
    mb = wd.shape[0]
    pairs = ((r_hbm, r_new), (c_hbm, c_new), (a_in, a_v), (l_in, l_v),
             (a_v, a_out.at[pl.ds(0, a_v.shape[0])]))
    copies = [pltpu.make_async_copy(a, b, sem.at[j]) for j, (a, b) in enumerate(pairs)]
    own = placements(col, l_v, a_out, n_out, True)

    @pl.when(k == 0)
    def _():
        for c in copies[:4]:
            c.start()

    @pl.when(k == 1)
    def _():
        for c in copies[:4]:
            c.wait()
        for c in copies[4:]:
            c.start()
        per_side(col, own, sem, len(pairs), lambda c: c.start())
        rgo[...] = r_new[0:1, :].reshape(-1)
        ruo[...] = r_new[1:2, :].reshape(-1)
        rdo[...] = jnp.concatenate([r_new[8 + j:9 + j, 0:mb] for j in range(STEPS)], axis=1).reshape(-1)
        cgo[...] = jnp.concatenate([c_new[j:j + 1, :] for j in range(STEPS)], axis=1).reshape(-1)
        cuo[...] = jnp.concatenate([c_new[7 + j:8 + j, :] for j in range(STEPS)], axis=1).reshape(-1)
        cdo[...] = jnp.concatenate([c_new[14 + j:15 + j, 0:256] for j in range(5)], axis=1).reshape(-1)

    @pl.when(k == STEPS - 1)
    def _():
        for c in copies[4:]:
            c.wait()
        per_side(col, own, sem, len(pairs), lambda c: c.wait())

    ng[...] = wg[...]
    nu[...] = wu[...]
    nd[...] = wd[...]


def run_publish(r_new, c_new, wg, wu, wd, a_early, late):
    f32 = lambda *s: jax.ShapeDtypeStruct(s, F32)
    b16 = lambda *s: jax.ShapeDtypeStruct(s, BF16)
    n, i = wg.shape
    m, h = wd.shape
    t = late.shape[1]
    flat = lambda s: pl.BlockSpec((s,), lambda k: (0,))
    by_n = pl.BlockSpec((n // STEPS, i), lambda k: (k, 0))
    by_m = pl.BlockSpec((m // STEPS, h), lambda k: (k, 0))
    return pl.pallas_call(
        publish_kernel, grid=(STEPS,),
        out_shape=(f32(n, i), f32(n, i), f32(m, h), b16(m, t), b16(t, i), f32(i), f32(i), f32(m), f32(n), f32(n), f32(h)),
        in_specs=[HBM] * 2 + [by_n, by_n, by_m] + [HBM] * 2,
        out_specs=[by_n, by_n, by_m, HBM, HBM] + [flat(s) for s in (i, i, m, n, n, h)],
        scratch_shapes=[pltpu.VMEM(a.shape, a.dtype) for a in (r_new, c_new, a_early, late)] + [
            pltpu.SemaphoreType.DMA((16,))],
        compiler_params=pltpu.CompilerParams(vmem_limit_bytes=60 * 1024 * 1024),
        cost_estimate=pl.CostEstimate(flops=20_000_000_000, bytes_accessed=58_000_000, transcendentals=0),
        name="publish",
    )(r_new, c_new, wg, wu, wd, a_early, late)


def place_kernel(late_in, a_in, n_in, a_out, n_out, sem):
    col = lax.axis_index('col')
    got = placements(col, late_in, a_out, n_out, False)
    per_side(col, got, sem, 0, lambda c: c.start())
    per_side(col, got, sem, 0, lambda c: c.wait())


def run_place(late_in, dxa, dxn):
    return pl.pallas_call(
        place_kernel,
        out_shape=(jax.ShapeDtypeStruct(dxa.shape, BF16), jax.ShapeDtypeStruct(dxn.shape, BF16)),
        in_specs=[pl.BlockSpec(memory_space=pl.ANY), HBM, HBM], out_specs=[HBM, HBM], input_output_aliases={1: 0, 2: 1},
        scratch_shapes=[pltpu.SemaphoreType.DMA((10,))],
        compiler_params=pltpu.CompilerParams(vmem_limit_bytes=1024 * 1024),
        name="place",
    )(late_in, dxa, dxn)


SWAP = [(0, 1), (1, 0)]


def solution(mesh):
    row_size = mesh.shape['row']
    col_size = mesh.shape['col']
    weight_spec = P('row', 'col')
    act_spec = P(None, 'row')
    grad_spec = P(None, 'col')
    in_specs = (weight_spec,) * 3 + (act_spec, act_spec) + (grad_spec,) * 3 + (P('row'), P('col')) * 3 + (P(),)
    out_specs = (weight_spec,) * 3 + (P('row'), P('col')) * 3 + (act_spec, act_spec)

    def body(w_gate, w_up, w_down, x_norm, x_act, dy_gate, dy_up, dy_down, r_gate, c_gate, r_up, c_up, r_down, c_down, hyper_params):
        d_model = w_gate.shape[0] * row_size
        d_ff = w_gate.shape[1] * col_size
        _, _, _, ng, nu, nd, a_early, late, r_new, c_new = run_fused(
            col_size, row_size, (d_model, d_ff),
            w_gate.T, w_up.T, w_down, x_norm, x_act.T, dy_gate.T, dy_up.T, dy_down,
            r_gate, r_up, r_down, c_gate, c_up, c_down, hyper_params)
        late_in = lax.ppermute(late, 'col', SWAP)
        ng, nu, nd, dxa, dxn, rgo, ruo, rdo, cgo, cuo, cdo = run_publish(r_new, c_new, ng, nu, nd, a_early, late)
        dx_act, dx_norm = run_place(late_in, dxa, dxn)
        return (ng.T, nu.T, nd, rgo, cgo, ruo, cuo, rdo, cdo, dx_norm, dx_act.T)

    return jax.shard_map(body, mesh=mesh, in_specs=in_specs, out_specs=out_specs, check_vma=False)
```
